128 devices in a mesh: chain: 8 (over x, core), quad: 16 (over z, y).
Axes of the slice: x: 4, y: 4, z: 4, core: 2. Of those that a mesh axis runs over, the one named last changes fastest.
Arguments:
- sections: bfloat16 [8, 4096, 4096], P('chain', 'quad'), may hold values from -8 to 8
- anchor: bfloat16 [4096, 4096], P('quad'), may hold values from -8 to 8
Outputs:
- registered: bfloat16 [8, 4096, 4096], P('chain', 'quad')
- accumulated: float32 [8, 64, 128], P('chain')
The draws below stay inside these ranges and needn't reach their ends.
All inputs are finite; a program needn't handle non-finite values.
Results may differ from the reference program's by a relative error of at most 0.00135.
The reference program's roundings to bfloat16 on the way count: a program that leaves them out, or rounds other values in their place, can miss the bound.
Values may be sent and summed in bfloat16 or wider, within the bound.
A program may use at most 128 MiB of HBM per device.

```python
import math
import jax
import jax.numpy as jnp
from jax import lax

GRID_SIZE = 64
ITERATIONS = 4
HEIGHT = 4096
COLUMNS = 4096
SLICES = 8


def box_blur(values, window, which_axis):
    lead_pad = window // 2 + 1
    tail_pad = window - 1 - window // 2
    pad_spec = [(0, 0), (0, 0)]
    pad_spec[which_axis] = (lead_pad, tail_pad)
    padded = jnp.pad(values, pad_spec, mode='wrap')
    running = jnp.cumsum(padded, axis=which_axis)
    length = values.shape[which_axis]
    upper_sums = lax.slice_in_dim(running, window, window + length, axis=which_axis)
    lower_sums = lax.slice_in_dim(running, 0, length, axis=which_axis)
    return (upper_sums - lower_sums) / window


def mode_table(point_count, mode_count):
    positions = (jnp.arange(point_count, dtype=jnp.float32) + 0.5) / point_count
    orders = jnp.arange(mode_count, dtype=jnp.float32)
    return jnp.cos(math.pi * positions[:, None] * orders[None, :])


def stack_helper(key):
    base_key = jax.random.fold_in(key, 4111)
    key_list = jax.random.split(base_key, 4)
    row_spread, col_spread, floor_gain, background, noise_level, sway_scale = (3.0, 1.5, 0.5, 0.3, 0.25, 0.3)
    texture = jax.random.normal(key_list[0], (HEIGHT, COLUMNS), jnp.float32)
    for which_axis in (0, 1):
        texture = box_blur(box_blur(texture, 3, which_axis), 3, which_axis)
    texture = texture - jnp.mean(texture)
    texture = texture / jnp.sqrt(jnp.mean(texture * texture))
    row_pos = (jnp.arange(HEIGHT, dtype=jnp.float32) + 0.5) / HEIGHT
    col_pos = (jnp.arange(COLUMNS, dtype=jnp.float32) + 0.5) / COLUMNS
    gain_field = floor_gain * jnp.exp(math.log(row_spread) * row_pos[:, None] + math.log(col_spread) * col_pos[None, :])
    row_modes = mode_table(HEIGHT, 4)
    col_modes = mode_table(COLUMNS, 4)
    steps_xy = sway_scale * jax.random.normal(key_list[1], (SLICES + 1, 2, 4, 4), jnp.float32)
    totals = jnp.cumsum(steps_xy, axis=0)
    stains = jnp.exp(jax.random.uniform(key_list[2], (SLICES + 1,), jnp.float32, -0.25, 0.25))
    flat_texture = texture.reshape(-1)
    row_coord = jnp.arange(HEIGHT, dtype=jnp.float32)[:, None]
    col_coord = jnp.arange(COLUMNS, dtype=jnp.float32)[None, :]

    def one_slice(slice_number):
        mixing = totals[slice_number]
        move_x = jnp.dot(jnp.dot(row_modes, mixing[0]), col_modes.T)
        move_y = jnp.dot(jnp.dot(row_modes, mixing[1]), col_modes.T)
        pos_y = jnp.clip(row_coord + move_y, 0.0, HEIGHT - 1.0)
        pos_x = jnp.clip(col_coord + move_x, 0.0, COLUMNS - 1.0)
        floor_y = jnp.floor(pos_y)
        floor_x = jnp.floor(pos_x)
        frac_y = pos_y - floor_y
        frac_x = pos_x - floor_x
        low_y = floor_y.astype(jnp.int32)
        low_x = floor_x.astype(jnp.int32)
        high_y = jnp.minimum(low_y + 1, HEIGHT - 1)
        high_x = jnp.minimum(low_x + 1, COLUMNS - 1)
        sample = (1.0 - frac_y) * (1.0 - frac_x) * flat_texture[low_y * COLUMNS + low_x]
        sample = sample + (1.0 - frac_y) * frac_x * flat_texture[low_y * COLUMNS + high_x]
        sample = sample + frac_y * (1.0 - frac_x) * flat_texture[high_y * COLUMNS + low_x]
        sample = sample + frac_y * frac_x * flat_texture[high_y * COLUMNS + high_x]
        noise_field = jax.random.normal(jax.random.fold_in(key_list[3], slice_number), (HEIGHT, COLUMNS), jnp.float32)
        section_image = stains[slice_number] * gain_field * sample + background + noise_level * noise_field
        return jnp.clip(section_image, -8.0, 8.0)
    return lax.map(one_slice, jnp.arange(SLICES + 1, dtype=jnp.int32))


def draw_sections(key, part):
    return stack_helper(key)[1:].astype(jnp.bfloat16)


def draw_anchor(key, part):
    return stack_helper(key)[0].astype(jnp.bfloat16)


def setup_inputs(seed: int = 0) -> dict:
    streams_of = jax.random.split(jax.random.key(seed), 3)
    return {
        "sections": draw_sections(jax.random.fold_in(streams_of[2], 71), 0),
        "anchor": draw_anchor(jax.random.fold_in(streams_of[2], 71), 0),
    }


EPSILON = 1e-06
SMOOTHING = 0.25
EXACT_PRECISION = lax.Precision.HIGHEST

def spline_weight(offset):
    distance = jnp.abs(offset)
    near_part = 2.0 / 3.0 - distance * distance + 0.5 * distance * distance * distance
    remain = 2.0 - distance
    far_part = remain * remain * remain / 6.0
    return jnp.where(distance < 1.0, near_part, jnp.where(distance < 2.0, far_part, 0.0 * distance))

def spline_basis(first_row, pixel_count, extent):
    spacing = extent // GRID_SIZE
    pixels = (first_row + jnp.arange(pixel_count, dtype=jnp.int32)).astype(jnp.float32)
    knot_pos = jnp.arange(GRID_SIZE, dtype=jnp.int32).astype(jnp.float32)
    offset = (pixels[:, None] + 0.5) / spacing - knot_pos[None, :] - 0.5
    return spline_weight(offset)

def slopes(images):
    padded = jnp.pad(images, ((0, 0), (1, 1), (1, 1)))
    along_x = 0.5 * (padded[:, 1:-1, 2:] - padded[:, 1:-1, :-2])
    along_y = 0.5 * (padded[:, 2:, 1:-1] - padded[:, :-2, 1:-1])
    return (along_x, along_y)

def displace(coefficients, row_basis, col_half):
    row_mixed = jnp.einsum('hg,bgk->bhk', row_basis, coefficients, precision=EXACT_PRECISION)
    row_mixed = row_mixed.astype(jnp.bfloat16).astype(jnp.float32)
    col_wide = col_half.astype(jnp.float32)
    shift_x = jnp.einsum('bhg,wg->bhw', row_mixed[:, :, :GRID_SIZE], col_wide, precision=EXACT_PRECISION)
    shift_y = jnp.einsum('bhg,wg->bhw', row_mixed[:, :, GRID_SIZE:], col_wide, precision=EXACT_PRECISION)
    return (shift_x, shift_y)

def project(field_x, field_y, row_basis, col_half):
    col_wide = col_half.astype(jnp.float32)
    rounded_x = field_x.astype(jnp.bfloat16).astype(jnp.float32)
    rounded_y = field_y.astype(jnp.bfloat16).astype(jnp.float32)
    cols_x = jnp.einsum('bhw,wg->bhg', rounded_x, col_wide, precision=EXACT_PRECISION)
    cols_y = jnp.einsum('bhw,wg->bhg', rounded_y, col_wide, precision=EXACT_PRECISION)
    joined = jnp.concatenate([cols_x, cols_y], axis=2)
    return jnp.einsum('hg,bhk->bgk', row_basis, joined, precision=EXACT_PRECISION)

def normalized(gradient):
    magnitude = lax.optimization_barrier(jnp.mean(gradient * gradient, axis=(1, 2), keepdims=True))
    return gradient / jnp.sqrt(magnitude + EPSILON)

def ncc_direction(moving, fixed_image, coefficients, row_basis, col_half):
    along_x, along_y = slopes(moving)
    shift_x, shift_y = displace(coefficients, row_basis, col_half)
    warped = moving + shift_x * along_x + shift_y * along_y
    pixel_count = moving.shape[1] * moving.shape[2]
    centred_f = fixed_image - lax.optimization_barrier(jnp.mean(fixed_image, axis=(1, 2), keepdims=True))
    centred_m = warped - lax.optimization_barrier(jnp.mean(warped, axis=(1, 2), keepdims=True))
    moving_var = lax.optimization_barrier(jnp.sum(centred_m * centred_m, axis=(1, 2), keepdims=True))
    cross_var = lax.optimization_barrier(jnp.sum(centred_f * centred_m, axis=(1, 2), keepdims=True))
    denominator = jnp.sqrt(moving_var + EPSILON)
    ncc_score = cross_var / denominator
    pixel_grad = pixel_count * (centred_f / denominator - ncc_score / (moving_var + EPSILON) * centred_m)
    return normalized(project(pixel_grad * along_x, pixel_grad * along_y, row_basis, col_half))

def reference(sections, anchor):
    slice_total, height, columns = sections.shape
    row_basis = spline_basis(0, height, height)
    col_half = spline_basis(0, columns, columns).astype(jnp.bfloat16)
    step_rate = 1.0 / ITERATIONS
    previous = jnp.concatenate([anchor[None], sections[:-1]], axis=0)
    moving_blocks = sections.reshape(slice_total, 1, height, columns)
    fixed_blocks = previous.reshape(slice_total, 1, height, columns)
    coefficients = jnp.zeros((slice_total, GRID_SIZE, 2 * GRID_SIZE), jnp.float32)

    def one_block(packed):
        moving, fixed_image, block_coef = packed
        return ncc_direction(moving.astype(jnp.float32), fixed_image.astype(jnp.float32), block_coef, row_basis, col_half)
    for iteration in range(ITERATIONS):
        shaped = coefficients.reshape(slice_total, 1, GRID_SIZE, 2 * GRID_SIZE)
        direction = lax.map(one_block, (moving_blocks, fixed_blocks, shaped))
        direction = direction.reshape(slice_total, GRID_SIZE, 2 * GRID_SIZE)
        padded = jnp.pad(coefficients, ((1, 1), (0, 0), (0, 0)))
        smooth = padded[:-2] - 2.0 * coefficients + padded[2:]
        coefficients = coefficients + step_rate * direction + SMOOTHING * smooth
    accumulated = jnp.cumsum(coefficients, axis=0)

    def warp_block(packed):
        moving, block_coef = packed
        moving = moving.astype(jnp.float32)
        along_x, along_y = slopes(moving)
        shift_x, shift_y = displace(block_coef, row_basis, col_half)
        return (moving + shift_x * along_x + shift_y * along_y).astype(jnp.bfloat16)
    registered = lax.map(warp_block, (moving_blocks, accumulated.reshape(slice_total, 1, GRID_SIZE, 2 * GRID_SIZE)))
    registered = registered.reshape(slice_total, height, columns)
    return (registered, accumulated)
```

```python
import numpy as np
import jax
import jax.numpy as jnp
from jax import lax
from jax.experimental import pallas as pl
from jax.experimental.pallas import tpu as pltpu
from jax.sharding import PartitionSpec as P

GRID = 64
ITERATIONS = 4
EPS = 1e-6
SMOOTHING = 0.25
MESH = pl.DeviceIdType.MESH
F32 = jnp.float32
BF16 = jnp.bfloat16

ROWS = 256
COLS = 4096
HALF = 128
CH = 256
NCH = COLS // CH
PAD = 128
NC = 8
NQ = 16
PIXELS = float(4096 * 4096)


def weight(offset):
    d = np.abs(offset)
    near = 2.0 / 3.0 - d * d + 0.5 * d * d * d
    r = 2.0 - d
    far = r * r * r / 6.0
    return np.where(d < 1.0, near, np.where(d < 2.0, far, 0.0 * d)).astype(np.float32)


def bf(x):
    return np.asarray(jnp.asarray(x, jnp.float32).astype(BF16).astype(jnp.float32))


def hi_lo(x):
    hi = bf(x)
    return [hi, bf(x - hi)]


def tables():
    f = np.float32
    x = np.arange(COLS, dtype=f)
    c = weight((x[:, None] + f(0.5)) / f(64) - np.arange(GRID, dtype=f)[None, :] - f(0.5))
    c = np.concatenate([c, c], axis=1)
    y = np.arange(-1, ROWS + 1, dtype=f)
    ext = weight((y[:, None] + f(0.5)) / f(64) - (np.arange(8, dtype=f) - f(2))[None, :] - f(0.5)).T
    r = ext[:, 1:-1]
    pairs = np.zeros((4, 8, ROWS), f)
    for d in range(4):
        pairs[d, : 8 - d] = r[: 8 - d] * r[d:]
    step = 0.5 * (r - ext[:, 2:])
    rows = []
    for variant in range(3):
        e = ext.copy()
        if variant == 0:
            e[:, 0] = 0.0
        if variant == 2:
            e[:, -1] = 0.0
        slope = 0.5 * (e[:, :-2] - e[:, 2:])
        rows.append(np.concatenate([pairs.reshape(32, ROWS)] + hi_lo(r) + hi_lo(slope) + hi_lo(step), axis=0))
    top = (np.arange(ROWS) < HALF).astype(f)[None]
    split = np.concatenate([h * top for h in hi_lo(r)] + [h * (1 - top) for h in hi_lo(r)], axis=0)
    hi = bf(r)
    mid = bf(r - hi)
    low = bf(r - hi - mid)
    mix = np.concatenate([hi, hi, hi, mid, mid, low, np.zeros((80, ROWS), f)], axis=0).T
    return c, np.stack(rows), split, mix


def kernel(
    sec, anc, cd_in, rt_in, sp_in, mx_in,
    reg, acc,
    ib, fb, jb, ab, i32, j32, lxb, lyb, cd, w1, rt, sp, mx,
    qb, qd, tg, ub, lhs, bdacc, sums, dsums,
    etop, ebot, emid, htop, hbot, jmid, jbot,
    gfs, gbs, gf, gb, ga, gx, bds, bhs, bdo, bdh,
    cpad, csend, cprev, cnext, ew_s, ew, tw_s, tw,
    sem_in, sem_c, sem_a,
    s_f, r_f, s_j, r_j, s_h, r_h, s_gf, r_gf, s_gb, r_gb,
    s_bo, r_bo, s_bh, r_bh, s_cp, r_cp, s_cn, r_cn, s_ew, r_ew, s_tw, r_tw,
):
    k = lax.axis_index("chain")
    s = lax.axis_index("quad")
    has_prev = k > 0
    has_next = k < NC - 1

    def remote(src, dst, ss, rs, kk, qq):
        return pltpu.make_async_remote_copy(
            src_ref=src, dst_ref=dst, send_sem=ss, recv_sem=rs,
            device_id={"chain": kk, "quad": qq}, device_id_type=MESH,
        )

    def in_copy(c):
        w = COLS // 4
        return pltpu.make_async_copy(
            sec.at[0, :, pl.ds(c * w, w)], ib.at[:, pl.ds(c * w, w)], sem_in.at[c]
        )

    for c in range(4):
        in_copy(c).start()
    consts = [
        pltpu.make_async_copy(cd_in, cd, sem_c.at[0]),
        pltpu.make_async_copy(rt_in, rt, sem_c.at[1]),
        pltpu.make_async_copy(sp_in, sp, sem_c.at[2]),
        pltpu.make_async_copy(mx_in, mx, sem_c.at[3]),
    ]
    for d in consts:
        d.start()
    anc_copies = [
        pltpu.make_async_copy(anc.at[pl.ds(0, HALF)], fb, sem_a.at[0]),
        pltpu.make_async_copy(anc.at[pl.ds(HALF, HALF)], ab, sem_a.at[1]),
    ]

    @pl.when(k == 0)
    def _():
        for d in anc_copies:
            d.start()

    barrier = pltpu.get_barrier_semaphore()

    def hello(kk, qq):
        pl.semaphore_signal(barrier, inc=1, device_id={"chain": kk, "quad": qq}, device_id_type=MESH)

    @pl.loop(1, NQ)
    def _(d):
        hello(k, lax.rem(s + d, NQ))

    @pl.loop(0, NQ)
    def _(q):
        @pl.when(has_next)
        def _():
            hello(k + 1, q)

        @pl.when(has_prev)
        def _():
            hello(k - 1, q)

    @pl.loop(0, NC)
    def _(kk):
        @pl.when((kk > k + 1) | (kk < k - 1))
        def _():
            hello(kk, s)

    one = jnp.int32(1)
    zero = jnp.int32(0)
    nn = jnp.where(has_next, one, zero)
    np_ = jnp.where(has_prev, one, zero)
    partners = (NQ - 1) + NQ * nn + NQ * np_ + (NC - 1) - nn - np_

    i32[:, :PAD] = jnp.zeros((ROWS + 16, PAD), F32)
    i32[:, PAD + COLS :] = jnp.zeros((ROWS + 16, PAD), F32)
    j32[:, :PAD] = jnp.zeros((HALF + 16, PAD), F32)
    j32[:, PAD + COLS :] = jnp.zeros((HALF + 16, PAD), F32)
    ub[:, :PAD] = jnp.zeros((32, PAD), F32)
    ub[:, PAD + COLS :] = jnp.zeros((32, PAD), F32)
    sums[...] = jnp.zeros_like(sums)
    dsums[...] = jnp.zeros_like(dsums)
    bdacc[...] = jnp.zeros_like(bdacc)
    cpad[...] = jnp.zeros_like(cpad)

    @pl.when(s == 0)
    def _():
        htop[...] = jnp.zeros_like(htop)

    @pl.when(s == NQ - 1)
    def _():
        hbot[...] = jnp.zeros_like(hbot)

    @pl.when(k == 0)
    def _():
        bdh[...] = jnp.zeros_like(bdh)
        cprev[...] = jnp.zeros_like(cprev)

    @pl.when(k == NC - 1)
    def _():
        jb[...] = jnp.zeros_like(jb)
        jmid[...] = jnp.zeros_like(jmid)
        jbot[...] = jnp.zeros_like(jbot)
        cnext[...] = jnp.zeros_like(cnext)

    for j in range(NC - 1):
        @pl.when(j >= k)
        def _():
            ew[j] = jnp.zeros((8, 128), F32)

    for c in range(4):
        in_copy(c).wait()

    @pl.loop(0, NCH)
    def _(c):
        at = pl.multiple_of(c * CH, CH)
        i32[8 : 8 + ROWS, pl.ds(at + PAD, CH)] = ib[:, pl.ds(at, CH)].astype(F32)

    etop[...] = i32[8:9, PAD : PAD + COLS]
    ebot[...] = i32[7 + ROWS : 8 + ROWS, PAD : PAD + COLS]
    emid[...] = i32[7 + HALF : 8 + HALF, PAD : PAD + COLS]

    pl.semaphore_wait(barrier, partners)

    up_top = remote(etop, hbot, s_h.at[0], r_h.at[0], k, jnp.maximum(s - 1, 0))
    down_bot = remote(ebot, htop, s_h.at[1], r_h.at[1], k, jnp.minimum(s + 1, NQ - 1))
    mid_prev = remote(emid, jmid, s_h.at[2], r_h.at[2], jnp.maximum(k - 1, 0), s)
    bot_prev = remote(hbot, jbot, s_h.at[3], r_h.at[3], jnp.maximum(k - 1, 0), s)

    @pl.when(s > 0)
    def _():
        up_top.start()

    @pl.when(s < NQ - 1)
    def _():
        down_bot.start()

    def f_copy(c):
        at = pl.multiple_of(c * CH, CH)
        return remote(
            ib.at[pl.ds(0, HALF), pl.ds(at, CH)], fb.at[:, pl.ds(at, CH)],
            s_f.at[c], r_f.at[c], jnp.minimum(k + 1, NC - 1), s,
        )

    def j_copy(c):
        at = pl.multiple_of(c * CH, CH)
        return remote(
            ib.at[pl.ds(HALF, HALF), pl.ds(at, CH)], jb.at[:, pl.ds(at, CH)],
            s_j.at[c], r_j.at[c], jnp.maximum(k - 1, 0), s,
        )

    @pl.when(has_prev)
    def _():
        mid_prev.start()

    @pl.loop(0, NCH)
    def _(c):
        @pl.when(has_next)
        def _():
            f_copy(c).start()

        @pl.when(has_prev)
        def _():
            j_copy(c).start()

    for d in consts:
        d.wait()
    lane = lax.broadcasted_iota(jnp.int32, (8, 128), 1)

    @pl.loop(0, NCH)
    def _(c):
        at = pl.multiple_of(c * CH, CH)
        v = cd[pl.ds(at, CH), :].astype(F32)
        ln = lax.broadcasted_iota(jnp.int32, (CH, 128), 1)
        j = jnp.where(ln < GRID, ln, ln - GRID)
        for h in range(2):
            lo_d, hi_d = 2 * h, 2 * h + 1
            a = v if lo_d == 0 else pltpu.roll(v, 128 - lo_d, 1)
            b = pltpu.roll(v, 128 - hi_d, 1)
            a = jnp.where(j < GRID - lo_d, a, 0.0)
            b = jnp.where(j < GRID - hi_d, b, 0.0)
            w1[pl.ds(at, CH), h * 128 : (h + 1) * 128] = (v * jnp.where(ln < GRID, a, b)).astype(BF16)

    @pl.when(s < NQ - 1)
    def _():
        up_top.wait_recv()

    @pl.when(s > 0)
    def _():
        down_bot.wait_recv()

    @pl.when(has_prev)
    def _():
        bot_prev.start()

    i32[7:8, PAD : PAD + COLS] = htop[...]
    i32[8 + ROWS : 9 + ROWS, PAD : PAD + COLS] = hbot[...]

    variant = jnp.where(s == 0, 0, jnp.where(s == NQ - 1, 2, 1))
    RB = 32

    @pl.loop(0, NCH)
    def _(c):
        at = pl.multiple_of(c * CH, CH)
        s1 = jnp.zeros((8, CH), F32)
        s2 = jnp.zeros((8, CH), F32)
        for r in range(0, ROWS, RB):
            mid = i32[8 + r : 8 + r + RB, pl.ds(at, CH + 2 * PAD)]
            x = mid[:, PAD : PAD + CH]
            right = pltpu.roll(mid, CH + 2 * PAD - 1, 1)[:, PAD : PAD + CH]
            left = pltpu.roll(mid, 1, 1)[:, PAD : PAD + CH]
            tall = i32[r : r + RB + 16, pl.ds(at + PAD, CH)]
            below = pltpu.roll(tall, RB + 15, 0)[8 : 8 + RB]
            above = pltpu.roll(tall, 1, 0)[8 : 8 + RB]
            lx = right - left
            ly = below - above
            lxb[r : r + RB, pl.ds(at, CH)] = lx
            lyb[r : r + RB, pl.ds(at, CH)] = ly
            qb[0, r : r + RB, :] = (lx * lx).astype(BF16)
            qb[1, r : r + RB, :] = (lx * ly).astype(BF16)
            qb[2, r : r + RB, :] = (ly * ly).astype(BF16)
            qb[3, r : r + RB, :] = (x * right).astype(BF16)
            qb[4, r : r + RB, :] = (x * below).astype(BF16)
            for t in range(0, RB, 8):
                xt = x[t : t + 8]
                s1 = s1 + xt
                s2 = s2 + xt * xt
        sums[0] = sums[0] + s1[:, :128] + s1[:, 128:]
        sums[1] = sums[1] + s2[:, :128] + s2[:, 128:]
        for i in range(3):
            tg[32 * i : 32 * i + 32, pl.ds(at, CH)] = jnp.dot(
                rt[variant, 0:32, :], qb[i], preferred_element_type=F32
            ).astype(BF16)
        u = jnp.dot(rt[variant, 32:64, :], ib[:, pl.ds(at, CH)], preferred_element_type=F32)
        z = jnp.dot(rt[variant, 32:48, :], qb[3], preferred_element_type=F32)
        q = jnp.dot(rt[variant, 64:80, :], qb[4], preferred_element_type=F32)
        ub[0:8, pl.ds(at + PAD, CH)] = u[0:8] + u[8:16]
        ub[8:16, pl.ds(at + PAD, CH)] = u[16:24] + u[24:32]
        ub[16:24, pl.ds(at + PAD, CH)] = z[0:8] + z[8:16]
        ub[24:32, pl.ds(at + PAD, CH)] = q[0:8] + q[8:16]

    g = jnp.dot(tg[...], w1[...], preferred_element_type=F32) * 0.25
    first = lane < GRID

    def swap(v):
        return pltpu.roll(v, GRID, 1)

    fslots = []
    bslots = []
    for di in range(4):
        for h in range(2):
            xx = g[8 * di : 8 * di + 8, 128 * h : 128 * h + 128]
            xy = g[32 + 8 * di : 40 + 8 * di, 128 * h : 128 * h + 128]
            yy = g[64 + 8 * di : 72 + 8 * di, 128 * h : 128 * h + 128]
            a0 = jnp.where(first, xx, swap(yy))
            a1 = jnp.where(first, swap(xx), yy)
            (fslots if di < 2 and h == 0 else bslots).extend([a0, a1, xy])
    for i in range(0, 18, 2):
        gbs[8 * i : 8 * i + 16, :] = jnp.concatenate([bslots[i], bslots[i + 1]], axis=0).astype(BF16)
    for i in range(6):
        gfs[8 * i : 8 * i + 8, :] = fslots[i]

    @pl.loop(0, NCH)
    def _(c):
        at = pl.multiple_of(c * CH, CH)
        wide = ub[:, pl.ds(at, CH + 2 * PAD)]
        right = pltpu.roll(wide, CH + 2 * PAD - 1, 1)[:, PAD : PAD + CH]
        left = pltpu.roll(wide, 1, 1)[:, PAD : PAD + CH]
        x = wide[:, PAD : PAD + CH]
        v = jnp.concatenate(
            [0.5 * (right[0:8] - left[0:8]), x[8:16], 0.5 * (x[16:24] - left[16:24]), x[24:32]], axis=0
        )
        hi = v.astype(BF16)
        lhs[0:32, pl.ds(at, CH)] = hi
        lhs[32:64, pl.ds(at, CH)] = (v - hi.astype(F32)).astype(BF16)

    bb = jnp.dot(lhs[...], cd[...], preferred_element_type=F32)
    bb = bb[0:32] + bb[32:64]
    gfs[48:56, :] = jnp.where(first, bb[16:24], bb[24:32])
    gfs[56:64, :] = jnp.where(first, bb[0:8], bb[8:16])

    def fold(a, b):
        sub = lax.broadcasted_iota(jnp.int32, (8, 128), 0)
        ra = jnp.sum(a, axis=0, keepdims=True)
        rb = jnp.sum(b, axis=0, keepdims=True)
        return jnp.where(sub == 0, ra, jnp.where(sub == 1, rb, 0.0))

    gfs[64:72, :] = fold(sums[0], sums[1])

    def gf_copy(to, slot):
        return remote(gfs, gf.at[slot], s_gf.at[to], r_gf.at[slot], k, to)

    def gb_copy(to, slot):
        return remote(gbs, gb.at[slot], s_gb.at[to], r_gb.at[slot], k, to)

    @pl.loop(1, NQ)
    def _(d):
        to = lax.rem(s + d, NQ)
        gf_copy(to, s).start()
        gb_copy(to, s).start()

    gf[s] = gfs[...]
    gb[s] = gbs[...]

    @pl.when(has_next)
    def _():
        mid_prev.wait_recv()
        bot_prev.wait_recv()

    j32[7:8, PAD : PAD + COLS] = jmid[...]
    j32[8 + HALF : 9 + HALF, PAD : PAD + COLS] = jbot[...]

    def arrive(c):
        @pl.when(has_prev)
        def _():
            f_copy(c).wait_recv()

        @pl.when(has_next)
        def _():
            j_copy(c).wait_recv()

        at = pl.multiple_of(c * CH, CH)
        j32[8 : 8 + HALF, pl.ds(at + PAD, CH)] = jb[:, pl.ds(at, CH)].astype(F32)

    def tally(i, d, x):
        a = jnp.zeros((8, CH), F32)
        b = jnp.zeros((8, CH), F32)
        for t in range(0, d.shape[0], 8):
            a = a + d[t : t + 8]
            b = b + d[t : t + 8] * x[t : t + 8]
        dsums[i] = dsums[i] + a[:, :128] + a[:, 128:]
        dsums[i + 1] = dsums[i + 1] + b[:, :128] + b[:, 128:]

    def contract(at, rows):
        v = jnp.concatenate([jnp.dot(sp[...], qd[i], preferred_element_type=F32) for i in range(2)], axis=0)
        v = jnp.concatenate(
            [v[0:8] + v[8:16], v[16:24] + v[24:32], v[32:40] + v[40:48], v[48:56] + v[56:64]], axis=0
        )
        hi = v.astype(BF16)
        lo = (v - hi.astype(F32)).astype(BF16)
        b = jnp.dot(jnp.concatenate([hi, lo], axis=0), cd[pl.ds(at, CH), :], preferred_element_type=F32)
        return b[0:32] + b[32:64]

    @pl.when(k == 0)
    def _():
        for d in anc_copies:
            d.wait()
        qd[...] = jnp.zeros_like(qd)

        @pl.loop(0, NCH)
        def _(c):
            at = pl.multiple_of(c * CH, CH)
            for r in range(0, HALF, RB):
                x = i32[8 + HALF + r : 8 + HALF + r + RB, pl.ds(at + PAD, CH)]
                d = ab[r : r + RB, pl.ds(at, CH)].astype(F32) - x
                qd[0, HALF + r : HALF + r + RB, :] = (d * lxb[HALF + r : HALF + r + RB, pl.ds(at, CH)]).astype(BF16)
                qd[1, HALF + r : HALF + r + RB, :] = (d * lyb[HALF + r : HALF + r + RB, pl.ds(at, CH)]).astype(BF16)
                tally(0, d, x)
            b = contract(at, 0)
            bdacc[0:8] = bdacc[0:8] + b[8:16]
            bdacc[16:24] = bdacc[16:24] + b[24:32]

    arrive(0)

    @pl.loop(0, NCH)
    def _(c):
        at = pl.multiple_of(c * CH, CH)

        @pl.when(c < NCH - 1)
        def _():
            arrive(c + 1)

        for r in range(0, HALF, RB):
            x = i32[8 + r : 8 + r + RB, pl.ds(at + PAD, CH)]
            d = fb[r : r + RB, pl.ds(at, CH)].astype(F32) - x
            qd[0, r : r + RB, :] = (d * lxb[r : r + RB, pl.ds(at, CH)]).astype(BF16)
            qd[1, r : r + RB, :] = (d * lyb[r : r + RB, pl.ds(at, CH)]).astype(BF16)
            tally(0, d, x)
            mid = j32[8 + r : 8 + r + RB, pl.ds(at, CH + 2 * PAD)]
            x = mid[:, PAD : PAD + CH]
            right = pltpu.roll(mid, CH + 2 * PAD - 1, 1)[:, PAD : PAD + CH]
            left = pltpu.roll(mid, 1, 1)[:, PAD : PAD + CH]
            tall = j32[r : r + RB + 16, pl.ds(at + PAD, CH)]
            below = pltpu.roll(tall, RB + 15, 0)[8 : 8 + RB]
            above = pltpu.roll(tall, 1, 0)[8 : 8 + RB]
            d = i32[8 + HALF + r : 8 + HALF + r + RB, pl.ds(at + PAD, CH)] - x
            qd[0, HALF + r : HALF + r + RB, :] = (d * (right - left)).astype(BF16)
            qd[1, HALF + r : HALF + r + RB, :] = (d * (below - above)).astype(BF16)
            tally(2, d, x)
        bdacc[...] = bdacc[...] + contract(at, 0)

    bds[0:8, :] = 0.5 * jnp.where(first, bdacc[0:8], bdacc[16:24])
    bhs[0:8, :] = 0.5 * jnp.where(first, bdacc[8:16], bdacc[24:32])
    bds[8:16, :] = fold(dsums[0], dsums[1])
    bhs[8:16, :] = fold(dsums[2], dsums[3])

    def bo_copy(to, slot):
        return remote(bds, bdo.at[slot], s_bo.at[to], r_bo.at[slot], k, to)

    def bh_copy(to, slot):
        return remote(bhs, bdh.at[slot], s_bh.at[to], r_bh.at[slot], jnp.minimum(k + 1, NC - 1), to)

    @pl.loop(0, NQ)
    def _(d):
        to = lax.rem(s + d, NQ)

        @pl.when(has_next)
        def _():
            bh_copy(to, s).start()

        @pl.when(d > 0)
        def _():
            bo_copy(to, s).start()

    bdo[s] = bds[...]

    @pl.loop(1, NQ)
    def _(d):
        p = lax.rem(s + d, NQ)
        gf_copy(p, p).wait_recv()
        gb_copy(p, p).wait_recv()

    row = lax.broadcasted_iota(jnp.int32, (GRID, 128), 0)
    wide_first = lax.broadcasted_iota(jnp.int32, (GRID, 128), 1) < GRID

    def merge(parts):
        even = jnp.concatenate(parts[0::2], axis=0)
        odd = jnp.concatenate(parts[1::2], axis=0)
        even = jnp.where(row < GRID - 2, pltpu.roll(even, GRID - 2, 0), 0.0)
        odd = jnp.where(row >= 2, pltpu.roll(odd, 2, 0), 0.0)
        return even + odd

    def place(di, h, which, v):
        if di:
            v = jnp.where(row < GRID - di, v, 0.0)
        if which < 2:
            ga[4 * di + 2 * h + which] = v
        else:
            o = swap(v)
            gx[4 * di + 2 * h] = jnp.where(wide_first, v, o)
            gx[4 * di + 2 * h + 1] = jnp.where(wide_first, o, v)

    fi = 0
    bi = 0
    for di in range(4):
        for h in range(2):
            for which in range(3):
                if di < 2 and h == 0:
                    v = merge([gf[p, 8 * fi : 8 * fi + 8, :] for p in range(NQ)])
                    fi += 1
                else:
                    o = 8 * (bi % 2)
                    b0 = 16 * (bi // 2)
                    v = merge([gb[p, b0 : b0 + 16, :].astype(F32)[o : o + 8] for p in range(NQ)])
                    bi += 1
                place(di, h, which, v)
    b_i = merge([gf[p, 48:56, :] for p in range(NQ)])
    b_1 = merge([gf[p, 56:64, :] for p in range(NQ)])

    def total(v):
        return jnp.sum(v, axis=(0, 1), keepdims=True)

    tot = gf[0, 64:72, :]
    for p in range(1, NQ):
        tot = tot + gf[p, 64:72, :]
    sum_i = total(tot[0:1])
    sum_ii = total(tot[1:2])

    @pl.loop(0, NQ)
    def _(p):
        @pl.when(p != s)
        def _():
            bo_copy(p, p).wait_recv()

        @pl.when(has_prev)
        def _():
            bh_copy(p, p).wait_recv()

    b_f = b_i + merge([bdo[p, 0:8, :] + bdh[p, 0:8, :] for p in range(NQ)])
    tot = bdo[0, 8:16, :] + bdh[0, 8:16, :]
    for p in range(1, NQ):
        tot = tot + bdo[p, 8:16, :] + bdh[p, 8:16, :]
    sum_f = sum_i + total(tot[0:1])
    sum_fi = sum_ii + total(tot[1:2])
    mean_f = sum_f * (1.0 / PIXELS)

    def apply_gram(c):
        cl = [c] + [pltpu.roll(c, 128 - d, 1) for d in range(1, 4)]
        cs = swap(c)
        csl = [cs] + [pltpu.roll(cs, 128 - d, 1) for d in range(1, 4)]
        out = None
        lacc = [None] * 4

        def add(a, b):
            return b if a is None else a + b

        for di in range(4):
            racc = None
            for dj in range(4):
                a = ga[4 * di + dj]
                x = gx[4 * di + dj]
                up = (lambda v: v) if di == 0 else (lambda v: pltpu.roll(v, GRID - di, 0))
                out = add(out, a * up(cl[dj]) + x * up(csl[dj]))
                if dj:
                    lacc[dj] = add(lacc[dj], a * up(c) + x * up(cs))
                if di:
                    racc = add(racc, a * cl[dj] + x * csl[dj])
                if di and dj:
                    racc = racc + pltpu.roll(a * c + x * cs, dj, 1)
            if di:
                out = out + pltpu.roll(racc, di, 0)
        for dj in range(1, 4):
            out = out + pltpu.roll(lacc[dj], dj, 1)
        return out

    def direction(c):
        if c is None:
            mean_w = sum_i * (1.0 / PIXELS)
            sq = sum_ii
            cross = sum_fi
            b_w = b_i
        else:
            h = apply_gram(c)
            mean_w = (sum_i + total(c * b_1)) * (1.0 / PIXELS)
            sq = sum_ii + total(c * (2.0 * b_i + h))
            cross = sum_fi + total(c * b_f)
            b_w = b_i + h
        var = sq - PIXELS * mean_w * mean_w
        cov = cross - PIXELS * mean_f * mean_w
        den = jnp.sqrt(var + EPS)
        ratio = cov / den / (var + EPS)
        grad = PIXELS * ((b_f - mean_f * b_1) / den - ratio * (b_w - mean_w * b_1))
        mag = total(grad * grad) * (1.0 / (GRID * 2 * GRID))
        return grad / jnp.sqrt(mag + EPS)

    rate = 1.0 / ITERATIONS

    def cp_copy(i):
        return remote(csend.at[i], cprev.at[i], s_cp.at[i], r_cp.at[i], jnp.minimum(k + 1, NC - 1), s)

    def cn_copy(i):
        return remote(csend.at[i], cnext.at[i], s_cn.at[i], r_cn.at[i], jnp.maximum(k - 1, 0), s)

    def exchange(i, c):
        csend[i] = c

        @pl.when(has_next)
        def _():
            cp_copy(i).start()

        @pl.when(has_prev)
        def _():
            cn_copy(i).start()

    def receive(i):
        @pl.when(has_prev)
        def _():
            cp_copy(i).wait_recv()

        @pl.when(has_next)
        def _():
            cn_copy(i).wait_recv()

    c = rate * direction(None)
    exchange(0, c)
    for i in range(1, ITERATIONS - 1):
        step = c + rate * direction(c)
        receive(i - 1)
        c = step + SMOOTHING * (cprev[i - 1] - 2.0 * c + cnext[i - 1])
        exchange(i, c)
    step = c + rate * direction(c)

    base = pl.multiple_of(lax.div(4 * s + 6, 8) * 8, 8)
    even = lax.rem(s, 2) == 0

    def window(v):
        cpad[8 : 8 + GRID] = v
        w = cpad[pl.ds(base, 16), :]
        return jnp.where(even, w[6:14], w[2:10])

    cw = window(c)
    mine = window(step) - jnp.where(k == 0, SMOOTHING, 0.0) * cw
    ew_s[...] = mine

    def ew_copy(to, slot):
        return remote(ew_s, ew.at[slot], s_ew.at[to], r_ew.at[slot], to, s)

    for kk in range(1, NC):
        @pl.when(kk > k)
        def _():
            ew_copy(kk, k).start()

    receive(ITERATIONS - 2)
    nxt = window(cnext[ITERATIONS - 2])
    own = mine + SMOOTHING * (nxt - cw)

    for kk in range(NC - 1):
        @pl.when(kk < k)
        def _():
            ew_copy(kk, kk).wait_recv()

    t = ew[0]
    for kk in range(1, NC - 1):
        t = t + ew[kk]
    t = t + own
    tw_s[...] = t

    def tw_copy(to, slot):
        return remote(tw_s, tw.at[slot], s_tw.at[to], r_tw.at[slot], k, to)

    @pl.loop(1, NQ)
    def _(d):
        tw_copy(lax.rem(s + d, NQ), s).start()

    tw[s] = t

    hi = t.astype(BF16)
    rest = t - hi.astype(F32)
    mid = rest.astype(BF16)
    low = (rest - mid.astype(F32)).astype(BF16)
    stack = jnp.concatenate(
        [v.astype(F32) for v in (hi, mid, low, hi, mid, hi)] + [jnp.zeros((80, 128), F32)], axis=0
    ).astype(BF16)
    mixed = jnp.dot(mx[...], stack, preferred_element_type=F32).astype(BF16).astype(F32) * 0.5
    big_first = lax.broadcasted_iota(jnp.int32, (ROWS, 128), 1) < GRID
    mixed_x = jnp.where(big_first, mixed, 0.0).astype(BF16)
    mixed_y = jnp.where(big_first, 0.0, mixed).astype(BF16)
    dims = (((1,), (1,)), ((), ()))

    @pl.loop(0, NCH)
    def _(c):
        at = pl.multiple_of(c * CH, CH)
        table = cd[pl.ds(at, CH), :]
        sx = lax.dot_general(mixed_x, table, dims, preferred_element_type=F32)
        sy = lax.dot_general(mixed_y, table, dims, preferred_element_type=F32)
        v = (
            i32[8 : 8 + ROWS, pl.ds(at + PAD, CH)]
            + sx * lxb[:, pl.ds(at, CH)]
            + sy * lyb[:, pl.ds(at, CH)]
        )
        reg[0, :, pl.ds(at, CH)] = v.astype(BF16)

    @pl.loop(1, NQ)
    def _(d):
        p = lax.rem(s + d, NQ)
        tw_copy(p, p).wait_recv()

    for m in range(8):
        acc[0, 8 * m : 8 * m + 8, :] = jnp.concatenate([tw[2 * m, 2:6, :], tw[2 * m + 1, 2:6, :]], axis=0)

    @pl.when(s > 0)
    def _():
        up_top.wait_send()

    @pl.when(s < NQ - 1)
    def _():
        down_bot.wait_send()

    @pl.when(has_prev)
    def _():
        mid_prev.wait_send()
        bot_prev.wait_send()

    @pl.loop(0, NCH)
    def _(c):
        @pl.when(has_next)
        def _():
            f_copy(c).wait_send()

        @pl.when(has_prev)
        def _():
            j_copy(c).wait_send()

    @pl.loop(0, NQ)
    def _(d):
        to = lax.rem(s + d, NQ)

        @pl.when(has_next)
        def _():
            bh_copy(to, s).wait_send()

        @pl.when(d > 0)
        def _():
            gf_copy(to, s).wait_send()
            gb_copy(to, s).wait_send()
            bo_copy(to, s).wait_send()
            tw_copy(to, s).wait_send()

    for i in range(ITERATIONS - 1):
        @pl.when(has_next)
        def _():
            cp_copy(i).wait_send()

        @pl.when(has_prev)
        def _():
            cn_copy(i).wait_send()

    for kk in range(1, NC):
        @pl.when(kk > k)
        def _():
            ew_copy(kk, k).wait_send()


def solution(mesh):
    c, rows, split, mix = tables()

    def body(sections, anchor):
        v = pltpu.VMEM
        dma = pltpu.SemaphoreType.DMA
        row = v((1, COLS), F32)
        win = v((NQ, 16, 128), F32)
        scratch = [
            v((ROWS, COLS), BF16), v((HALF, COLS), BF16), v((HALF, COLS), BF16), v((HALF, COLS), BF16),
            v((ROWS + 16, COLS + 2 * PAD), F32), v((HALF + 16, COLS + 2 * PAD), F32),
            v((ROWS, COLS), F32), v((ROWS, COLS), F32),
            v((COLS, 128), BF16), v((COLS, 256), BF16),
            v((3, 80, ROWS), BF16), v((32, ROWS), BF16), v((ROWS, 128), BF16),
            v((5, ROWS, CH), BF16), v((2, ROWS, CH), BF16), v((96, COLS), BF16),
            v((32, COLS + 2 * PAD), F32), v((64, COLS), BF16), v((32, 128), F32),
            v((2, 8, 128), F32), v((4, 8, 128), F32),
            row, row, row, row, row, row, row,
            v((72, 128), F32), v((144, 128), BF16), v((NQ, 72, 128), F32), v((NQ, 144, 128), BF16),
            v((16, GRID, 128), F32), v((16, GRID, 128), F32),
            v((16, 128), F32), v((16, 128), F32), win, win,
            v((GRID + 16, 128), F32), v((3, GRID, 128), F32), v((3, GRID, 128), F32), v((3, GRID, 128), F32),
            v((8, 128), F32), v((NC - 1, 8, 128), F32), v((8, 128), F32), v((NQ, 8, 128), F32),
            dma((4,)), dma((4,)), dma((2,)),
            dma((NCH,)), dma((NCH,)), dma((NCH,)), dma((NCH,)), dma((4,)), dma((4,)),
            dma((NQ,)), dma((NQ,)), dma((NQ,)), dma((NQ,)),
            dma((NQ,)), dma((NQ,)), dma((NQ,)), dma((NQ,)),
            dma((3,)), dma((3,)), dma((3,)), dma((3,)), dma((NC,)), dma((NC,)), dma((NQ,)), dma((NQ,)),
        ]
        anywhere = pl.BlockSpec(memory_space=pl.ANY)
        inside = pl.BlockSpec(memory_space=pltpu.VMEM)
        return pl.pallas_call(
            kernel,
            out_shape=(
                jax.ShapeDtypeStruct((1, ROWS, COLS), BF16),
                jax.ShapeDtypeStruct((1, GRID, 2 * GRID), F32),
            ),
            in_specs=[anywhere] * 6,
            out_specs=(inside, inside),
            scratch_shapes=scratch,
            compiler_params=pltpu.CompilerParams(
                collective_id=0, has_side_effects=True, vmem_limit_bytes=60 * 1024 * 1024
            ),
        )(
            sections, anchor,
            jnp.asarray(c, BF16), jnp.asarray(rows, BF16), jnp.asarray(split, BF16), jnp.asarray(mix, BF16),
        )

    return jax.shard_map(
        body, mesh=mesh,
        in_specs=(P("chain", "quad", None), P("quad", None)),
        out_specs=(P("chain", "quad", None), P("chain", None, None)),
        check_vma=False,
    )
```

```python
import numpy as np
import jax
import jax.numpy as jnp
from jax import lax
from jax.experimental import pallas as pl
from jax.experimental.pallas import tpu as pltpu
from jax.sharding import PartitionSpec as P

GRID = 64
ITERATIONS = 4
EPS = 1e-6
SMOOTHING = 0.25
MESH = pl.DeviceIdType.MESH
F32 = jnp.float32
BF16 = jnp.bfloat16

ROWS = 256
COLS = 4096
HALF = 128
CH = 256
NCH = COLS // CH
CX = 512
NX = COLS // CX
PAD = 128
NC = 8
NQ = 16
PIXELS = float(4096 * 4096)


def weight(offset):
    d = np.abs(offset)
    near = 2.0 / 3.0 - d * d + 0.5 * d * d * d
    r = 2.0 - d
    far = r * r * r / 6.0
    return np.where(d < 1.0, near, np.where(d < 2.0, far, 0.0 * d)).astype(np.float32)


def bf(x):
    return np.asarray(jnp.asarray(x, jnp.float32).astype(BF16).astype(jnp.float32))


def hi_lo(x):
    hi = bf(x)
    return [hi, bf(x - hi)]


def tables():
    f = np.float32
    x = np.arange(COLS, dtype=f)
    c = weight((x[:, None] + f(0.5)) / f(64) - np.arange(GRID, dtype=f)[None, :] - f(0.5))
    c = np.concatenate([c, c], axis=1)
    y = np.arange(-1, ROWS + 1, dtype=f)
    ext = weight((y[:, None] + f(0.5)) / f(64) - (np.arange(8, dtype=f) - f(2))[None, :] - f(0.5)).T
    r = ext[:, 1:-1]
    pairs = np.zeros((4, 8, ROWS), f)
    for d in range(4):
        pairs[d, : 8 - d] = r[: 8 - d] * r[d:]
    step = 0.5 * (r - ext[:, 2:])
    rows = []
    for variant in range(3):
        e = ext.copy()
        if variant == 0:
            e[:, 0] = 0.0
        if variant == 2:
            e[:, -1] = 0.0
        slope = 0.5 * (e[:, :-2] - e[:, 2:])
        rows.append(np.concatenate([pairs.reshape(32, ROWS)] + hi_lo(r) + hi_lo(slope) + hi_lo(step), axis=0))
    top = (np.arange(ROWS) < HALF).astype(f)[None]
    split = np.concatenate([h * top for h in hi_lo(r)] + [h * (1 - top) for h in hi_lo(r)], axis=0)
    hi = bf(r)
    mid = bf(r - hi)
    low = bf(r - hi - mid)
    mix = np.concatenate([hi, hi, hi, mid, mid, low, np.zeros((80, ROWS), f)], axis=0).T
    return c, np.stack(rows), split, mix


def kernel(
    sec, anc, cd_in, rt_in, sp_in, mx_in,
    reg, acc,
    ib, fb, jb, ab, i32, j32, lxb, lyb, cd, w1, rt, sp, mx,
    qb, tb, gacc, qd, vb, ub, lhs, bdacc, sums, dsums,
    etop, ebot, emid, htop, hbot, jmid, jbot,
    gs, gn, gp, gall, ga, gx, bms, bm, bds, bhs, bdo, bdh,
    cpad, csend, cprev, cnext, ew_s, ew, tw_s, tw,
    sem_in, sem_c, sem_a, rounds,
    s_f, r_f, s_j, r_j, s_h, r_h, s_n, r_n, s_g, r_g, s_bm, r_bm,
    s_bo, r_bo, s_bh, r_bh, s_cp, r_cp, s_cn, r_cn, s_ew, r_ew, s_tw, r_tw,
):
    k = lax.axis_index("chain")
    s = lax.axis_index("quad")
    has_prev = k > 0
    has_next = k < NC - 1

    def remote(src, dst, ss, rs, kk, qq):
        return pltpu.make_async_remote_copy(
            src_ref=src, dst_ref=dst, send_sem=ss, recv_sem=rs,
            device_id={"chain": kk, "quad": qq}, device_id_type=MESH,
        )

    def in_copy(c):
        w = COLS // 4
        return pltpu.make_async_copy(
            sec.at[0, :, pl.ds(c * w, w)], ib.at[:, pl.ds(c * w, w)], sem_in.at[c]
        )

    for c in range(4):
        in_copy(c).start()
    consts = [
        pltpu.make_async_copy(cd_in, cd, sem_c.at[0]),
        pltpu.make_async_copy(rt_in, rt, sem_c.at[1]),
        pltpu.make_async_copy(sp_in, sp, sem_c.at[2]),
        pltpu.make_async_copy(mx_in, mx, sem_c.at[3]),
    ]
    for d in consts:
        d.start()
    anc_copies = [
        pltpu.make_async_copy(anc.at[pl.ds(0, HALF)], fb, sem_a.at[0]),
        pltpu.make_async_copy(anc.at[pl.ds(HALF, HALF)], ab, sem_a.at[1]),
    ]

    @pl.when(k == 0)
    def _():
        for d in anc_copies:
            d.start()

    barrier = pltpu.get_barrier_semaphore()

    def hello(sem, step):
        for sign in (1, -1):
            kk = k + sign * step
            pl.semaphore_signal(
                sem, inc=1, device_id={"chain": k, "quad": lax.rem(s + sign * step + NQ, NQ)}, device_id_type=MESH
            )

            @pl.when((kk >= 0) & (kk < NC))
            def _():
                pl.semaphore_signal(sem, inc=1, device_id={"chain": kk, "quad": s}, device_id_type=MESH)

    def heard(sem, step):
        one = jnp.int32(1)
        zero = jnp.int32(0)
        pl.semaphore_wait(
            sem, 2 + jnp.where(k >= step, one, zero) + jnp.where(k + step < NC, one, zero)
        )

    hello(barrier, 1)

    i32[:, :PAD] = jnp.zeros((ROWS + 16, PAD), F32)
    i32[:, PAD + COLS :] = jnp.zeros((ROWS + 16, PAD), F32)
    j32[:, :PAD] = jnp.zeros((HALF + 16, PAD), F32)
    j32[:, PAD + COLS :] = jnp.zeros((HALF + 16, PAD), F32)
    ub[:, :PAD] = jnp.zeros((32, PAD), F32)
    ub[:, PAD + COLS :] = jnp.zeros((32, PAD), F32)
    sums[...] = jnp.zeros_like(sums)
    qb[1] = jnp.zeros((5, ROWS, CH), BF16)
    tb[0] = jnp.zeros((96, CH), BF16)
    gacc[...] = jnp.zeros_like(gacc)
    qd[...] = jnp.zeros_like(qd)
    vb[...] = jnp.zeros_like(vb)
    dsums[...] = jnp.zeros_like(dsums)
    bdacc[...] = jnp.zeros_like(bdacc)
    cpad[...] = jnp.zeros_like(cpad)

    @pl.when(s == 0)
    def _():
        htop[...] = jnp.zeros_like(htop)
        gn[0] = jnp.zeros((96, 128), F32)

    @pl.when(s == NQ - 1)
    def _():
        hbot[...] = jnp.zeros_like(hbot)
        gn[1] = jnp.zeros((96, 128), F32)

    @pl.when(k == 0)
    def _():
        bdh[...] = jnp.zeros_like(bdh)
        cprev[...] = jnp.zeros_like(cprev)

    @pl.when(k == NC - 1)
    def _():
        jb[...] = jnp.zeros_like(jb)
        jmid[...] = jnp.zeros_like(jmid)
        jbot[...] = jnp.zeros_like(jbot)
        cnext[...] = jnp.zeros_like(cnext)

    for j in range(NC - 1):
        @pl.when(j >= k)
        def _():
            ew[j] = jnp.zeros((8, 128), F32)

    heard(barrier, 1)
    hello(rounds.at[0], 1)

    def f_copy(c):
        at = pl.multiple_of(c * CX, CX)
        return remote(
            sec.at[0, pl.ds(0, HALF), pl.ds(at, CX)], fb.at[:, pl.ds(at, CX)],
            s_f, r_f.at[c], jnp.minimum(k + 1, NC - 1), s,
        )

    def j_copy(c):
        at = pl.multiple_of(c * CX, CX)
        return remote(
            sec.at[0, pl.ds(HALF, HALF), pl.ds(at, CX)], jb.at[:, pl.ds(at, CX)],
            s_j, r_j.at[c], jnp.maximum(k - 1, 0), s,
        )

    @pl.loop(0, NX)
    def _(c):
        @pl.when(has_next)
        def _():
            f_copy(c).start()

        @pl.when(has_prev)
        def _():
            j_copy(c).start()

    up_top = remote(etop, hbot, s_h.at[0], r_h.at[0], k, jnp.maximum(s - 1, 0))
    down_bot = remote(ebot, htop, s_h.at[1], r_h.at[1], k, jnp.minimum(s + 1, NQ - 1))
    mid_prev = remote(emid, jmid, s_h.at[2], r_h.at[2], jnp.maximum(k - 1, 0), s)
    bot_prev = remote(hbot, jbot, s_h.at[3], r_h.at[3], jnp.maximum(k - 1, 0), s)

    for c in range(4):
        in_copy(c).wait()
    etop[...] = ib[0:16, :].astype(F32)[0:1]
    ebot[...] = ib[ROWS - 16 : ROWS, :].astype(F32)[15:16]
    emid[...] = ib[HALF - 16 : HALF, :].astype(F32)[15:16]

    @pl.when(s > 0)
    def _():
        up_top.start()

    @pl.when(s < NQ - 1)
    def _():
        down_bot.start()

    @pl.when(has_prev)
    def _():
        mid_prev.start()

    @pl.loop(0, NCH)
    def _(c):
        at = pl.multiple_of(c * CH, CH)
        i32[8 : 8 + ROWS, pl.ds(at + PAD, CH)] = ib[:, pl.ds(at, CH)].astype(F32)

    for d in consts:
        d.wait()
    lane = lax.broadcasted_iota(jnp.int32, (8, 128), 1)

    @pl.loop(0, NCH)
    def _(c):
        at = pl.multiple_of(c * CH, CH)
        v = cd[pl.ds(at, CH), :].astype(F32)
        ln = lax.broadcasted_iota(jnp.int32, (CH, 128), 1)
        j = jnp.where(ln < GRID, ln, ln - GRID)
        for h in range(2):
            lo_d, hi_d = 2 * h, 2 * h + 1
            a = v if lo_d == 0 else pltpu.roll(v, 128 - lo_d, 1)
            b = pltpu.roll(v, 128 - hi_d, 1)
            a = jnp.where(j < GRID - lo_d, a, 0.0)
            b = jnp.where(j < GRID - hi_d, b, 0.0)
            w1[pl.ds(at, CH), h * 128 : (h + 1) * 128] = (v * jnp.where(ln < GRID, a, b)).astype(BF16)

    @pl.when(s < NQ - 1)
    def _():
        up_top.wait_recv()

    @pl.when(s > 0)
    def _():
        down_bot.wait_recv()

    @pl.when(has_prev)
    def _():
        bot_prev.start()

    i32[7:8, PAD : PAD + COLS] = htop[...]
    i32[8 + ROWS : 9 + ROWS, PAD : PAD + COLS] = hbot[...]

    variant = jnp.where(s == 0, 0, jnp.where(s == NQ - 1, 2, 1))
    RB = 32

    def pixels(at, slot):
        s1 = jnp.zeros((8, CH), F32)
        s2 = jnp.zeros((8, CH), F32)
        for r in range(0, ROWS, RB):
            mid = i32[8 + r : 8 + r + RB, pl.ds(at, CH + 2 * PAD)]
            x = mid[:, PAD : PAD + CH]
            right = pltpu.roll(mid, CH + 2 * PAD - 1, 1)[:, PAD : PAD + CH]
            left = pltpu.roll(mid, 1, 1)[:, PAD : PAD + CH]
            tall = i32[r : r + RB + 16, pl.ds(at + PAD, CH)]
            below = pltpu.roll(tall, RB + 15, 0)[8 : 8 + RB]
            above = pltpu.roll(tall, 1, 0)[8 : 8 + RB]
            lx = right - left
            ly = below - above
            lxb[r : r + RB, pl.ds(at, CH)] = lx
            lyb[r : r + RB, pl.ds(at, CH)] = ly
            qb[slot, 0, r : r + RB, :] = (lx * lx).astype(BF16)
            qb[slot, 1, r : r + RB, :] = (lx * ly).astype(BF16)
            qb[slot, 2, r : r + RB, :] = (ly * ly).astype(BF16)
            qb[slot, 3, r : r + RB, :] = (x * right).astype(BF16)
            qb[slot, 4, r : r + RB, :] = (x * below).astype(BF16)
            for t in range(0, RB, 8):
                xt = x[t : t + 8]
                s1 = s1 + xt
                s2 = s2 + xt * xt
        sums[0] = sums[0] + s1[:, :128] + s1[:, 128:]
        sums[1] = sums[1] + s2[:, :128] + s2[:, 128:]

    def rows_out(at, slot):
        for i in range(3):
            tb[slot, 32 * i : 32 * i + 32, :] = jnp.dot(
                rt[variant, 0:32, :], qb[slot, i], preferred_element_type=F32
            ).astype(BF16)
        u = jnp.dot(rt[variant, 32:64, :], ib[:, pl.ds(at, CH)], preferred_element_type=F32)
        z = jnp.dot(rt[variant, 32:48, :], qb[slot, 3], preferred_element_type=F32)
        q = jnp.dot(rt[variant, 64:80, :], qb[slot, 4], preferred_element_type=F32)
        ub[0:8, pl.ds(at + PAD, CH)] = u[0:8] + u[8:16]
        ub[8:16, pl.ds(at + PAD, CH)] = u[16:24] + u[24:32]
        ub[16:24, pl.ds(at + PAD, CH)] = z[0:8] + z[8:16]
        ub[24:32, pl.ds(at + PAD, CH)] = q[0:8] + q[8:16]

    def columns_out(at, slot):
        gacc[...] = gacc[...] + jnp.dot(tb[slot], w1[pl.ds(at, CH), :], preferred_element_type=F32)

    def spot(c):
        return pl.multiple_of(jnp.maximum(c, 0) * CH, CH)

    @pl.loop(0, NCH // 2)
    def _(p):
        @pl.when(p == 1)
        def _():
            heard(rounds.at[0], 1)
            hello(rounds.at[1], 2)

        @pl.when(p == 4)
        def _():
            heard(rounds.at[1], 2)
            hello(rounds.at[2], 4)

        @pl.when(p == 7)
        def _():
            heard(rounds.at[2], 4)
            hello(rounds.at[3], 1)

        for u in range(2):
            c = 2 * p + u
            columns_out(spot(c - 2), u)
            pixels(spot(c), u)
            rows_out(spot(c - 1), 1 - u)

    columns_out(spot(NCH - 2), 0)
    rows_out(spot(NCH - 1), 1)
    columns_out(spot(NCH - 1), 1)

    first = lane < GRID

    def swap(v):
        return pltpu.roll(v, GRID, 1)

    quarter = lax.broadcasted_iota(jnp.int32, (8, 128), 0)

    def pack(a, b):
        return jnp.where(quarter < 4, pltpu.roll(a, 6, 0), pltpu.roll(b, 2, 0))

    slots = []
    for di in range(4):
        for h in range(2):
            part = lambda q: 0.25 * gacc[32 * q + 8 * di : 32 * q + 8 * di + 8, 128 * h : 128 * h + 128]
            xx, xy, yy = part(0), part(1), part(2)
            slots.append(jnp.where(first, xx, swap(yy)))
            slots.append(jnp.where(first, swap(xx), yy))
            slots.append(xy)
    for i in range(12):
        a, b = slots[2 * i], slots[2 * i + 1]
        gs[8 * i : 8 * i + 8, :] = pack(a, b)
        gp[8 * i : 8 * i + 8, :] = pack(pltpu.roll(a, 4, 0), pltpu.roll(b, 4, 0))

    to_next = remote(gp, gn.at[0], s_n.at[0], r_n.at[0], k, jnp.minimum(s + 1, NQ - 1))
    to_prev = remote(gp, gn.at[1], s_n.at[1], r_n.at[1], k, jnp.maximum(s - 1, 0))

    @pl.when(s < NQ - 1)
    def _():
        to_next.start()

    @pl.when(s > 0)
    def _():
        to_prev.start()

    @pl.loop(0, NCH)
    def _(c):
        at = pl.multiple_of(c * CH, CH)
        wide = ub[:, pl.ds(at, CH + 2 * PAD)]
        right = pltpu.roll(wide, CH + 2 * PAD - 1, 1)[:, PAD : PAD + CH]
        left = pltpu.roll(wide, 1, 1)[:, PAD : PAD + CH]
        x = wide[:, PAD : PAD + CH]
        v = jnp.concatenate(
            [0.5 * (right[0:8] - left[0:8]), x[8:16], 0.5 * (x[16:24] - left[16:24]), x[24:32]], axis=0
        )
        hi = v.astype(BF16)
        lhs[0:32, pl.ds(at, CH)] = hi
        lhs[32:64, pl.ds(at, CH)] = (v - hi.astype(F32)).astype(BF16)

    bb = jnp.dot(lhs[...], cd[...], preferred_element_type=F32)
    bb = bb[0:32] + bb[32:64]
    bms[0:8, :] = jnp.where(first, bb[16:24], bb[24:32])
    bms[8:16, :] = jnp.where(first, bb[0:8], bb[8:16])

    def fold(a, b):
        ra = jnp.sum(a, axis=0, keepdims=True)
        rb = jnp.sum(b, axis=0, keepdims=True)
        return jnp.where(quarter == 0, ra, jnp.where(quarter == 1, rb, 0.0))

    bms[16:24, :] = fold(sums[0], sums[1])
    bm[s] = bms[...]

    @pl.when(s > 0)
    def _():
        to_next.wait_recv()

    @pl.when(s < NQ - 1)
    def _():
        to_prev.wait_recv()

    for i in range(12):
        b8 = slice(8 * i, 8 * i + 8)
        g = gs[b8, :] + jnp.where((quarter == 0) | (quarter == 1) | (quarter == 4) | (quarter == 5), gn[0, b8, :], gn[1, b8, :])
        gs[b8, :] = g
        gall[s, b8, :] = g

    def g_copy(to, slot):
        return remote(gs, gall.at[slot], s_g, r_g, k, to)

    def bm_copy(to, slot):
        return remote(bms, bm.at[slot], s_bm, r_bm, k, to)

    @pl.loop(1, NQ)
    def _(d):
        to = lax.rem(s + d, NQ)
        bm_copy(to, s).start()
        g_copy(to, s).start()

    heard(rounds.at[3], 1)

    @pl.when(has_next)
    def _():
        mid_prev.wait_recv()
        bot_prev.wait_recv()

    j32[7:8, PAD : PAD + COLS] = jmid[...]
    j32[8 + HALF : 9 + HALF, PAD : PAD + COLS] = jbot[...]

    def tally(i, d, x):
        a = jnp.zeros((8, CH), F32)
        b = jnp.zeros((8, CH), F32)
        for t in range(0, d.shape[0], 8):
            a = a + d[t : t + 8]
            b = b + d[t : t + 8] * x[t : t + 8]
        dsums[i] = dsums[i] + a[:, :128] + a[:, 128:]
        dsums[i + 1] = dsums[i + 1] + b[:, :128] + b[:, 128:]

    def cross_rows(slot):
        v = jnp.concatenate(
            [jnp.dot(sp[...], qd[slot, i], preferred_element_type=F32) for i in range(2)], axis=0
        )
        v = jnp.concatenate(
            [v[0:8] + v[8:16], v[16:24] + v[24:32], v[32:40] + v[40:48], v[48:56] + v[56:64]], axis=0
        )
        hi = v.astype(BF16)
        vb[slot, 0:32, :] = hi
        vb[slot, 32:64, :] = (v - hi.astype(F32)).astype(BF16)

    def cross_columns(at, slot):
        b = jnp.dot(vb[slot], cd[pl.ds(at, CH), :], preferred_element_type=F32)
        bdacc[...] = bdacc[...] + b[0:32] + b[32:64]

    def lower(at, slot):
        for r in range(0, HALF, RB):
            rr = HALF + r
            x = i32[8 + rr : 8 + rr + RB, pl.ds(at + PAD, CH)]
            d = ab[r : r + RB, pl.ds(at, CH)].astype(F32) - x
            qd[slot, 0, rr : rr + RB, :] = (d * lxb[rr : rr + RB, pl.ds(at, CH)]).astype(BF16)
            qd[slot, 1, rr : rr + RB, :] = (d * lyb[rr : rr + RB, pl.ds(at, CH)]).astype(BF16)
            tally(0, d, x)

    def both(at, slot):
        for r in range(0, HALF, RB):
            x = i32[8 + r : 8 + r + RB, pl.ds(at + PAD, CH)]
            d = fb[r : r + RB, pl.ds(at, CH)].astype(F32) - x
            qd[slot, 0, r : r + RB, :] = (d * lxb[r : r + RB, pl.ds(at, CH)]).astype(BF16)
            qd[slot, 1, r : r + RB, :] = (d * lyb[r : r + RB, pl.ds(at, CH)]).astype(BF16)
            tally(0, d, x)
            rr = HALF + r
            mid = j32[8 + r : 8 + r + RB, pl.ds(at, CH + 2 * PAD)]
            x = mid[:, PAD : PAD + CH]
            right = pltpu.roll(mid, CH + 2 * PAD - 1, 1)[:, PAD : PAD + CH]
            left = pltpu.roll(mid, 1, 1)[:, PAD : PAD + CH]
            tall = j32[r : r + RB + 16, pl.ds(at + PAD, CH)]
            below = pltpu.roll(tall, RB + 15, 0)[8 : 8 + RB]
            above = pltpu.roll(tall, 1, 0)[8 : 8 + RB]
            d = i32[8 + rr : 8 + rr + RB, pl.ds(at + PAD, CH)] - x
            qd[slot, 0, rr : rr + RB, :] = (d * (right - left)).astype(BF16)
            qd[slot, 1, rr : rr + RB, :] = (d * (below - above)).astype(BF16)
            tally(2, d, x)

    def cross(work, ahead):
        @pl.loop(0, NCH // 2)
        def _(p):
            for u in range(2):
                c = 2 * p + u
                if ahead is not None:
                    ahead(c + 1)
                cross_columns(spot(c - 2), u)
                work(spot(c), u)
                cross_rows(1 - u)

        cross_columns(spot(NCH - 2), 0)
        cross_rows(1)
        cross_columns(spot(NCH - 1), 1)

    @pl.when(k == 0)
    def _():
        for d in anc_copies:
            d.wait()
        cross(lower, None)
        bdacc[0:8] = bdacc[8:16]
        bdacc[16:24] = bdacc[24:32]
        bdacc[8:16] = jnp.zeros((8, 128), F32)
        bdacc[24:32] = jnp.zeros((8, 128), F32)
        qd[1] = jnp.zeros((2, ROWS, CH), BF16)
        vb[...] = jnp.zeros_like(vb)

    def arrive(c):
        whole = lax.rem(c, CX // CH) == 0
        piece = lax.div(c, CX // CH)

        @pl.when(has_prev & whole & (c < NCH))
        def _():
            f_copy(piece).wait_recv()

        @pl.when(has_next & whole & (c < NCH))
        def _():
            j_copy(piece).wait_recv()

        at = pl.multiple_of(jnp.minimum(c, NCH - 1) * CH, CH)
        j32[8 : 8 + HALF, pl.ds(at + PAD, CH)] = jb[:, pl.ds(at, CH)].astype(F32)

    arrive(jnp.int32(0))
    cross(both, arrive)

    bds[0:8, :] = 0.5 * jnp.where(first, bdacc[0:8], bdacc[16:24])
    bhs[0:8, :] = 0.5 * jnp.where(first, bdacc[8:16], bdacc[24:32])
    bds[8:16, :] = fold(dsums[0], dsums[1])
    bhs[8:16, :] = fold(dsums[2], dsums[3])

    def bo_copy(to, slot):
        return remote(bds, bdo.at[slot], s_bo, r_bo, k, to)

    def bh_copy(to, slot):
        return remote(bhs, bdh.at[slot], s_bh, r_bh, jnp.minimum(k + 1, NC - 1), to)

    @pl.loop(0, NQ)
    def _(d):
        to = lax.rem(s + d, NQ)

        @pl.when(has_next)
        def _():
            bh_copy(to, s).start()

        @pl.when(d > 0)
        def _():
            bo_copy(to, s).start()

    bdo[s] = bds[...]

    def all_of(ref, n, ss, rs):
        return remote(ref.at[pl.ds(0, n)], ref.at[pl.ds(0, n)], ss, rs, k, lax.rem(s + 1, NQ))

    all_of(bm, NQ - 1, s_bm, r_bm).wait_recv()
    all_of(gall, NQ - 1, s_g, r_g).wait_recv()

    row = lax.broadcasted_iota(jnp.int32, (GRID, 128), 0)

    def merge(parts):
        even = jnp.concatenate(parts[0::2], axis=0)
        odd = jnp.concatenate(parts[1::2], axis=0)
        even = jnp.where(row < GRID - 2, pltpu.roll(even, GRID - 2, 0), 0.0)
        odd = jnp.where(row >= 2, pltpu.roll(odd, 2, 0), 0.0)
        return even + odd

    for i in range(12):
        for m in range(8):
            a = gall[2 * m, 8 * i : 8 * i + 8, :]
            b = gall[2 * m + 1, 8 * i : 8 * i + 8, :]
            pair = (
                jnp.where(quarter < 4, a, pltpu.roll(b, 4, 0)),
                jnp.where(quarter < 4, pltpu.roll(a, 4, 0), b),
            )
            for j in range(2):
                di, h, which = (2 * i + j) // 6, ((2 * i + j) // 3) % 2, (2 * i + j) % 3
                v = pair[j]
                if di and m == 7:
                    v = jnp.where(quarter < 8 - di, v, 0.0)
                m8 = slice(8 * m, 8 * m + 8)
                if which < 2:
                    ga[4 * di + 2 * h + which, m8, :] = v
                else:
                    o = swap(v)
                    gx[4 * di + 2 * h, m8, :] = jnp.where(first, v, o)
                    gx[4 * di + 2 * h + 1, m8, :] = jnp.where(first, o, v)
    b_i = merge([bm[p, 0:8, :] for p in range(NQ)])
    b_1 = merge([bm[p, 8:16, :] for p in range(NQ)])

    def total(v):
        return jnp.sum(v, axis=(0, 1), keepdims=True)

    tot = bm[0, 16:24, :]
    for p in range(1, NQ):
        tot = tot + bm[p, 16:24, :]
    sum_i = total(tot[0:1])
    sum_ii = total(tot[1:2])

    all_of(bdo, NQ - 1, s_bo, r_bo).wait_recv()

    @pl.when(has_prev)
    def _():
        all_of(bdh, NQ, s_bh, r_bh).wait_recv()

    b_f = b_i + merge([bdo[p, 0:8, :] + bdh[p, 0:8, :] for p in range(NQ)])
    tot = bdo[0, 8:16, :] + bdh[0, 8:16, :]
    for p in range(1, NQ):
        tot = tot + bdo[p, 8:16, :] + bdh[p, 8:16, :]
    sum_f = sum_i + total(tot[0:1])
    sum_fi = sum_ii + total(tot[1:2])
    mean_f = sum_f * (1.0 / PIXELS)

    def apply_gram(c):
        cl = [c] + [pltpu.roll(c, 128 - d, 1) for d in range(1, 4)]
        cs = swap(c)
        csl = [cs] + [pltpu.roll(cs, 128 - d, 1) for d in range(1, 4)]
        out = None
        lacc = [None] * 4

        def add(a, b):
            return b if a is None else a + b

        for di in range(4):
            racc = None
            for dj in range(4):
                a = ga[4 * di + dj]
                x = gx[4 * di + dj]
                up = (lambda v: v) if di == 0 else (lambda v: pltpu.roll(v, GRID - di, 0))
                out = add(out, a * up(cl[dj]) + x * up(csl[dj]))
                if dj:
                    lacc[dj] = add(lacc[dj], a * up(c) + x * up(cs))
                if di:
                    racc = add(racc, a * cl[dj] + x * csl[dj])
                if di and dj:
                    racc = racc + pltpu.roll(a * c + x * cs, dj, 1)
            if di:
                out = out + pltpu.roll(racc, di, 0)
        for dj in range(1, 4):
            out = out + pltpu.roll(lacc[dj], dj, 1)
        return out

    def direction(c):
        if c is None:
            mean_w = sum_i * (1.0 / PIXELS)
            sq = sum_ii
            cross = sum_fi
            b_w = b_i
        else:
            h = apply_gram(c)
            mean_w = (sum_i + total(c * b_1)) * (1.0 / PIXELS)
            sq = sum_ii + total(c * (2.0 * b_i + h))
            cross = sum_fi + total(c * b_f)
            b_w = b_i + h
        var = sq - PIXELS * mean_w * mean_w
        cov = cross - PIXELS * mean_f * mean_w
        den = jnp.sqrt(var + EPS)
        ratio = cov / den / (var + EPS)
        grad = PIXELS * ((b_f - mean_f * b_1) / den - ratio * (b_w - mean_w * b_1))
        mag = total(grad * grad) * (1.0 / (GRID * 2 * GRID))
        return grad / jnp.sqrt(mag + EPS)

    rate = 1.0 / ITERATIONS

    def cp_copy(i):
        return remote(csend.at[i], cprev.at[i], s_cp.at[i], r_cp.at[i], jnp.minimum(k + 1, NC - 1), s)

    def cn_copy(i):
        return remote(csend.at[i], cnext.at[i], s_cn.at[i], r_cn.at[i], jnp.maximum(k - 1, 0), s)

    def exchange(i, c):
        csend[i] = c

        @pl.when(has_next)
        def _():
            cp_copy(i).start()

        @pl.when(has_prev)
        def _():
            cn_copy(i).start()

    def receive(i):
        @pl.when(has_prev)
        def _():
            cp_copy(i).wait_recv()

        @pl.when(has_next)
        def _():
            cn_copy(i).wait_recv()

    c = rate * direction(None)
    exchange(0, c)
    for i in range(1, ITERATIONS - 1):
        step = c + rate * direction(c)
        receive(i - 1)
        c = step + SMOOTHING * (cprev[i - 1] - 2.0 * c + cnext[i - 1])
        exchange(i, c)
    step = c + rate * direction(c)

    base = pl.multiple_of(lax.div(4 * s + 6, 8) * 8, 8)
    even = lax.rem(s, 2) == 0

    def window(v):
        cpad[8 : 8 + GRID] = v
        w = cpad[pl.ds(base, 16), :]
        return jnp.where(even, w[6:14], w[2:10])

    cw = window(c)
    mine = window(step) - jnp.where(k == 0, SMOOTHING, 0.0) * cw
    ew_s[...] = mine

    def ew_copy(to, slot):
        return remote(ew_s, ew.at[slot], s_ew.at[to], r_ew.at[slot], to, s)

    for kk in range(1, NC):
        @pl.when(kk > k)
        def _():
            ew_copy(kk, k).start()

    receive(ITERATIONS - 2)
    nxt = window(cnext[ITERATIONS - 2])
    own = mine + SMOOTHING * (nxt - cw)

    for kk in range(NC - 1):
        @pl.when(kk < k)
        def _():
            ew_copy(kk, kk).wait_recv()

    t = ew[0]
    for kk in range(1, NC - 1):
        t = t + ew[kk]
    t = t + own
    tw_s[...] = t

    def tw_copy(to, slot):
        return remote(tw_s, tw.at[slot], s_tw, r_tw, k, to)

    @pl.loop(1, NQ)
    def _(d):
        tw_copy(lax.rem(s + d, NQ), s).start()

    tw[s] = t

    hi = t.astype(BF16)
    rest = t - hi.astype(F32)
    mid = rest.astype(BF16)
    low = (rest - mid.astype(F32)).astype(BF16)
    stack = jnp.concatenate(
        [v.astype(F32) for v in (hi, mid, low, hi, mid, hi)] + [jnp.zeros((80, 128), F32)], axis=0
    ).astype(BF16)
    mixed = jnp.dot(mx[...], stack, preferred_element_type=F32).astype(BF16).astype(F32) * 0.5
    big_first = lax.broadcasted_iota(jnp.int32, (ROWS, 128), 1) < GRID
    mixed_x = jnp.where(big_first, mixed, 0.0).astype(BF16)
    mixed_y = jnp.where(big_first, 0.0, mixed).astype(BF16)
    dims = (((1,), (1,)), ((), ()))

    @pl.loop(0, NCH // 4)
    def _(p):
        for u in range(4):
            at = pl.multiple_of((4 * p + u) * CH, CH)
            table = cd[pl.ds(at, CH), :]
            sx = lax.dot_general(mixed_x, table, dims, preferred_element_type=F32)
            sy = lax.dot_general(mixed_y, table, dims, preferred_element_type=F32)
            v = (
                i32[8 : 8 + ROWS, pl.ds(at + PAD, CH)]
                + sx * lxb[:, pl.ds(at, CH)]
                + sy * lyb[:, pl.ds(at, CH)]
            )
            reg[0, :, pl.ds(at, CH)] = v.astype(BF16)

    all_of(tw, NQ - 1, s_tw, r_tw).wait_recv()

    for m in range(8):
        acc[0, 8 * m : 8 * m + 8, :] = jnp.concatenate([tw[2 * m, 2:6, :], tw[2 * m + 1, 2:6, :]], axis=0)

    @pl.when(s > 0)
    def _():
        up_top.wait_send()

    @pl.when(s < NQ - 1)
    def _():
        down_bot.wait_send()

    @pl.when(has_prev)
    def _():
        mid_prev.wait_send()
        bot_prev.wait_send()

    half = sec.at[0, pl.ds(0, HALF)]

    @pl.when(has_next)
    def _():
        remote(half, fb, s_f, r_f.at[0], jnp.minimum(k + 1, NC - 1), s).wait_send()

    @pl.when(has_prev)
    def _():
        remote(half, jb, s_j, r_j.at[0], jnp.maximum(k - 1, 0), s).wait_send()

    @pl.when(s < NQ - 1)
    def _():
        to_next.wait_send()

    @pl.when(s > 0)
    def _():
        to_prev.wait_send()

    @pl.when(has_next)
    def _():
        all_of(bdh, NQ, s_bh, r_bh).wait_send()

    all_of(gall, NQ - 1, s_g, r_g).wait_send()
    all_of(bm, NQ - 1, s_bm, r_bm).wait_send()
    all_of(bdo, NQ - 1, s_bo, r_bo).wait_send()
    all_of(tw, NQ - 1, s_tw, r_tw).wait_send()

    for i in range(ITERATIONS - 1):
        @pl.when(has_next)
        def _():
            cp_copy(i).wait_send()

        @pl.when(has_prev)
        def _():
            cn_copy(i).wait_send()

    for kk in range(1, NC):
        @pl.when(kk > k)
        def _():
            ew_copy(kk, k).wait_send()


def solution(mesh):
    c, rows, split, mix = tables()

    def body(sections, anchor):
        v = pltpu.VMEM
        dma = pltpu.SemaphoreType.DMA
        row = v((1, COLS), F32)
        win = v((NQ, 16, 128), F32)
        scratch = [
            v((ROWS, COLS), BF16), v((HALF, COLS), BF16), v((HALF, COLS), BF16), v((HALF, COLS), BF16),
            v((ROWS + 16, COLS + 2 * PAD), F32), v((HALF + 16, COLS + 2 * PAD), F32),
            v((ROWS, COLS), F32), v((ROWS, COLS), F32),
            v((COLS, 128), BF16), v((COLS, 256), BF16),
            v((3, 80, ROWS), BF16), v((32, ROWS), BF16), v((ROWS, 128), BF16),
            v((2, 5, ROWS, CH), BF16), v((2, 96, CH), BF16), v((96, CH), F32),
            v((2, 2, ROWS, CH), BF16), v((2, 64, CH), BF16),
            v((32, COLS + 2 * PAD), F32), v((64, COLS), BF16), v((32, 128), F32),
            v((2, 8, 128), F32), v((4, 8, 128), F32),
            row, row, row, row, row, row, row,
            v((96, 128), F32), v((2, 96, 128), F32), v((96, 128), F32), v((NQ, 96, 128), F32),
            v((16, GRID, 128), F32), v((16, GRID, 128), F32),
            v((24, 128), F32), v((NQ, 24, 128), F32), v((16, 128), F32), v((16, 128), F32), win, win,
            v((GRID + 16, 128), F32), v((3, GRID, 128), F32), v((3, GRID, 128), F32), v((3, GRID, 128), F32),
            v((8, 128), F32), v((NC - 1, 8, 128), F32), v((8, 128), F32), v((NQ, 8, 128), F32),
            dma((4,)), dma((4,)), dma((2,)), pltpu.SemaphoreType.REGULAR((4,)),
            dma, dma((NX,)), dma, dma((NX,)), dma((4,)), dma((4,)), dma((2,)), dma((2,)),
            dma, dma, dma, dma, dma, dma, dma, dma,
            dma((3,)), dma((3,)), dma((3,)), dma((3,)), dma((NC,)), dma((NC,)), dma, dma,
        ]
        anywhere = pl.BlockSpec(memory_space=pl.ANY)
        inside = pl.BlockSpec(memory_space=pltpu.VMEM)
        return pl.pallas_call(
            kernel,
            out_shape=(
                pltpu.VMEM((1, ROWS, COLS), BF16),
                pltpu.VMEM((1, GRID, 2 * GRID), F32),
            ),
            in_specs=[anywhere] * 6,
            out_specs=(inside, inside),
            scratch_shapes=scratch,
            compiler_params=pltpu.CompilerParams(
                collective_id=0, has_side_effects=True, vmem_limit_bytes=64_900_000
            ),
        )(
            sections, anchor,
            jnp.asarray(c, BF16), jnp.asarray(rows, BF16), jnp.asarray(split, BF16), jnp.asarray(mix, BF16),
        )

    return jax.shard_map(
        body, mesh=mesh,
        in_specs=(P("chain", "quad", None), P("quad", None)),
        out_specs=(P("chain", "quad", None), P("chain", None, None)),
        check_vma=False,
    )
```

```python
import numpy as np
import jax
import jax.numpy as jnp
from jax import lax
from jax.experimental import pallas as pl
from jax.experimental.pallas import tpu as pltpu
from jax.sharding import PartitionSpec as P

GRID = 64
ITERATIONS = 4
EPS = 1e-6
SMOOTHING = 0.25
MESH = pl.DeviceIdType.MESH
F32 = jnp.float32
BF16 = jnp.bfloat16

ROWS = 256
COLS = 4096
UP = 160
LOW = ROWS - UP
CH = 256
NCH = COLS // CH
CX = 512
NX = COLS // CX
PAD = 128
NC = 8
NQ = 16
PIXELS = float(4096 * 4096)


def weight(offset):
    d = np.abs(offset)
    near = 2.0 / 3.0 - d * d + 0.5 * d * d * d
    r = 2.0 - d
    far = r * r * r / 6.0
    return np.where(d < 1.0, near, np.where(d < 2.0, far, 0.0 * d)).astype(np.float32)


def bf(x):
    return np.asarray(jnp.asarray(x, jnp.float32).astype(BF16).astype(jnp.float32))


def hi_lo(x):
    hi = bf(x)
    return [hi, bf(x - hi)]


def tables():
    f = np.float32
    x = np.arange(COLS, dtype=f)
    c = weight((x[:, None] + f(0.5)) / f(64) - np.arange(GRID, dtype=f)[None, :] - f(0.5))
    c = np.concatenate([c, c], axis=1)
    y = np.arange(-1, ROWS + 1, dtype=f)
    ext = weight((y[:, None] + f(0.5)) / f(64) - (np.arange(8, dtype=f) - f(2))[None, :] - f(0.5)).T
    r = ext[:, 1:-1]
    pairs = np.zeros((4, 8, ROWS), f)
    for d in range(4):
        pairs[d, : 8 - d] = r[: 8 - d] * r[d:]
    step = 0.5 * (r - ext[:, 2:])
    rows = []
    for variant in range(3):
        e = ext.copy()
        if variant == 0:
            e[:, 0] = 0.0
        if variant == 2:
            e[:, -1] = 0.0
        slope = 0.5 * (e[:, :-2] - e[:, 2:])
        rows.append(np.concatenate([pairs.reshape(32, ROWS)] + hi_lo(r) + hi_lo(slope) + hi_lo(step), axis=0))
    top = (np.arange(ROWS) < UP).astype(f)[None]
    split = np.concatenate([h * top for h in hi_lo(r)] + [h * (1 - top) for h in hi_lo(r)], axis=0)
    hi = bf(r)
    mid = bf(r - hi)
    low = bf(r - hi - mid)
    mix = np.concatenate([hi, hi, hi, mid, mid, low, np.zeros((80, ROWS), f)], axis=0).T
    return c, np.stack(rows), split, mix


def kernel(
    sec, anc, cd_in, rt_in, sp_in, mx_in,
    reg, acc,
    ib, fb, jb, ab, i32, j32, lxb, lyb, cd, w1, rt, sp, mx,
    wb, qb, tb, gacc, qd, vb, ub, lhs, bdacc, sums, dsums,
    etop, ebot, emid, htop, hbot, jmid, jbot,
    gs, gn, gp, gt, gfs, gbs, gf, gb, ga, gx, bms, bm, bds, bhs, baa, bdo, bdh,
    cpad, csend, cprev, cnext, ew_s, ew, tw_s, tw,
    sem_in, sem_c, sem_a, rounds,
    s_f, r_f, s_j, r_j, s_h, r_h, s_n, r_n, s_g, r_g, s_bm, r_bm,
    s_bo, r_bo, s_bh, r_bh, s_ba, s_cp, r_cp, s_cn, r_cn, s_ew, r_ew, s_tw, r_tw,
):
    k = lax.axis_index("chain")
    s = lax.axis_index("quad")
    has_prev = k > 0
    has_next = k < NC - 1

    def remote(src, dst, ss, rs, kk, qq):
        return pltpu.make_async_remote_copy(
            src_ref=src, dst_ref=dst, send_sem=ss, recv_sem=rs,
            device_id={"chain": kk, "quad": qq}, device_id_type=MESH,
        )

    def in_copy(c):
        w = COLS // 4
        return pltpu.make_async_copy(
            sec.at[0, :, pl.ds(c * w, w)], ib.at[:, pl.ds(c * w, w)], sem_in.at[c]
        )

    for c in range(4):
        in_copy(c).start()
    consts = [
        pltpu.make_async_copy(cd_in, cd, sem_c.at[0]),
        pltpu.make_async_copy(rt_in, rt, sem_c.at[1]),
        pltpu.make_async_copy(sp_in, sp, sem_c.at[2]),
        pltpu.make_async_copy(mx_in, mx, sem_c.at[3]),
    ]
    for d in consts:
        d.start()
    anc_copies = [
        pltpu.make_async_copy(anc.at[pl.ds(0, UP)], fb, sem_a.at[0]),
        pltpu.make_async_copy(anc.at[pl.ds(UP, LOW)], ab, sem_a.at[1]),
    ]

    @pl.when(k == 0)
    def _():
        for d in anc_copies:
            d.start()

    barrier = pltpu.get_barrier_semaphore()

    def hello(sem, step):
        for sign in (1, -1):
            kk = k + sign * step
            pl.semaphore_signal(
                sem, inc=1, device_id={"chain": k, "quad": lax.rem(s + sign * step + NQ, NQ)}, device_id_type=MESH
            )

            @pl.when((kk >= 0) & (kk < NC))
            def _():
                pl.semaphore_signal(sem, inc=1, device_id={"chain": kk, "quad": s}, device_id_type=MESH)

    def heard(sem, step):
        one = jnp.int32(1)
        zero = jnp.int32(0)
        pl.semaphore_wait(
            sem, 2 + jnp.where(k >= step, one, zero) + jnp.where(k + step < NC, one, zero)
        )

    hello(barrier, 1)

    i32[:, :PAD] = jnp.zeros((ROWS + 16, PAD), F32)
    i32[:, PAD + COLS :] = jnp.zeros((ROWS + 16, PAD), F32)
    j32[:, :PAD] = jnp.zeros((LOW + 16, PAD), F32)
    j32[:, PAD + COLS :] = jnp.zeros((LOW + 16, PAD), F32)
    ub[:, :PAD] = jnp.zeros((32, PAD), F32)
    ub[:, PAD + COLS :] = jnp.zeros((32, PAD), F32)
    sums[...] = jnp.zeros_like(sums)
    qb[1] = jnp.zeros((5, ROWS, CH), BF16)
    tb[0] = jnp.zeros((96, CH), BF16)
    gacc[...] = jnp.zeros_like(gacc)
    qd[...] = jnp.zeros_like(qd)
    vb[...] = jnp.zeros_like(vb)
    dsums[...] = jnp.zeros_like(dsums)
    bdacc[...] = jnp.zeros_like(bdacc)
    cpad[...] = jnp.zeros_like(cpad)

    @pl.when(s == 0)
    def _():
        htop[...] = jnp.zeros_like(htop)
        gn[0] = jnp.zeros((96, 128), F32)

    @pl.when(s == NQ - 1)
    def _():
        hbot[...] = jnp.zeros_like(hbot)
        gn[1] = jnp.zeros((96, 128), F32)

    @pl.when(k == 0)
    def _():
        cprev[...] = jnp.zeros_like(cprev)

    @pl.when(k == NC - 1)
    def _():
        jb[...] = jnp.zeros_like(jb)
        jmid[...] = jnp.zeros_like(jmid)
        jbot[...] = jnp.zeros_like(jbot)
        cnext[...] = jnp.zeros_like(cnext)

    for j in range(NC - 1):
        @pl.when(j >= k)
        def _():
            ew[j] = jnp.zeros((8, 128), F32)

    heard(barrier, 1)
    hello(rounds.at[0], 1)

    def f_copy(c):
        at = pl.multiple_of(c * CX, CX)
        return remote(
            sec.at[0, pl.ds(0, UP), pl.ds(at, CX)], fb.at[:, pl.ds(at, CX)],
            s_f, r_f.at[c], jnp.minimum(k + 1, NC - 1), s,
        )

    def j_copy(c):
        at = pl.multiple_of(c * CX, CX)
        return remote(
            sec.at[0, pl.ds(UP, LOW), pl.ds(at, CX)], jb.at[:, pl.ds(at, CX)],
            s_j, r_j.at[c], jnp.maximum(k - 1, 0), s,
        )

    @pl.loop(0, NX)
    def _(c):
        @pl.when(has_next)
        def _():
            f_copy(c).start()

        @pl.when(has_prev)
        def _():
            j_copy(c).start()

    up_top = remote(etop, hbot, s_h.at[0], r_h.at[0], k, jnp.maximum(s - 1, 0))
    down_bot = remote(ebot, htop, s_h.at[1], r_h.at[1], k, jnp.minimum(s + 1, NQ - 1))
    mid_prev = remote(emid, jmid, s_h.at[2], r_h.at[2], jnp.maximum(k - 1, 0), s)
    bot_prev = remote(hbot, jbot, s_h.at[3], r_h.at[3], jnp.maximum(k - 1, 0), s)

    for c in range(4):
        in_copy(c).wait()
    etop[...] = ib[0:16, :].astype(F32)[0:1]
    ebot[...] = ib[ROWS - 16 : ROWS, :].astype(F32)[15:16]
    emid[...] = ib[UP - 16 : UP, :].astype(F32)[15:16]

    @pl.when(s > 0)
    def _():
        up_top.start()

    @pl.when(s < NQ - 1)
    def _():
        down_bot.start()

    @pl.when(has_prev)
    def _():
        mid_prev.start()

    for d in consts:
        d.wait()
    lane = lax.broadcasted_iota(jnp.int32, (8, 128), 1)

    v = cd[pl.ds(CH, CH), :].astype(F32)
    ln = lax.broadcasted_iota(jnp.int32, (CH, 128), 1)
    knot = jnp.where(ln < GRID, ln, ln - GRID)
    for h in range(2):
        a = v if h == 0 else pltpu.roll(v, 128 - 2 * h, 1)
        b = pltpu.roll(v, 127 - 2 * h, 1)
        wb[:, h * 128 : (h + 1) * 128] = v * jnp.where(ln < GRID, a, b)

    @pl.loop(0, NCH // 4)
    def _(c4):
      for c in [4 * c4 + u for u in range(4)]:
        at = pl.multiple_of(c * CH, CH)
        for h in range(2):
            partner = knot + jnp.where(ln < GRID, 2 * h, 2 * h + 1)
            near = (jnp.abs(2 * (knot - 4 * c) - 3) < 16) & (partner < GRID)
            t = pltpu.roll(wb[:, h * 128 : (h + 1) * 128], lax.rem(4 * c + 124, 128), 1)
            w1[pl.ds(at, CH), h * 128 : (h + 1) * 128] = jnp.where(near, t, 0.0).astype(BF16)

    variant = jnp.where(s == 0, 0, jnp.where(s == NQ - 1, 2, 1))
    RB = 32

    def spot(c):
        return pl.multiple_of(jnp.maximum(c, 0) * CH, CH)

    @pl.loop(0, NCH // 2)
    def _(p):
        for c in [2 * p, 2 * p + 1]:
            at = pl.multiple_of(c * CH, CH)
            u = jnp.dot(rt[variant, 32:64, :], ib[:, pl.ds(at, CH)], preferred_element_type=F32)
            ub[0:8, pl.ds(at + PAD, CH)] = u[0:8] + u[8:16]
            ub[8:16, pl.ds(at + PAD, CH)] = u[16:24] + u[24:32]
            s1 = jnp.zeros((8, CH), F32)
            s2 = jnp.zeros((8, CH), F32)
            for r in range(0, ROWS, RB):
                x = ib[r : r + RB, pl.ds(at, CH)].astype(F32)
                i32[8 + r : 8 + r + RB, pl.ds(at + PAD, CH)] = x
                for t in range(0, RB, 8):
                    xt = x[t : t + 8]
                    s1 = s1 + xt
                    s2 = s2 + xt * xt
            sums[0] = sums[0] + s1[:, :128] + s1[:, 128:]
            sums[1] = sums[1] + s2[:, :128] + s2[:, 128:]

    @pl.when(s < NQ - 1)
    def _():
        up_top.wait_recv()

    @pl.when(s > 0)
    def _():
        down_bot.wait_recv()

    @pl.when(has_prev)
    def _():
        bot_prev.start()

    i32[7:8, PAD : PAD + COLS] = htop[...]
    i32[8 + ROWS : 9 + ROWS, PAD : PAD + COLS] = hbot[...]

    heard(rounds.at[0], 1)
    hello(rounds.at[1], 2)

    def tally(i, d, x):
        a = jnp.zeros((8, CH), F32)
        b = jnp.zeros((8, CH), F32)
        for t in range(0, d.shape[0], 8):
            a = a + d[t : t + 8]
            b = b + d[t : t + 8] * x[t : t + 8]
        dsums[i] = dsums[i] + a[:, :128] + a[:, 128:]
        dsums[i + 1] = dsums[i + 1] + b[:, :128] + b[:, 128:]

    def pixels(at, slot, with_anchor):
        for r in range(0, ROWS, RB):
            mid = i32[8 + r : 8 + r + RB, pl.ds(at, CH + 2 * PAD)]
            x = mid[:, PAD : PAD + CH]
            right = pltpu.roll(mid, CH + 2 * PAD - 1, 1)[:, PAD : PAD + CH]
            left = pltpu.roll(mid, 1, 1)[:, PAD : PAD + CH]
            lx = right - left
            lxb[r : r + RB, pl.ds(at, CH)] = lx
            tall = i32[r : r + RB + 16, pl.ds(at + PAD, CH)]
            below = pltpu.roll(tall, RB + 15, 0)[8 : 8 + RB]
            above = pltpu.roll(tall, 1, 0)[8 : 8 + RB]
            ly = below - above
            lyb[r : r + RB, pl.ds(at, CH)] = ly
            qb[slot, 0, r : r + RB, :] = (lx * lx).astype(BF16)
            qb[slot, 3, r : r + RB, :] = (x * right).astype(BF16)
            qb[slot, 1, r : r + RB, :] = (lx * ly).astype(BF16)
            qb[slot, 2, r : r + RB, :] = (ly * ly).astype(BF16)
            qb[slot, 4, r : r + RB, :] = (x * below).astype(BF16)
            if with_anchor:
                src, rr = (fb, r) if r < UP else (ab, r - UP)
                d = src[rr : rr + RB, pl.ds(at, CH)].astype(F32) - x
                qd[slot, 0, r : r + RB, :] = (d * lx).astype(BF16)
                qd[slot, 1, r : r + RB, :] = (d * ly).astype(BF16)
                tally(0, d, x)

    def rows_out(at, slot, with_anchor):
        for i in range(3):
            tb[slot, 32 * i : 32 + 32 * i, :] = jnp.dot(
                rt[variant, 0:32, :], qb[slot, i], preferred_element_type=F32
            ).astype(BF16)
        z = jnp.dot(rt[variant, 32:48, :], qb[slot, 3], preferred_element_type=F32)
        ub[16:24, pl.ds(at + PAD, CH)] = z[0:8] + z[8:16]
        q = jnp.dot(rt[variant, 64:80, :], qb[slot, 4], preferred_element_type=F32)
        ub[24:32, pl.ds(at + PAD, CH)] = q[0:8] + q[8:16]
        if with_anchor:
            for i in range(2):
                v = jnp.dot(rt[variant, 32:48, :], qd[slot, i], preferred_element_type=F32)
                v = v[0:8] + v[8:16]
                hi = v.astype(BF16).astype(F32)
                vb[slot, 16 * i : 16 * i + 16, :] = jnp.concatenate([hi, v - hi], axis=0).astype(BF16)

    def columns_out(at, slot, with_anchor):
        gacc[...] = gacc[...] + jnp.dot(tb[slot], w1[pl.ds(at, CH), :], preferred_element_type=F32)
        if with_anchor:
            b = jnp.dot(vb[slot, 0:32, :], cd[pl.ds(at, CH), :], preferred_element_type=F32)
            bdacc[0:8] = bdacc[0:8] + b[0:8] + b[8:16]
            bdacc[16:24] = bdacc[16:24] + b[16:24] + b[24:32]

    def own_pass(with_anchor):
        @pl.loop(0, NCH // 2)
        def _(p):
            @pl.when(p == 3)
            def _():
                heard(rounds.at[1], 2)
                hello(rounds.at[2], 4)

            @pl.when(p == 7)
            def _():
                heard(rounds.at[2], 4)
                hello(rounds.at[3], 1)

            for u in range(2):
                c = 2 * p + u
                columns_out(spot(c - 2), u, with_anchor)
                pixels(spot(c), u, with_anchor)
                rows_out(spot(c - 1), 1 - u, with_anchor)

        columns_out(spot(NCH - 2), 0, with_anchor)
        rows_out(spot(NCH - 1), 1, with_anchor)
        columns_out(spot(NCH - 1), 1, with_anchor)

    @pl.when(k > 0)
    def _():
        own_pass(False)

    @pl.when(k == 0)
    def _():
        for d in anc_copies:
            d.wait()
        own_pass(True)

    first = lane < GRID

    def swap(v):
        return pltpu.roll(v, GRID, 1)

    quarter = lax.broadcasted_iota(jnp.int32, (8, 128), 0)

    def pack(a, b):
        return jnp.where(quarter < 4, pltpu.roll(a, 6, 0), pltpu.roll(b, 2, 0))

    order = [(di, h) for di in range(2) for h in range(1)]
    order = order + [(di, h) for di in range(4) for h in range(2) if (di, h) not in order]
    slots = []
    for di, h in order:
        part = lambda q: 0.25 * gacc[32 * q + 8 * di : 32 * q + 8 * di + 8, 128 * h : 128 * h + 128]
        xx, xy, yy = part(0), part(1), part(2)
        slots.append(jnp.where(first, xx, swap(yy)))
        slots.append(jnp.where(first, swap(xx), yy))
        slots.append(xy)
    for i in range(12):
        a, b = slots[2 * i], slots[2 * i + 1]
        gs[8 * i : 8 * i + 8, :] = pack(a, b)
        gp[8 * i : 8 * i + 8, :] = pack(pltpu.roll(a, 4, 0), pltpu.roll(b, 4, 0))

    to_next = remote(gp, gn.at[0], s_n.at[0], r_n.at[0], k, jnp.minimum(s + 1, NQ - 1))
    to_prev = remote(gp, gn.at[1], s_n.at[1], r_n.at[1], k, jnp.maximum(s - 1, 0))

    @pl.when(s < NQ - 1)
    def _():
        to_next.start()

    @pl.when(s > 0)
    def _():
        to_prev.start()

    @pl.loop(0, NCH // 4)
    def _(c4):
      for c in [4 * c4 + u for u in range(4)]:
        at = pl.multiple_of(c * CH, CH)
        wide = ub[:, pl.ds(at, CH + 2 * PAD)]
        right = pltpu.roll(wide, CH + 2 * PAD - 1, 1)[:, PAD : PAD + CH]
        left = pltpu.roll(wide, 1, 1)[:, PAD : PAD + CH]
        x = wide[:, PAD : PAD + CH]
        v = jnp.concatenate(
            [0.5 * (right[0:8] - left[0:8]), x[8:16], 0.5 * (x[16:24] - left[16:24]), x[24:32]], axis=0
        )
        hi = v.astype(BF16)
        lhs[0:32, pl.ds(at, CH)] = hi
        lhs[32:64, pl.ds(at, CH)] = (v - hi.astype(F32)).astype(BF16)

    bb = jnp.dot(lhs[...], cd[...], preferred_element_type=F32)
    bb = bb[0:32] + bb[32:64]
    bms[0:8, :] = jnp.where(first, bb[16:24], bb[24:32])
    bms[8:16, :] = jnp.where(first, bb[0:8], bb[8:16])

    def fold(a, b):
        ra = jnp.sum(a, axis=0, keepdims=True)
        rb = jnp.sum(b, axis=0, keepdims=True)
        return jnp.where(quarter == 0, ra, jnp.where(quarter == 1, rb, 0.0))

    bms[16:24, :] = fold(sums[0], sums[1])
    bm[s] = bms[...]

    def bm_copy(to, slot):
        return remote(bms, bm.at[slot], s_bm, r_bm, k, to)

    @pl.loop(1, NQ)
    def _(d):
        bm_copy(lax.rem(s + d, NQ), s).start()

    heard(rounds.at[3], 1)

    def gf_copy(to, slot):
        return remote(gfs, gf.at[slot], s_g.at[0], r_g.at[0], k, to)

    def gb_copy(to, slot):
        return remote(gbs, gb.at[slot], s_g.at[1], r_g.at[1], k, to)

    def spread_gram():
        @pl.when(s > 0)
        def _():
            to_next.wait_recv()

        @pl.when(s < NQ - 1)
        def _():
            to_prev.wait_recv()

        lower_rows = (quarter == 0) | (quarter == 1) | (quarter == 4) | (quarter == 5)
        for i in range(12):
            b8 = slice(8 * i, 8 * i + 8)
            gt[b8, :] = gs[b8, :] + jnp.where(lower_rows, gn[0, b8, :], gn[1, b8, :])
        gfs[...] = gt[0:24, :]
        gbs[0:64, :] = gt[24:88, :].astype(BF16)
        gbs[64:80, :] = jnp.concatenate([gt[88:96, :], jnp.zeros((8, 128), F32)], axis=0).astype(BF16)
        gf[s] = gfs[...]
        gb[s] = gbs[...]

        @pl.loop(1, NQ)
        def _(d):
            to = lax.rem(s + d, NQ)
            gf_copy(to, s).start()

    @pl.when(has_next)
    def _():
        mid_prev.wait_recv()
        bot_prev.wait_recv()

    j32[7:8, PAD : PAD + COLS] = jmid[...]
    j32[8 + LOW : 9 + LOW, PAD : PAD + COLS] = jbot[...]

    def tuck(ref, at, a, b):
        ref[at : at + 1, :] = jnp.sum(a, axis=0, keepdims=True)
        ref[at + 1 : at + 2, :] = jnp.sum(b, axis=0, keepdims=True)

    def ba_copy(to, slot):
        return remote(baa, bdh.at[slot], s_ba, r_bh, k, to)

    def cross_rows(slot):
        v = jnp.concatenate(
            [jnp.dot(sp[...], qd[slot, i], preferred_element_type=F32) for i in range(2)], axis=0
        )
        v = jnp.concatenate(
            [v[0:8] + v[8:16], v[16:24] + v[24:32], v[32:40] + v[40:48], v[48:56] + v[56:64]], axis=0
        )
        hi = v.astype(BF16)
        vb[slot, 0:32, :] = hi
        vb[slot, 32:64, :] = (v - hi.astype(F32)).astype(BF16)

    def cross_columns(at, slot):
        b = jnp.dot(vb[slot], cd[pl.ds(at, CH), :], preferred_element_type=F32)
        bdacc[...] = bdacc[...] + b[0:32] + b[32:64]

    def both(at, slot, upper):
        for r in range(0, UP if upper else 0, RB):
            x = i32[8 + r : 8 + r + RB, pl.ds(at + PAD, CH)]
            d = fb[r : r + RB, pl.ds(at, CH)].astype(F32) - x
            qd[slot, 0, r : r + RB, :] = (d * lxb[r : r + RB, pl.ds(at, CH)]).astype(BF16)
            qd[slot, 1, r : r + RB, :] = (d * lyb[r : r + RB, pl.ds(at, CH)]).astype(BF16)
            tally(0, d, x)
        for r in range(0, LOW, RB):
            rr = UP + r
            mid = j32[8 + r : 8 + r + RB, pl.ds(at, CH + 2 * PAD)]
            x = mid[:, PAD : PAD + CH]
            right = pltpu.roll(mid, CH + 2 * PAD - 1, 1)[:, PAD : PAD + CH]
            left = pltpu.roll(mid, 1, 1)[:, PAD : PAD + CH]
            tall = j32[r : r + RB + 16, pl.ds(at + PAD, CH)]
            below = pltpu.roll(tall, RB + 15, 0)[8 : 8 + RB]
            above = pltpu.roll(tall, 1, 0)[8 : 8 + RB]
            d = i32[8 + rr : 8 + rr + RB, pl.ds(at + PAD, CH)] - x
            qd[slot, 0, rr : rr + RB, :] = (d * (right - left)).astype(BF16)
            qd[slot, 1, rr : rr + RB, :] = (d * (below - above)).astype(BF16)
            tally(2, d, x)

    def cross(upper):
        @pl.loop(0, NCH // 2)
        def _(p):
            @pl.when(p == 2)
            def _():
                spread_gram()

            arrive(p + 1)
            for u in range(2):
                c = 2 * p + u
                cross_columns(spot(c - 2), u)
                both(spot(c), u, upper)
                cross_rows(1 - u)

        cross_columns(spot(NCH - 2), 0)
        cross_rows(1)
        cross_columns(spot(NCH - 1), 1)

    @pl.when(k == 0)
    def _():
        baa[0:8, :] = 0.5 * jnp.where(first, bdacc[0:8], bdacc[16:24])
        bdacc[...] = jnp.zeros_like(bdacc)
        qd[...] = jnp.zeros_like(qd)
        vb[...] = jnp.zeros_like(vb)

        @pl.loop(1, NQ)
        def _(d):
            ba_copy(lax.rem(s + d, NQ), s).start()

        bdh[s] = baa[...]

    def arrive(piece):
        @pl.when(has_prev & (piece < NX))
        def _():
            f_copy(piece).wait_recv()

        @pl.when(has_next & (piece < NX))
        def _():
            j_copy(piece).wait_recv()

        at = pl.multiple_of(jnp.minimum(piece, NX - 1) * CX, CX)
        j32[8 : 8 + LOW, pl.ds(at + PAD, CX)] = jb[:, pl.ds(at, CX)].astype(F32)

    arrive(jnp.int32(0))

    @pl.when(k > 0)
    def _():
        cross(True)

    @pl.when(k == 0)
    def _():
        cross(False)

    bds[0:8, :] = 0.5 * jnp.where(first, bdacc[0:8], bdacc[16:24])
    bhs[0:8, :] = 0.5 * jnp.where(first, bdacc[8:16], bdacc[24:32])
    tuck(bds, 6, dsums[0], dsums[1])
    tuck(bhs, 0, dsums[2], dsums[3])

    def bo_copy(to, slot):
        return remote(bds, bdo.at[slot], s_bo, r_bo, k, to)

    def bh_copy(to, slot):
        return remote(bhs, bdh.at[slot], s_bh, r_bh, jnp.minimum(k + 1, NC - 1), to)

    @pl.loop(0, NQ)
    def _(d):
        to = lax.rem(s + d, NQ)

        @pl.when(has_next)
        def _():
            bh_copy(to, s).start()

        @pl.when(d > 0)
        def _():
            bo_copy(to, s).start()

    bdo[s] = bds[...]

    @pl.loop(1, NQ)
    def _(d):
        gb_copy(lax.rem(s + d, NQ), s).start()


    def all_of(ref, n, ss, rs):
        return remote(ref.at[pl.ds(0, n)], ref.at[pl.ds(0, n)], ss, rs, k, lax.rem(s + 1, NQ))

    all_of(bm, NQ - 1, s_bm, r_bm).wait_recv()

    row = lax.broadcasted_iota(jnp.int32, (GRID, 128), 0)

    def merge(parts):
        even = jnp.concatenate(parts[0::2], axis=0)
        odd = jnp.concatenate(parts[1::2], axis=0)
        even = jnp.where(row < GRID - 2, pltpu.roll(even, GRID - 2, 0), 0.0)
        odd = jnp.where(row >= 2, pltpu.roll(odd, 2, 0), 0.0)
        return even + odd

    b_i = merge([bm[p, 0:8, :] for p in range(NQ)])
    b_1 = merge([bm[p, 8:16, :] for p in range(NQ)])

    def total(v):
        return jnp.sum(v, axis=(0, 1), keepdims=True)

    tot = bm[0, 16:24, :]
    for p in range(1, NQ):
        tot = tot + bm[p, 16:24, :]
    sum_i = total(tot[0:1])
    sum_ii = total(tot[1:2])

    all_of(bdo, NQ - 1, s_bo, r_bo).wait_recv()

    @pl.when(has_prev)
    def _():
        all_of(bdh, NQ, s_bh, r_bh).wait_recv()

    @pl.when(k == 0)
    def _():
        all_of(bdh, NQ - 1, s_ba, r_bh).wait_recv()

    parts = []
    tot_d = None
    tot_di = None
    for p in range(NQ):
        up, dn = bdo[p], bdh[p]
        parts.append(jnp.where(quarter < 6, up, 0.0) + jnp.where((quarter >= 2) | (k == 0), dn, 0.0))
        a = up[6:7] + jnp.where(k == 0, 0.0, dn[0:1])
        b = up[7:8] + jnp.where(k == 0, 0.0, dn[1:2])
        tot_d = a if p == 0 else tot_d + a
        tot_di = b if p == 0 else tot_di + b
    b_f = b_i + merge(parts)
    sum_f = sum_i + total(tot_d)
    sum_fi = sum_ii + total(tot_di)
    mean_f = sum_f * (1.0 / PIXELS)

    def apply_gram(c):
        cl = [c] + [pltpu.roll(c, 128 - d, 1) for d in range(1, 4)]
        cs = swap(c)
        csl = [cs] + [pltpu.roll(cs, 128 - d, 1) for d in range(1, 4)]
        out = None
        lacc = [None] * 4

        def add(a, b):
            return b if a is None else a + b

        for di in range(4):
            racc = None
            for dj in range(4):
                a = ga[4 * di + dj]
                x = gx[4 * di + dj]
                up = (lambda v: v) if di == 0 else (lambda v: pltpu.roll(v, GRID - di, 0))
                out = add(out, a * up(cl[dj]) + x * up(csl[dj]))
                if dj:
                    lacc[dj] = add(lacc[dj], a * up(c) + x * up(cs))
                if di:
                    racc = add(racc, a * cl[dj] + x * csl[dj])
                if di and dj:
                    racc = racc + pltpu.roll(a * c + x * cs, dj, 1)
            if di:
                out = out + pltpu.roll(racc, di, 0)
        for dj in range(1, 4):
            out = out + pltpu.roll(lacc[dj], dj, 1)
        return out

    def direction(c):
        if c is None:
            mean_w = sum_i * (1.0 / PIXELS)
            sq = sum_ii
            cross = sum_fi
            b_w = b_i
        else:
            h = apply_gram(c)
            mean_w = (sum_i + total(c * b_1)) * (1.0 / PIXELS)
            sq = sum_ii + total(c * (2.0 * b_i + h))
            cross = sum_fi + total(c * b_f)
            b_w = b_i + h
        var = sq - PIXELS * mean_w * mean_w
        cov = cross - PIXELS * mean_f * mean_w
        den = jnp.sqrt(var + EPS)
        ratio = cov / den / (var + EPS)
        grad = PIXELS * ((b_f - mean_f * b_1) / den - ratio * (b_w - mean_w * b_1))
        mag = total(grad * grad) * (1.0 / (GRID * 2 * GRID))
        return grad / jnp.sqrt(mag + EPS)

    rate = 1.0 / ITERATIONS

    def cp_copy(i):
        return remote(csend.at[i], cprev.at[i], s_cp.at[i], r_cp.at[i], jnp.minimum(k + 1, NC - 1), s)

    def cn_copy(i):
        return remote(csend.at[i], cnext.at[i], s_cn.at[i], r_cn.at[i], jnp.maximum(k - 1, 0), s)

    def exchange(i, c):
        csend[i] = c

        @pl.when(has_next)
        def _():
            cp_copy(i).start()

        @pl.when(has_prev)
        def _():
            cn_copy(i).start()

    def receive(i):
        @pl.when(has_prev)
        def _():
            cp_copy(i).wait_recv()

        @pl.when(has_next)
        def _():
            cn_copy(i).wait_recv()

    c = rate * direction(None)
    exchange(0, c)

    all_of(gf, NQ - 1, s_g.at[0], r_g.at[0]).wait_recv()
    all_of(gb, NQ - 1, s_g.at[1], r_g.at[1]).wait_recv()
    for m in range(8):
        ab_f = [gf[2 * m + j] for j in range(2)]
        ab_b = [gb[2 * m + j].astype(F32) for j in range(2)]
        for i in range(12):
            src = ab_f if i < 3 else ab_b
            o = 8 * i if i < 3 else 8 * (i - 3)
            a, b = src[0][o : o + 8], src[1][o : o + 8]
            pair = (
                jnp.where(quarter < 4, a, pltpu.roll(b, 4, 0)),
                jnp.where(quarter < 4, pltpu.roll(a, 4, 0), b),
            )
            for j in range(2):
                (di, h), which = order[(2 * i + j) // 3], (2 * i + j) % 3
                v = pair[j]
                if di and m == 7:
                    v = jnp.where(quarter < 8 - di, v, 0.0)
                m8 = slice(8 * m, 8 * m + 8)
                if which < 2:
                    ga[4 * di + 2 * h + which, m8, :] = v
                else:
                    o2 = swap(v)
                    gx[4 * di + 2 * h, m8, :] = jnp.where(first, v, o2)
                    gx[4 * di + 2 * h + 1, m8, :] = jnp.where(first, o2, v)

    for i in range(1, ITERATIONS - 1):
        step = c + rate * direction(c)
        receive(i - 1)
        c = step + SMOOTHING * (cprev[i - 1] - 2.0 * c + cnext[i - 1])
        exchange(i, c)
    step = c + rate * direction(c)

    base = pl.multiple_of(lax.div(4 * s + 6, 8) * 8, 8)
    even = lax.rem(s, 2) == 0

    def window(v):
        cpad[8 : 8 + GRID] = v
        w = cpad[pl.ds(base, 16), :]
        return jnp.where(even, w[6:14], w[2:10])

    cw = window(c)
    mine = window(step) - jnp.where(k == 0, SMOOTHING, 0.0) * cw
    ew_s[...] = mine

    def ew_copy(to, slot):
        return remote(ew_s, ew.at[slot], s_ew.at[to], r_ew.at[slot], to, s)

    for kk in range(1, NC):
        @pl.when(kk > k)
        def _():
            ew_copy(kk, k).start()

    receive(ITERATIONS - 2)
    nxt = window(cnext[ITERATIONS - 2])
    own = mine + SMOOTHING * (nxt - cw)

    for kk in range(NC - 1):
        @pl.when(kk < k)
        def _():
            ew_copy(kk, kk).wait_recv()

    t = ew[0]
    for kk in range(1, NC - 1):
        t = t + ew[kk]
    t = t + own
    tw_s[...] = t

    def tw_copy(to, slot):
        return remote(tw_s, tw.at[slot], s_tw, r_tw, k, to)

    @pl.loop(1, NQ)
    def _(d):
        tw_copy(lax.rem(s + d, NQ), s).start()

    tw[s] = t

    hi = t.astype(BF16)
    rest = t - hi.astype(F32)
    mid = rest.astype(BF16)
    low = (rest - mid.astype(F32)).astype(BF16)
    stack = jnp.concatenate(
        [v.astype(F32) for v in (hi, mid, low, hi, mid, hi)] + [jnp.zeros((80, 128), F32)], axis=0
    ).astype(BF16)
    mixed = jnp.dot(mx[...], stack, preferred_element_type=F32).astype(BF16).astype(F32) * 0.5
    big_first = lax.broadcasted_iota(jnp.int32, (ROWS, 128), 1) < GRID
    mixed_x = jnp.where(big_first, mixed, 0.0).astype(BF16)
    mixed_y = jnp.where(big_first, 0.0, mixed).astype(BF16)
    dims = (((1,), (1,)), ((), ()))

    @pl.loop(0, NCH // 8)
    def _(p):
        for u in range(8):
            at = pl.multiple_of((8 * p + u) * CH, CH)
            table = cd[pl.ds(at, CH), :]
            sx = lax.dot_general(mixed_x, table, dims, preferred_element_type=F32)
            sy = lax.dot_general(mixed_y, table, dims, preferred_element_type=F32)
            v = (
                i32[8 : 8 + ROWS, pl.ds(at + PAD, CH)]
                + sx * lxb[:, pl.ds(at, CH)]
                + sy * lyb[:, pl.ds(at, CH)]
            )
            reg[0, :, pl.ds(at, CH)] = v.astype(BF16)

    all_of(tw, NQ - 1, s_tw, r_tw).wait_recv()

    for m in range(8):
        acc[0, 8 * m : 8 * m + 8, :] = jnp.concatenate([tw[2 * m, 2:6, :], tw[2 * m + 1, 2:6, :]], axis=0)

    @pl.when(s > 0)
    def _():
        up_top.wait_send()

    @pl.when(s < NQ - 1)
    def _():
        down_bot.wait_send()

    @pl.when(has_prev)
    def _():
        mid_prev.wait_send()
        bot_prev.wait_send()


    @pl.when(has_next)
    def _():
        remote(sec.at[0, pl.ds(0, UP)], fb, s_f, r_f.at[0], jnp.minimum(k + 1, NC - 1), s).wait_send()

    @pl.when(has_prev)
    def _():
        remote(sec.at[0, pl.ds(UP, LOW)], jb, s_j, r_j.at[0], jnp.maximum(k - 1, 0), s).wait_send()

    @pl.when(s < NQ - 1)
    def _():
        to_next.wait_send()

    @pl.when(s > 0)
    def _():
        to_prev.wait_send()

    @pl.when(has_next)
    def _():
        all_of(bdh, NQ, s_bh, r_bh).wait_send()

    all_of(gf, NQ - 1, s_g.at[0], r_g.at[0]).wait_send()
    all_of(gb, NQ - 1, s_g.at[1], r_g.at[1]).wait_send()
    all_of(bm, NQ - 1, s_bm, r_bm).wait_send()
    all_of(bdo, NQ - 1, s_bo, r_bo).wait_send()

    @pl.when(k == 0)
    def _():
        all_of(bdh, NQ - 1, s_ba, r_bh).wait_send()

    all_of(tw, NQ - 1, s_tw, r_tw).wait_send()

    for i in range(ITERATIONS - 1):
        @pl.when(has_next)
        def _():
            cp_copy(i).wait_send()

        @pl.when(has_prev)
        def _():
            cn_copy(i).wait_send()

    for kk in range(1, NC):
        @pl.when(kk > k)
        def _():
            ew_copy(kk, k).wait_send()


def solution(mesh):
    c, rows, split, mix = tables()

    def body(sections, anchor):
        v = pltpu.VMEM
        dma = pltpu.SemaphoreType.DMA
        row = v((1, COLS), F32)
        win = v((NQ, 8, 128), F32)
        scratch = [
            v((ROWS, COLS), BF16), v((UP, COLS), BF16), v((LOW, COLS), BF16), v((LOW, COLS), BF16),
            v((ROWS + 16, COLS + 2 * PAD), F32), v((LOW + 16, COLS + 2 * PAD), F32),
            v((ROWS, COLS), F32), v((ROWS, COLS), F32),
            v((COLS, 128), BF16), v((COLS, 256), BF16),
            v((3, 80, ROWS), BF16), v((32, ROWS), BF16), v((ROWS, 128), BF16),
            v((CH, 256), F32), v((2, 5, ROWS, CH), BF16), v((2, 96, CH), BF16), v((96, CH), F32),
            v((2, 2, ROWS, CH), BF16), v((2, 64, CH), BF16),
            v((32, COLS + 2 * PAD), F32), v((64, COLS), BF16), v((32, 128), F32),
            v((2, 8, 128), F32), v((4, 8, 128), F32),
            row, row, row, row, row, row, row,
            v((96, 128), F32), v((2, 96, 128), F32), v((96, 128), F32), v((96, 128), F32),
            v((24, 128), F32), v((80, 128), BF16), v((NQ, 24, 128), F32), v((NQ, 80, 128), BF16),
            v((16, GRID, 128), F32), v((16, GRID, 128), F32),
            v((24, 128), F32), v((NQ, 24, 128), F32), v((8, 128), F32), v((8, 128), F32), v((8, 128), F32), win, win,
            v((GRID + 16, 128), F32), v((3, GRID, 128), F32), v((3, GRID, 128), F32), v((3, GRID, 128), F32),
            v((8, 128), F32), v((NC - 1, 8, 128), F32), v((8, 128), F32), v((NQ, 8, 128), F32),
            dma((4,)), dma((4,)), dma((2,)), pltpu.SemaphoreType.REGULAR((4,)),
            dma, dma((NX,)), dma, dma((NX,)), dma((4,)), dma((4,)), dma((2,)), dma((2,)),
            dma((2,)), dma((2,)), dma, dma, dma, dma, dma, dma, dma,
            dma((3,)), dma((3,)), dma((3,)), dma((3,)), dma((NC,)), dma((NC,)), dma, dma,
        ]
        anywhere = pl.BlockSpec(memory_space=pl.ANY)
        inside = pl.BlockSpec(memory_space=pltpu.VMEM)
        return pl.pallas_call(
            kernel,
            out_shape=(
                pltpu.VMEM((1, ROWS, COLS), BF16),
                pltpu.VMEM((1, GRID, 2 * GRID), F32),
            ),
            in_specs=[anywhere] * 6,
            out_specs=(inside, inside),
            scratch_shapes=scratch,
            compiler_params=pltpu.CompilerParams(
                collective_id=0, has_side_effects=True, vmem_limit_bytes=64_900_000
            ),
        )(
            sections, anchor,
            jnp.asarray(c, BF16), jnp.asarray(rows, BF16), jnp.asarray(split, BF16), jnp.asarray(mix, BF16),
        )

    return jax.shard_map(
        body, mesh=mesh,
        in_specs=(P("chain", "quad", None), P("quad", None)),
        out_specs=(P("chain", "quad", None), P("chain", None, None)),
        check_vma=False,
    )
```

```python
import numpy as np
import jax
import jax.numpy as jnp
from jax import lax
from jax.experimental import pallas as pl
from jax.experimental.pallas import tpu as pltpu
from jax.sharding import PartitionSpec as P

GRID = 64
ITERATIONS = 4
EPS = 1e-6
SMOOTHING = 0.25
MESH = pl.DeviceIdType.MESH
F32 = jnp.float32
BF16 = jnp.bfloat16

ROWS = 256
COLS = 4096
UP = 160
LOW = ROWS - UP
CH = 256
NCH = COLS // CH
CX = 512
NX = COLS // CX
HOOK = 3
PAD = 128
NC = 8
NQ = 16
PIXELS = float(4096 * 4096)


def weight(offset):
    d = np.abs(offset)
    near = 2.0 / 3.0 - d * d + 0.5 * d * d * d
    r = 2.0 - d
    far = r * r * r / 6.0
    return np.where(d < 1.0, near, np.where(d < 2.0, far, 0.0 * d)).astype(np.float32)


def bf(x):
    return np.asarray(jnp.asarray(x, jnp.float32).astype(BF16).astype(jnp.float32))


def hi_lo(x):
    hi = bf(x)
    return [hi, bf(x - hi)]


def tables():
    f = np.float32
    x = np.arange(COLS, dtype=f)
    c = weight((x[:, None] + f(0.5)) / f(64) - np.arange(GRID, dtype=f)[None, :] - f(0.5))
    c = np.concatenate([c, c], axis=1)
    y = np.arange(-1, ROWS + 1, dtype=f)
    ext = weight((y[:, None] + f(0.5)) / f(64) - (np.arange(8, dtype=f) - f(2))[None, :] - f(0.5)).T
    r = ext[:, 1:-1]
    pairs = np.zeros((4, 8, ROWS), f)
    for d in range(4):
        pairs[d, : 8 - d] = r[: 8 - d] * r[d:]
    step = 0.5 * (r - ext[:, 2:])
    rows = []
    for variant in range(3):
        e = ext.copy()
        if variant == 0:
            e[:, 0] = 0.0
        if variant == 2:
            e[:, -1] = 0.0
        slope = 0.5 * (e[:, :-2] - e[:, 2:])
        rows.append(np.concatenate([pairs.reshape(32, ROWS)] + hi_lo(r) + hi_lo(slope) + hi_lo(step), axis=0))
    top = (np.arange(ROWS) < UP).astype(f)[None]
    split = np.concatenate([h * top for h in hi_lo(r)] + [h * (1 - top) for h in hi_lo(r)], axis=0)
    hi = bf(r)
    mid = bf(r - hi)
    low = bf(r - hi - mid)
    mix = np.concatenate([hi, hi, hi, mid, mid, low, np.zeros((80, ROWS), f)], axis=0).T
    return c, np.stack(rows), split, mix


def kernel(
    sec, anc, cd_in, rt_in, sp_in, mx_in,
    reg, acc,
    ib, fb, jb, ab, i32, j32, lxb, lyb, cd, w1, rt, sp, mx,
    wb, qb, tb, gacc, qd, vb, ub, lhs, bdacc, sums, dsums,
    etop, ebot, emid, htop, hbot, jmid, jbot,
    gs, gn, gp, gt, gfs, gbs, gb2s, gf, gb, gb2, ga, gx, bms, bm, bds, bhs, baa, bdo, bdh,
    cpad, csend, cprev, cnext, ew_s, ew, tw_s, tw,
    sem_in, sem_c, sem_a, rounds,
    s_f, r_f, s_j, r_j, s_h, r_h, s_n, r_n, s_g, r_g, s_bm, r_bm,
    s_bo, r_bo, s_bh, r_bh, s_ba, s_cp, r_cp, s_cn, r_cn, s_ew, r_ew, s_tw, r_tw,
):
    k = lax.axis_index("chain")
    s = lax.axis_index("quad")
    has_prev = k > 0
    has_next = k < NC - 1

    def remote(src, dst, ss, rs, kk, qq):
        return pltpu.make_async_remote_copy(
            src_ref=src, dst_ref=dst, send_sem=ss, recv_sem=rs,
            device_id={"chain": kk, "quad": qq}, device_id_type=MESH,
        )

    edge_rows = [(0, 16), (UP - 16, 16), (ROWS - 16, 16)]
    inner_rows = [(16, UP - 32), (UP, LOW - 16)]

    def in_copy(i):
        at, n = (edge_rows + inner_rows)[i]
        return pltpu.make_async_copy(sec.at[0, pl.ds(at, n)], ib.at[pl.ds(at, n)], sem_in.at[i])

    for i in range(3):
        in_copy(i).start()
    consts = [
        pltpu.make_async_copy(cd_in, cd, sem_c.at[0]),
        pltpu.make_async_copy(rt_in, rt, sem_c.at[1]),
        pltpu.make_async_copy(sp_in, sp, sem_c.at[2]),
        pltpu.make_async_copy(mx_in, mx, sem_c.at[3]),
    ]
    for d in consts:
        d.start()
    for i in range(3, 5):
        in_copy(i).start()
    anc_copies = [
        pltpu.make_async_copy(anc.at[pl.ds(0, UP)], fb, sem_a.at[0]),
        pltpu.make_async_copy(anc.at[pl.ds(UP, LOW)], ab, sem_a.at[1]),
    ]

    @pl.when(k == 0)
    def _():
        for d in anc_copies:
            d.start()

    barrier = pltpu.get_barrier_semaphore()

    qz = lax.div(s, 4)
    qy = lax.rem(s, 4)

    def greet(sem, q):
        pl.semaphore_signal(sem, inc=1, device_id={"chain": k, "quad": q}, device_id_type=MESH)

    def hello_quad(sem):
        for d in (1, 3):
            greet(sem, 4 * qz + lax.rem(qy + d, 4))
            greet(sem, 4 * lax.rem(qz + d, 4) + qy)

    far_next = (qy == 3) & (s < NQ - 1)
    far_prev = (qy == 0) & (s > 0)

    def hello_chain(sem, step):
        for sign in (1, -1):
            kk = k + sign * step

            @pl.when((kk >= 0) & (kk < NC))
            def _():
                pl.semaphore_signal(sem, inc=1, device_id={"chain": kk, "quad": s}, device_id_type=MESH)

    def on_chain(step):
        one = jnp.int32(1)
        zero = jnp.int32(0)
        return jnp.where(k >= step, one, zero) + jnp.where(k + step < NC, one, zero)

    hello_quad(barrier)

    @pl.when(far_next)
    def _():
        greet(barrier, s + 1)

    @pl.when(far_prev)
    def _():
        greet(barrier, s - 1)

    hello_chain(barrier, 1)

    i32[:, :PAD] = jnp.zeros((ROWS + 16, PAD), F32)
    i32[:, PAD + COLS :] = jnp.zeros((ROWS + 16, PAD), F32)
    j32[:, :PAD] = jnp.zeros((LOW + 16, PAD), F32)
    j32[:, PAD + COLS :] = jnp.zeros((LOW + 16, PAD), F32)
    ub[:, :PAD] = jnp.zeros((32, PAD), F32)
    ub[:, PAD + COLS :] = jnp.zeros((32, PAD), F32)
    sums[...] = jnp.zeros_like(sums)
    qb[1] = jnp.zeros((5, ROWS, CH), BF16)
    tb[0] = jnp.zeros((96, CH), BF16)
    gacc[...] = jnp.zeros_like(gacc)
    qd[...] = jnp.zeros_like(qd)
    vb[...] = jnp.zeros_like(vb)
    dsums[...] = jnp.zeros_like(dsums)
    bdacc[...] = jnp.zeros_like(bdacc)
    cpad[...] = jnp.zeros_like(cpad)

    @pl.when(s == 0)
    def _():
        htop[...] = jnp.zeros_like(htop)
        gn[0] = jnp.zeros((96, 128), F32)

    @pl.when(s == NQ - 1)
    def _():
        hbot[...] = jnp.zeros_like(hbot)
        gn[1] = jnp.zeros((96, 128), F32)

    @pl.when(k == 0)
    def _():
        cprev[...] = jnp.zeros_like(cprev)

    @pl.when(k == NC - 1)
    def _():
        jb[...] = jnp.zeros_like(jb)
        jmid[...] = jnp.zeros_like(jmid)
        jbot[...] = jnp.zeros_like(jbot)
        cnext[...] = jnp.zeros_like(cnext)

    for j in range(NC - 1):
        @pl.when(j >= k)
        def _():
            ew[j] = jnp.zeros((8, 128), F32)

    far = jnp.where(far_next, jnp.int32(1), jnp.int32(0)) + jnp.where(far_prev, jnp.int32(1), jnp.int32(0))
    pl.semaphore_wait(barrier, 4 + far + on_chain(1))
    hello_quad(rounds.at[0])

    def f_copy(c):
        at = pl.multiple_of(c * CX, CX)
        return remote(
            sec.at[0, pl.ds(0, UP), pl.ds(at, CX)], fb.at[:, pl.ds(at, CX)],
            s_f, r_f.at[c], jnp.minimum(k + 1, NC - 1), s,
        )

    def j_copy(c):
        at = pl.multiple_of(c * CX, CX)
        return remote(
            sec.at[0, pl.ds(UP, LOW), pl.ds(at, CX)], jb.at[:, pl.ds(at, CX)],
            s_j, r_j.at[c], jnp.maximum(k - 1, 0), s,
        )

    @pl.loop(0, NX)
    def _(c):
        @pl.when(has_next)
        def _():
            f_copy(c).start()

        @pl.when(has_prev)
        def _():
            j_copy(c).start()

    up_top = remote(etop, hbot, s_h.at[0], r_h.at[0], k, jnp.maximum(s - 1, 0))
    down_bot = remote(ebot, htop, s_h.at[1], r_h.at[1], k, jnp.minimum(s + 1, NQ - 1))
    mid_prev = remote(emid, jmid, s_h.at[2], r_h.at[2], jnp.maximum(k - 1, 0), s)
    bot_prev = remote(hbot, jbot, s_h.at[3], r_h.at[3], jnp.maximum(k - 1, 0), s)

    for i in range(3):
        in_copy(i).wait()
    etop[...] = ib[0:16, :].astype(F32)[0:1]
    ebot[...] = ib[ROWS - 16 : ROWS, :].astype(F32)[15:16]
    emid[...] = ib[UP - 16 : UP, :].astype(F32)[15:16]

    @pl.when(s > 0)
    def _():
        up_top.start()

    @pl.when(s < NQ - 1)
    def _():
        down_bot.start()

    @pl.when(has_prev)
    def _():
        mid_prev.start()

    for d in consts:
        d.wait()
    lane = lax.broadcasted_iota(jnp.int32, (8, 128), 1)

    v = cd[pl.ds(CH, CH), :].astype(F32)
    ln = lax.broadcasted_iota(jnp.int32, (CH, 128), 1)
    knot = jnp.where(ln < GRID, ln, ln - GRID)
    for h in range(2):
        a = v if h == 0 else pltpu.roll(v, 128 - 2 * h, 1)
        b = pltpu.roll(v, 127 - 2 * h, 1)
        wb[:, h * 128 : (h + 1) * 128] = v * jnp.where(ln < GRID, a, b)

    @pl.loop(0, NCH // 4)
    def _(c4):
      for c in [4 * c4 + u for u in range(4)]:
        at = pl.multiple_of(c * CH, CH)
        for h in range(2):
            partner = knot + jnp.where(ln < GRID, 2 * h, 2 * h + 1)
            near = (jnp.abs(2 * (knot - 4 * c) - 3) < 16) & (partner < GRID)
            t = pltpu.roll(wb[:, h * 128 : (h + 1) * 128], lax.rem(4 * c + 124, 128), 1)
            w1[pl.ds(at, CH), h * 128 : (h + 1) * 128] = jnp.where(near, t, 0.0).astype(BF16)

    variant = jnp.where(s == 0, 0, jnp.where(s == NQ - 1, 2, 1))
    RB = 32

    def spot(c):
        return pl.multiple_of(jnp.maximum(c, 0) * CH, CH)

    for i in range(3, 5):
        in_copy(i).wait()

    pl.semaphore_wait(rounds.at[0], 4)
    hello_quad(rounds.at[1])

    @pl.loop(0, NCH // 2)
    def _(p):
        for c in [2 * p, 2 * p + 1]:
            at = pl.multiple_of(c * CH, CH)
            u = jnp.dot(rt[variant, 32:64, :], ib[:, pl.ds(at, CH)], preferred_element_type=F32)
            ub[0:8, pl.ds(at + PAD, CH)] = u[0:8] + u[8:16]
            ub[8:16, pl.ds(at + PAD, CH)] = u[16:24] + u[24:32]
            s1 = jnp.zeros((8, CH), F32)
            s2 = jnp.zeros((8, CH), F32)
            for r in range(0, ROWS, RB):
                x = ib[r : r + RB, pl.ds(at, CH)].astype(F32)
                i32[8 + r : 8 + r + RB, pl.ds(at + PAD, CH)] = x
                for t in range(0, RB, 8):
                    xt = x[t : t + 8]
                    s1 = s1 + xt
                    s2 = s2 + xt * xt
            sums[0] = sums[0] + s1[:, :128] + s1[:, 128:]
            sums[1] = sums[1] + s2[:, :128] + s2[:, 128:]

    @pl.when(s < NQ - 1)
    def _():
        up_top.wait_recv()

    @pl.when(s > 0)
    def _():
        down_bot.wait_recv()

    @pl.when(has_prev)
    def _():
        bot_prev.start()

    i32[7:8, PAD : PAD + COLS] = htop[...]
    i32[8 + ROWS : 9 + ROWS, PAD : PAD + COLS] = hbot[...]

    pl.semaphore_wait(rounds.at[1], 4)
    hello_quad(rounds.at[2])

    def tally(i, d, x):
        a = jnp.zeros((8, CH), F32)
        b = jnp.zeros((8, CH), F32)
        for t in range(0, d.shape[0], 8):
            a = a + d[t : t + 8]
            b = b + d[t : t + 8] * x[t : t + 8]
        dsums[i] = dsums[i] + a[:, :128] + a[:, 128:]
        dsums[i + 1] = dsums[i + 1] + b[:, :128] + b[:, 128:]

    def pixels(at, slot, with_anchor):
        for r in range(0, ROWS, RB):
            mid = i32[8 + r : 8 + r + RB, pl.ds(at, CH + 2 * PAD)]
            x = mid[:, PAD : PAD + CH]
            right = pltpu.roll(mid, CH + 2 * PAD - 1, 1)[:, PAD : PAD + CH]
            left = pltpu.roll(mid, 1, 1)[:, PAD : PAD + CH]
            lx = right - left
            lxb[r : r + RB, pl.ds(at, CH)] = lx
            tall = i32[r : r + RB + 16, pl.ds(at + PAD, CH)]
            below = pltpu.roll(tall, RB + 15, 0)[8 : 8 + RB]
            above = pltpu.roll(tall, 1, 0)[8 : 8 + RB]
            ly = below - above
            lyb[r : r + RB, pl.ds(at, CH)] = ly
            qb[slot, 0, r : r + RB, :] = (lx * lx).astype(BF16)
            qb[slot, 3, r : r + RB, :] = (x * right).astype(BF16)
            qb[slot, 1, r : r + RB, :] = (lx * ly).astype(BF16)
            qb[slot, 2, r : r + RB, :] = (ly * ly).astype(BF16)
            qb[slot, 4, r : r + RB, :] = (x * below).astype(BF16)
            if with_anchor:
                src, rr = (fb, r) if r < UP else (ab, r - UP)
                d = src[rr : rr + RB, pl.ds(at, CH)].astype(F32) - x
                qd[slot, 0, r : r + RB, :] = (d * lx).astype(BF16)
                qd[slot, 1, r : r + RB, :] = (d * ly).astype(BF16)
                tally(0, d, x)

    def rows_out(at, slot, with_anchor):
        for i in range(3):
            tb[slot, 32 * i : 32 + 32 * i, :] = jnp.dot(
                rt[variant, 0:32, :], qb[slot, i], preferred_element_type=F32
            ).astype(BF16)
        z = jnp.dot(rt[variant, 32:48, :], qb[slot, 3], preferred_element_type=F32)
        ub[16:24, pl.ds(at + PAD, CH)] = z[0:8] + z[8:16]
        q = jnp.dot(rt[variant, 64:80, :], qb[slot, 4], preferred_element_type=F32)
        ub[24:32, pl.ds(at + PAD, CH)] = q[0:8] + q[8:16]
        if with_anchor:
            for i in range(2):
                v = jnp.dot(rt[variant, 32:48, :], qd[slot, i], preferred_element_type=F32)
                v = v[0:8] + v[8:16]
                hi = v.astype(BF16).astype(F32)
                vb[slot, 16 * i : 16 * i + 16, :] = jnp.concatenate([hi, v - hi], axis=0).astype(BF16)

    def columns_out(at, slot, with_anchor):
        gacc[...] = gacc[...] + jnp.dot(tb[slot], w1[pl.ds(at, CH), :], preferred_element_type=F32)
        if with_anchor:
            b = jnp.dot(vb[slot, 0:32, :], cd[pl.ds(at, CH), :], preferred_element_type=F32)
            bdacc[0:8] = bdacc[0:8] + b[0:8] + b[8:16]
            bdacc[16:24] = bdacc[16:24] + b[16:24] + b[24:32]

    def own_pass(with_anchor):
        @pl.loop(0, NCH // 2)
        def _(p):
            @pl.when(p == 5)
            def _():
                pl.semaphore_wait(rounds.at[2], 4)
                hello_chain(rounds.at[3], 1)

            for u in range(2):
                c = 2 * p + u
                columns_out(spot(c - 2), u, with_anchor)
                pixels(spot(c), u, with_anchor)
                rows_out(spot(c - 1), 1 - u, with_anchor)

        columns_out(spot(NCH - 2), 0, with_anchor)
        rows_out(spot(NCH - 1), 1, with_anchor)
        columns_out(spot(NCH - 1), 1, with_anchor)

    @pl.when(k > 0)
    def _():
        own_pass(False)

    @pl.when(k == 0)
    def _():
        for d in anc_copies:
            d.wait()
        own_pass(True)

    first = lane < GRID

    def swap(v):
        return pltpu.roll(v, GRID, 1)

    quarter = lax.broadcasted_iota(jnp.int32, (8, 128), 0)

    def pack(a, b):
        return jnp.where(quarter < 4, pltpu.roll(a, 6, 0), pltpu.roll(b, 2, 0))

    order = [(di, h) for di in range(2) for h in range(1)]
    order = order + [(di, h) for di in range(4) for h in range(2) if (di, h) not in order]
    slots = []
    for di, h in order:
        part = lambda q: 0.25 * gacc[32 * q + 8 * di : 32 * q + 8 * di + 8, 128 * h : 128 * h + 128]
        xx, xy, yy = part(0), part(1), part(2)
        slots.append(jnp.where(first, xx, swap(yy)))
        slots.append(jnp.where(first, swap(xx), yy))
        slots.append(xy)
    for i in range(12):
        a, b = slots[2 * i], slots[2 * i + 1]
        gs[8 * i : 8 * i + 8, :] = pack(a, b)
        gp[8 * i : 8 * i + 8, :] = pack(pltpu.roll(a, 4, 0), pltpu.roll(b, 4, 0))

    to_next = remote(gp, gn.at[0], s_n.at[0], r_n.at[0], k, jnp.minimum(s + 1, NQ - 1))
    to_prev = remote(gp, gn.at[1], s_n.at[1], r_n.at[1], k, jnp.maximum(s - 1, 0))

    @pl.when(s < NQ - 1)
    def _():
        to_next.start()

    @pl.when(s > 0)
    def _():
        to_prev.start()

    @pl.loop(0, NCH // 4)
    def _(c4):
      for c in [4 * c4 + u for u in range(4)]:
        at = pl.multiple_of(c * CH, CH)
        wide = ub[:, pl.ds(at, CH + 2 * PAD)]
        right = pltpu.roll(wide, CH + 2 * PAD - 1, 1)[:, PAD : PAD + CH]
        left = pltpu.roll(wide, 1, 1)[:, PAD : PAD + CH]
        x = wide[:, PAD : PAD + CH]
        v = jnp.concatenate(
            [0.5 * (right[0:8] - left[0:8]), x[8:16], 0.5 * (x[16:24] - left[16:24]), x[24:32]], axis=0
        )
        hi = v.astype(BF16)
        lhs[0:32, pl.ds(at, CH)] = hi
        lhs[32:64, pl.ds(at, CH)] = (v - hi.astype(F32)).astype(BF16)

    bb = jnp.dot(lhs[...], cd[...], preferred_element_type=F32)
    bb = bb[0:32] + bb[32:64]
    bms[0:8, :] = jnp.where(first, bb[16:24], bb[24:32])
    bms[8:16, :] = jnp.where(first, bb[0:8], bb[8:16])

    def fold(a, b):
        ra = jnp.sum(a, axis=0, keepdims=True)
        rb = jnp.sum(b, axis=0, keepdims=True)
        return jnp.where(quarter == 0, ra, jnp.where(quarter == 1, rb, 0.0))

    bms[16:24, :] = fold(sums[0], sums[1])
    bm[s] = bms[...]

    def bm_copy(to, slot):
        return remote(bms, bm.at[slot], s_bm, r_bm, k, to)

    @pl.loop(1, NQ)
    def _(d):
        bm_copy(lax.rem(s + d, NQ), s).start()

    def gf_copy(to, slot):
        return remote(gfs, gf.at[slot], s_g.at[0], r_g.at[0], k, to)

    def gb_copy(to, slot):
        return remote(gbs, gb.at[slot], s_g.at[1], r_g.at[1], k, to)

    def gb2_copy(to, slot):
        return remote(gb2s, gb2.at[slot], s_g.at[2], r_g.at[2], k, to)

    def spread_gram():
        @pl.when(s > 0)
        def _():
            to_next.wait_recv()

        @pl.when(s < NQ - 1)
        def _():
            to_prev.wait_recv()

        lower_rows = (quarter == 0) | (quarter == 1) | (quarter == 4) | (quarter == 5)
        for i in range(12):
            b8 = slice(8 * i, 8 * i + 8)
            gt[b8, :] = gs[b8, :] + jnp.where(lower_rows, gn[0, b8, :], gn[1, b8, :])
        gfs[...] = gt[0:24, :]
        gbs[...] = gt[24:72, :].astype(BF16)
        gb2s[...] = jnp.concatenate([gt[72:96, :], jnp.zeros((8, 128), F32)], axis=0).astype(BF16)
        gb2[s] = gb2s[...]
        gf[s] = gfs[...]
        gb[s] = gbs[...]

        @pl.loop(1, NQ)
        def _(d):
            to = lax.rem(s + d, NQ)
            gf_copy(to, s).start()

    @pl.when(has_next)
    def _():
        mid_prev.wait_recv()
        bot_prev.wait_recv()

    j32[7:8, PAD : PAD + COLS] = jmid[...]
    j32[8 + LOW : 9 + LOW, PAD : PAD + COLS] = jbot[...]

    def tuck(ref, at, a, b):
        ref[at : at + 1, :] = jnp.sum(a, axis=0, keepdims=True)
        ref[at + 1 : at + 2, :] = jnp.sum(b, axis=0, keepdims=True)

    def ba_copy(to, slot):
        return remote(baa, bdh.at[slot], s_ba, r_bh, k, to)

    def cross_rows(slot):
        v = jnp.concatenate(
            [jnp.dot(sp[...], qd[slot, i], preferred_element_type=F32) for i in range(2)], axis=0
        )
        v = jnp.concatenate(
            [v[0:8] + v[8:16], v[16:24] + v[24:32], v[32:40] + v[40:48], v[48:56] + v[56:64]], axis=0
        )
        hi = v.astype(BF16)
        vb[slot, 0:32, :] = hi
        vb[slot, 32:64, :] = (v - hi.astype(F32)).astype(BF16)

    def cross_columns(at, slot):
        b = jnp.dot(vb[slot], cd[pl.ds(at, CH), :], preferred_element_type=F32)
        bdacc[...] = bdacc[...] + b[0:32] + b[32:64]

    def both(at, slot, upper):
        for r in range(0, UP if upper else 0, RB):
            x = i32[8 + r : 8 + r + RB, pl.ds(at + PAD, CH)]
            d = fb[r : r + RB, pl.ds(at, CH)].astype(F32) - x
            qd[slot, 0, r : r + RB, :] = (d * lxb[r : r + RB, pl.ds(at, CH)]).astype(BF16)
            qd[slot, 1, r : r + RB, :] = (d * lyb[r : r + RB, pl.ds(at, CH)]).astype(BF16)
            tally(0, d, x)
        for r in range(0, LOW, RB):
            rr = UP + r
            mid = j32[8 + r : 8 + r + RB, pl.ds(at, CH + 2 * PAD)]
            x = mid[:, PAD : PAD + CH]
            right = pltpu.roll(mid, CH + 2 * PAD - 1, 1)[:, PAD : PAD + CH]
            left = pltpu.roll(mid, 1, 1)[:, PAD : PAD + CH]
            tall = j32[r : r + RB + 16, pl.ds(at + PAD, CH)]
            below = pltpu.roll(tall, RB + 15, 0)[8 : 8 + RB]
            above = pltpu.roll(tall, 1, 0)[8 : 8 + RB]
            d = i32[8 + rr : 8 + rr + RB, pl.ds(at + PAD, CH)] - x
            qd[slot, 0, rr : rr + RB, :] = (d * (right - left)).astype(BF16)
            qd[slot, 1, rr : rr + RB, :] = (d * (below - above)).astype(BF16)
            tally(2, d, x)

    def cross(upper):
        @pl.loop(0, NCH // 2)
        def _(p):
            @pl.when(p == HOOK)
            def _():
                spread_gram()

            arrive(p + 1)
            for u in range(2):
                c = 2 * p + u
                cross_columns(spot(c - 2), u)
                both(spot(c), u, upper)
                cross_rows(1 - u)

        cross_columns(spot(NCH - 2), 0)
        cross_rows(1)
        cross_columns(spot(NCH - 1), 1)

    @pl.when(k == 0)
    def _():
        baa[0:8, :] = 0.5 * jnp.where(first, bdacc[0:8], bdacc[16:24])
        bdacc[...] = jnp.zeros_like(bdacc)
        qd[...] = jnp.zeros_like(qd)
        vb[...] = jnp.zeros_like(vb)

        @pl.loop(1, NQ)
        def _(d):
            ba_copy(lax.rem(s + d, NQ), s).start()

        bdh[s] = baa[...]

    def arrive(piece):
        @pl.when(has_prev & (piece < NX))
        def _():
            f_copy(piece).wait_recv()

        @pl.when(has_next & (piece < NX))
        def _():
            j_copy(piece).wait_recv()

        at = pl.multiple_of(jnp.minimum(piece, NX - 1) * CX, CX)
        j32[8 : 8 + LOW, pl.ds(at + PAD, CX)] = jb[:, pl.ds(at, CX)].astype(F32)

    arrive(jnp.int32(0))

    @pl.when(k > 0)
    def _():
        cross(True)

    @pl.when(k == 0)
    def _():
        cross(False)

    bds[0:8, :] = 0.5 * jnp.where(first, bdacc[0:8], bdacc[16:24])
    bhs[0:8, :] = 0.5 * jnp.where(first, bdacc[8:16], bdacc[24:32])
    tuck(bds, 6, dsums[0], dsums[1])
    tuck(bhs, 0, dsums[2], dsums[3])

    def bo_copy(to, slot):
        return remote(bds, bdo.at[slot], s_bo, r_bo, k, to)

    def bh_copy(to, slot):
        return remote(bhs, bdh.at[slot], s_bh, r_bh, jnp.minimum(k + 1, NC - 1), to)

    pl.semaphore_wait(rounds.at[3], on_chain(1))
    hello_chain(rounds.at[4], 2)

    @pl.loop(0, NQ)
    def _(d):
        to = lax.rem(s + d, NQ)

        @pl.when(has_next)
        def _():
            bh_copy(to, s).start()

        @pl.when(d > 0)
        def _():
            bo_copy(to, s).start()

    bdo[s] = bds[...]

    @pl.loop(1, NQ)
    def _(d):
        gb_copy(lax.rem(s + d, NQ), s).start()
        gb2_copy(lax.rem(s + d, NQ), s).start()


    def all_of(ref, n, ss, rs):
        return remote(ref.at[pl.ds(0, n)], ref.at[pl.ds(0, n)], ss, rs, k, lax.rem(s + 1, NQ))

    all_of(bm, NQ - 1, s_bm, r_bm).wait_recv()

    row = lax.broadcasted_iota(jnp.int32, (GRID, 128), 0)

    def merge(parts):
        even = jnp.concatenate(parts[0::2], axis=0)
        odd = jnp.concatenate(parts[1::2], axis=0)
        even = jnp.where(row < GRID - 2, pltpu.roll(even, GRID - 2, 0), 0.0)
        odd = jnp.where(row >= 2, pltpu.roll(odd, 2, 0), 0.0)
        return even + odd

    b_i = merge([bm[p, 0:8, :] for p in range(NQ)])
    b_1 = merge([bm[p, 8:16, :] for p in range(NQ)])

    def total(v):
        return jnp.sum(v, axis=(0, 1), keepdims=True)

    tot = bm[0, 16:24, :]
    for p in range(1, NQ):
        tot = tot + bm[p, 16:24, :]
    sum_i = total(tot[0:1])
    sum_ii = total(tot[1:2])

    all_of(bdo, NQ - 1, s_bo, r_bo).wait_recv()

    @pl.when(has_prev)
    def _():
        all_of(bdh, NQ, s_bh, r_bh).wait_recv()

    @pl.when(k == 0)
    def _():
        all_of(bdh, NQ - 1, s_ba, r_bh).wait_recv()

    parts = []
    tot_d = None
    tot_di = None
    for p in range(NQ):
        up, dn = bdo[p], bdh[p]
        parts.append(jnp.where(quarter < 6, up, 0.0) + jnp.where((quarter >= 2) | (k == 0), dn, 0.0))
        a = up[6:7] + jnp.where(k == 0, 0.0, dn[0:1])
        b = up[7:8] + jnp.where(k == 0, 0.0, dn[1:2])
        tot_d = a if p == 0 else tot_d + a
        tot_di = b if p == 0 else tot_di + b
    b_f = b_i + merge(parts)
    sum_f = sum_i + total(tot_d)
    sum_fi = sum_ii + total(tot_di)
    mean_f = sum_f * (1.0 / PIXELS)

    def apply_gram(c):
        cl = [c] + [pltpu.roll(c, 128 - d, 1) for d in range(1, 4)]
        cs = swap(c)
        csl = [cs] + [pltpu.roll(cs, 128 - d, 1) for d in range(1, 4)]
        out = None
        lacc = [None] * 4

        def add(a, b):
            return b if a is None else a + b

        for di in range(4):
            racc = None
            for dj in range(4):
                a = ga[4 * di + dj]
                x = gx[4 * di + dj]
                up = (lambda v: v) if di == 0 else (lambda v: pltpu.roll(v, GRID - di, 0))
                out = add(out, a * up(cl[dj]) + x * up(csl[dj]))
                if dj:
                    lacc[dj] = add(lacc[dj], a * up(c) + x * up(cs))
                if di:
                    racc = add(racc, a * cl[dj] + x * csl[dj])
                if di and dj:
                    racc = racc + pltpu.roll(a * c + x * cs, dj, 1)
            if di:
                out = out + pltpu.roll(racc, di, 0)
        for dj in range(1, 4):
            out = out + pltpu.roll(lacc[dj], dj, 1)
        return out

    def direction(c):
        if c is None:
            mean_w = sum_i * (1.0 / PIXELS)
            sq = sum_ii
            cross = sum_fi
            b_w = b_i
        else:
            h = apply_gram(c)
            mean_w = (sum_i + total(c * b_1)) * (1.0 / PIXELS)
            sq = sum_ii + total(c * (2.0 * b_i + h))
            cross = sum_fi + total(c * b_f)
            b_w = b_i + h
        var = sq - PIXELS * mean_w * mean_w
        cov = cross - PIXELS * mean_f * mean_w
        den = jnp.sqrt(var + EPS)
        ratio = cov / den / (var + EPS)
        grad = PIXELS * ((b_f - mean_f * b_1) / den - ratio * (b_w - mean_w * b_1))
        mag = total(grad * grad) * (1.0 / (GRID * 2 * GRID))
        return grad / jnp.sqrt(mag + EPS)

    rate = 1.0 / ITERATIONS

    def cp_copy(i):
        return remote(csend.at[i], cprev.at[i], s_cp.at[i], r_cp.at[i], jnp.minimum(k + 1, NC - 1), s)

    def cn_copy(i):
        return remote(csend.at[i], cnext.at[i], s_cn.at[i], r_cn.at[i], jnp.maximum(k - 1, 0), s)

    def exchange(i, c):
        csend[i] = c

        @pl.when(has_next)
        def _():
            cp_copy(i).start()

        @pl.when(has_prev)
        def _():
            cn_copy(i).start()

    def receive(i):
        @pl.when(has_prev)
        def _():
            cp_copy(i).wait_recv()

        @pl.when(has_next)
        def _():
            cn_copy(i).wait_recv()

    c = rate * direction(None)
    exchange(0, c)

    pl.semaphore_wait(rounds.at[4], on_chain(2))
    hello_chain(rounds.at[5], 4)

    all_of(gf, NQ - 1, s_g.at[0], r_g.at[0]).wait_recv()
    all_of(gb, NQ - 1, s_g.at[1], r_g.at[1]).wait_recv()
    all_of(gb2, NQ - 1, s_g.at[2], r_g.at[2]).wait_recv()
    for m in range(8):
        ab_f = [gf[2 * m + j] for j in range(2)]
        ab_b = [
            jnp.concatenate([gb[2 * m + j].astype(F32), gb2[2 * m + j].astype(F32)], axis=0) for j in range(2)
        ]
        for i in range(12):
            src = ab_f if i < 3 else ab_b
            o = 8 * i if i < 3 else 8 * (i - 3)
            a, b = src[0][o : o + 8], src[1][o : o + 8]
            pair = (
                jnp.where(quarter < 4, a, pltpu.roll(b, 4, 0)),
                jnp.where(quarter < 4, pltpu.roll(a, 4, 0), b),
            )
            for j in range(2):
                (di, h), which = order[(2 * i + j) // 3], (2 * i + j) % 3
                v = pair[j]
                if di and m == 7:
                    v = jnp.where(quarter < 8 - di, v, 0.0)
                m8 = slice(8 * m, 8 * m + 8)
                if which < 2:
                    ga[4 * di + 2 * h + which, m8, :] = v
                else:
                    o2 = swap(v)
                    gx[4 * di + 2 * h, m8, :] = jnp.where(first, v, o2)
                    gx[4 * di + 2 * h + 1, m8, :] = jnp.where(first, o2, v)

    for i in range(1, ITERATIONS - 1):
        step = c + rate * direction(c)
        receive(i - 1)
        c = step + SMOOTHING * (cprev[i - 1] - 2.0 * c + cnext[i - 1])
        exchange(i, c)
    step = c + rate * direction(c)

    base = pl.multiple_of(lax.div(4 * s + 6, 8) * 8, 8)
    even = lax.rem(s, 2) == 0

    def window(v):
        cpad[8 : 8 + GRID] = v
        w = cpad[pl.ds(base, 16), :]
        return jnp.where(even, w[6:14], w[2:10])

    cw = window(c)
    mine = window(step) - jnp.where(k == 0, SMOOTHING, 0.0) * cw
    ew_s[...] = mine

    pl.semaphore_wait(rounds.at[5], on_chain(4))

    def ew_copy(to, slot):
        return remote(ew_s, ew.at[slot], s_ew.at[to], r_ew.at[slot], to, s)

    for kk in range(1, NC):
        @pl.when(kk > k)
        def _():
            ew_copy(kk, k).start()

    receive(ITERATIONS - 2)
    nxt = window(cnext[ITERATIONS - 2])
    own = mine + SMOOTHING * (nxt - cw)

    for kk in range(NC - 1):
        @pl.when(kk < k)
        def _():
            ew_copy(kk, kk).wait_recv()

    t = ew[0]
    for kk in range(1, NC - 1):
        t = t + ew[kk]
    t = t + own
    tw_s[...] = t

    def tw_copy(to, slot):
        return remote(tw_s, tw.at[slot], s_tw, r_tw, k, to)

    @pl.loop(1, NQ)
    def _(d):
        tw_copy(lax.rem(s + d, NQ), s).start()

    tw[s] = t

    hi = t.astype(BF16)
    rest = t - hi.astype(F32)
    mid = rest.astype(BF16)
    low = (rest - mid.astype(F32)).astype(BF16)
    stack = jnp.concatenate(
        [v.astype(F32) for v in (hi, mid, low, hi, mid, hi)] + [jnp.zeros((80, 128), F32)], axis=0
    ).astype(BF16)
    mixed = jnp.dot(mx[...], stack, preferred_element_type=F32).astype(BF16).astype(F32) * 0.5
    big_first = lax.broadcasted_iota(jnp.int32, (ROWS, 128), 1) < GRID
    mixed_x = jnp.where(big_first, mixed, 0.0).astype(BF16)
    mixed_y = jnp.where(big_first, 0.0, mixed).astype(BF16)
    dims = (((1,), (1,)), ((), ()))

    @pl.loop(0, NCH // 8)
    def _(p):
        for u in range(8):
            at = pl.multiple_of((8 * p + u) * CH, CH)
            table = cd[pl.ds(at, CH), :]
            sx = lax.dot_general(mixed_x, table, dims, preferred_element_type=F32)
            sy = lax.dot_general(mixed_y, table, dims, preferred_element_type=F32)
            v = (
                i32[8 : 8 + ROWS, pl.ds(at + PAD, CH)]
                + sx * lxb[:, pl.ds(at, CH)]
                + sy * lyb[:, pl.ds(at, CH)]
            )
            reg[0, :, pl.ds(at, CH)] = v.astype(BF16)

    all_of(tw, NQ - 1, s_tw, r_tw).wait_recv()

    for m in range(8):
        acc[0, 8 * m : 8 * m + 8, :] = jnp.concatenate([tw[2 * m, 2:6, :], tw[2 * m + 1, 2:6, :]], axis=0)

    @pl.when(s > 0)
    def _():
        up_top.wait_send()

    @pl.when(s < NQ - 1)
    def _():
        down_bot.wait_send()

    @pl.when(has_prev)
    def _():
        mid_prev.wait_send()
        bot_prev.wait_send()


    @pl.when(has_next)
    def _():
        remote(sec.at[0, pl.ds(0, UP)], fb, s_f, r_f.at[0], jnp.minimum(k + 1, NC - 1), s).wait_send()

    @pl.when(has_prev)
    def _():
        remote(sec.at[0, pl.ds(UP, LOW)], jb, s_j, r_j.at[0], jnp.maximum(k - 1, 0), s).wait_send()

    @pl.when(s < NQ - 1)
    def _():
        to_next.wait_send()

    @pl.when(s > 0)
    def _():
        to_prev.wait_send()

    @pl.when(has_next)
    def _():
        all_of(bdh, NQ, s_bh, r_bh).wait_send()

    all_of(gf, NQ - 1, s_g.at[0], r_g.at[0]).wait_send()
    all_of(gb, NQ - 1, s_g.at[1], r_g.at[1]).wait_send()
    all_of(gb2, NQ - 1, s_g.at[2], r_g.at[2]).wait_send()
    all_of(bm, NQ - 1, s_bm, r_bm).wait_send()
    all_of(bdo, NQ - 1, s_bo, r_bo).wait_send()

    @pl.when(k == 0)
    def _():
        all_of(bdh, NQ - 1, s_ba, r_bh).wait_send()

    all_of(tw, NQ - 1, s_tw, r_tw).wait_send()

    for i in range(ITERATIONS - 1):
        @pl.when(has_next)
        def _():
            cp_copy(i).wait_send()

        @pl.when(has_prev)
        def _():
            cn_copy(i).wait_send()

    for kk in range(1, NC):
        @pl.when(kk > k)
        def _():
            ew_copy(kk, k).wait_send()


def solution(mesh):
    c, rows, split, mix = tables()

    def body(sections, anchor):
        v = pltpu.VMEM
        dma = pltpu.SemaphoreType.DMA
        row = v((1, COLS), F32)
        win = v((NQ, 8, 128), F32)
        scratch = [
            v((ROWS, COLS), BF16), v((UP, COLS), BF16), v((LOW, COLS), BF16), v((LOW, COLS), BF16),
            v((ROWS + 16, COLS + 2 * PAD), F32), v((LOW + 16, COLS + 2 * PAD), F32),
            v((ROWS, COLS), F32), v((ROWS, COLS), F32),
            v((COLS, 128), BF16), v((COLS, 256), BF16),
            v((3, 80, ROWS), BF16), v((32, ROWS), BF16), v((ROWS, 128), BF16),
            v((CH, 256), F32), v((2, 5, ROWS, CH), BF16), v((2, 96, CH), BF16), v((96, CH), F32),
            v((2, 2, ROWS, CH), BF16), v((2, 64, CH), BF16),
            v((32, COLS + 2 * PAD), F32), v((64, COLS), BF16), v((32, 128), F32),
            v((2, 8, 128), F32), v((4, 8, 128), F32),
            row, row, row, row, row, row, row,
            v((96, 128), F32), v((2, 96, 128), F32), v((96, 128), F32), v((96, 128), F32),
            v((24, 128), F32), v((48, 128), BF16), v((32, 128), BF16),
            v((NQ, 24, 128), F32), v((NQ, 48, 128), BF16), v((NQ, 32, 128), BF16),
            v((16, GRID, 128), F32), v((16, GRID, 128), F32),
            v((24, 128), F32), v((NQ, 24, 128), F32), v((8, 128), F32), v((8, 128), F32), v((8, 128), F32), win, win,
            v((GRID + 16, 128), F32), v((3, GRID, 128), F32), v((3, GRID, 128), F32), v((3, GRID, 128), F32),
            v((8, 128), F32), v((NC - 1, 8, 128), F32), v((8, 128), F32), v((NQ, 8, 128), F32),
            dma((5,)), dma((4,)), dma((2,)), pltpu.SemaphoreType.REGULAR((6,)),
            dma, dma((NX,)), dma, dma((NX,)), dma((4,)), dma((4,)), dma((2,)), dma((2,)),
            dma((3,)), dma((3,)), dma, dma, dma, dma, dma, dma, dma,
            dma((3,)), dma((3,)), dma((3,)), dma((3,)), dma((NC,)), dma((NC,)), dma, dma,
        ]
        anywhere = pl.BlockSpec(memory_space=pl.ANY)
        inside = pl.BlockSpec(memory_space=pltpu.VMEM)
        return pl.pallas_call(
            kernel,
            out_shape=(
                pltpu.VMEM((1, ROWS, COLS), BF16),
                pltpu.VMEM((1, GRID, 2 * GRID), F32),
            ),
            in_specs=[anywhere] * 6,
            out_specs=(inside, inside),
            scratch_shapes=scratch,
            compiler_params=pltpu.CompilerParams(
                collective_id=0, has_side_effects=True, vmem_limit_bytes=64_900_000
            ),
        )(
            sections, anchor,
            jnp.asarray(c, BF16), jnp.asarray(rows, BF16), jnp.asarray(split, BF16), jnp.asarray(mix, BF16),
        )

    return jax.shard_map(
        body, mesh=mesh,
        in_specs=(P("chain", "quad", None), P("quad", None)),
        out_specs=(P("chain", "quad", None), P("chain", None, None)),
        check_vma=False,
    )
```

```python
import numpy as np
import jax
import jax.numpy as jnp
from jax import lax
from jax.experimental import pallas as pl
from jax.experimental.pallas import tpu as pltpu
from jax.sharding import PartitionSpec as P

GRID = 64
ITERATIONS = 4
EPS = 1e-6
SMOOTHING = 0.25
MESH = pl.DeviceIdType.MESH
F32 = jnp.float32
BF16 = jnp.bfloat16

ROWS = 256
COLS = 4096
UP = 160
LOW = ROWS - UP
CH = 256
NCH = COLS // CH
CX = 512
NX = COLS // CX
HOOK = 3
PAD = 128
NC = 8
NQ = 16
PIXELS = float(4096 * 4096)


def weight(offset):
    d = np.abs(offset)
    near = 2.0 / 3.0 - d * d + 0.5 * d * d * d
    r = 2.0 - d
    far = r * r * r / 6.0
    return np.where(d < 1.0, near, np.where(d < 2.0, far, 0.0 * d)).astype(np.float32)


def bf(x):
    return np.asarray(jnp.asarray(x, jnp.float32).astype(BF16).astype(jnp.float32))


def hi_lo(x):
    hi = bf(x)
    return [hi, bf(x - hi)]


def tables():
    f = np.float32
    x = np.arange(COLS, dtype=f)
    c = weight((x[:, None] + f(0.5)) / f(64) - np.arange(GRID, dtype=f)[None, :] - f(0.5))
    c = np.concatenate([c, c], axis=1)
    y = np.arange(-1, ROWS + 1, dtype=f)
    ext = weight((y[:, None] + f(0.5)) / f(64) - (np.arange(8, dtype=f) - f(2))[None, :] - f(0.5)).T
    r = ext[:, 1:-1]
    pairs = np.zeros((4, 8, ROWS), f)
    for d in range(4):
        pairs[d, : 8 - d] = r[: 8 - d] * r[d:]
    step = 0.5 * (r - ext[:, 2:])
    rows = []
    for variant in range(3):
        e = ext.copy()
        if variant == 0:
            e[:, 0] = 0.0
        if variant == 2:
            e[:, -1] = 0.0
        slope = 0.5 * (e[:, :-2] - e[:, 2:])
        rows.append(np.concatenate([pairs.reshape(32, ROWS)] + hi_lo(r) + hi_lo(slope) + hi_lo(step), axis=0))
    top = (np.arange(ROWS) < UP).astype(f)[None]
    split = np.concatenate([h * top for h in hi_lo(r)] + [h * (1 - top) for h in hi_lo(r)], axis=0)
    hi = bf(r)
    mid = bf(r - hi)
    low = bf(r - hi - mid)
    mix = np.concatenate([hi, hi, hi, mid, mid, low, np.zeros((80, ROWS), f)], axis=0).T
    return c, np.stack(rows), split, mix


def kernel(
    sec, anc, cd_in, rt_in, sp_in, mx_in,
    reg, acc,
    ib, fb, jb, ab, i32, j32, lxb, lyb, cd, w1, rt, sp, mx,
    wb, qb, tb, gacc, qd, vb, ub, lhs, bdacc, sums, dsums,
    etop, ebot, emid, htop, hbot, jmid, jbot,
    gs, gn, gp, gt, gfs, gbs, gb2s, gf, gb, gb2, ga, gx, bms, bm, bds, bhs, baa, bdo, bdh,
    cpad, csend, cprev, cnext, ew_s, ew, tw_s, tw,
    sem_in, sem_c, sem_a, rounds,
    s_f, r_f, s_j, r_j, s_h, r_h, s_n, r_n, s_g, r_g, s_bm, r_bm,
    s_bo, r_bo, s_bh, r_bh, s_ba, s_cp, r_cp, s_cn, r_cn, s_ew, r_ew, s_tw, r_tw,
):
    k = lax.axis_index("chain")
    s = lax.axis_index("quad")
    has_prev = k > 0
    has_next = k < NC - 1

    def remote(src, dst, ss, rs, kk, qq):
        return pltpu.make_async_remote_copy(
            src_ref=src, dst_ref=dst, send_sem=ss, recv_sem=rs,
            device_id={"chain": kk, "quad": qq}, device_id_type=MESH,
        )

    edge_rows = [(0, 16), (UP - 16, 16), (ROWS - 16, 16)]
    inner_rows = [(16, UP - 32), (UP, LOW - 16)]

    def in_copy(i):
        at, n = (edge_rows + inner_rows)[i]
        return pltpu.make_async_copy(sec.at[0, pl.ds(at, n)], ib.at[pl.ds(at, n)], sem_in.at[i])

    for i in range(3):
        in_copy(i).start()
    consts = [
        pltpu.make_async_copy(cd_in, cd, sem_c.at[0]),
        pltpu.make_async_copy(rt_in, rt, sem_c.at[1]),
        pltpu.make_async_copy(sp_in, sp, sem_c.at[2]),
        pltpu.make_async_copy(mx_in, mx, sem_c.at[3]),
    ]
    for d in consts:
        d.start()
    for i in range(3, 5):
        in_copy(i).start()
    anc_copies = [
        pltpu.make_async_copy(anc.at[pl.ds(0, UP)], fb, sem_a.at[0]),
        pltpu.make_async_copy(anc.at[pl.ds(UP, LOW)], ab, sem_a.at[1]),
    ]

    @pl.when(k == 0)
    def _():
        for d in anc_copies:
            d.start()

    barrier = pltpu.get_barrier_semaphore()

    qz = lax.div(s, 4)
    qy = lax.rem(s, 4)

    def greet(sem, q):
        pl.semaphore_signal(sem, inc=1, device_id={"chain": k, "quad": q}, device_id_type=MESH)

    def hello_quad(sem):
        for d in (1, 3):
            greet(sem, 4 * qz + lax.rem(qy + d, 4))
            greet(sem, 4 * lax.rem(qz + d, 4) + qy)

    def others():
        hops = lambda d: min(d, 4 - d)
        steps = sorted(((z, y) for z in range(4) for y in range(4) if z or y), key=lambda t: -hops(t[0]) - hops(t[1]))
        return [4 * lax.rem(qz + z, 4) + lax.rem(qy + y, 4) for z, y in steps]

    far_next = (qy == 3) & (s < NQ - 1)
    far_prev = (qy == 0) & (s > 0)

    def hello_chain(sem, step):
        for sign in (1, -1):
            kk = k + sign * step

            @pl.when((kk >= 0) & (kk < NC))
            def _():
                pl.semaphore_signal(sem, inc=1, device_id={"chain": kk, "quad": s}, device_id_type=MESH)

    def on_chain(step):
        one = jnp.int32(1)
        zero = jnp.int32(0)
        return jnp.where(k >= step, one, zero) + jnp.where(k + step < NC, one, zero)

    hello_quad(barrier)

    @pl.when(far_next)
    def _():
        greet(barrier, s + 1)

    @pl.when(far_prev)
    def _():
        greet(barrier, s - 1)

    hello_chain(barrier, 1)

    i32[:, :PAD] = jnp.zeros((ROWS + 16, PAD), F32)
    i32[:, PAD + COLS :] = jnp.zeros((ROWS + 16, PAD), F32)
    j32[:, :PAD] = jnp.zeros((LOW + 16, PAD), F32)
    j32[:, PAD + COLS :] = jnp.zeros((LOW + 16, PAD), F32)
    ub[:, :PAD] = jnp.zeros((32, PAD), F32)
    ub[:, PAD + COLS :] = jnp.zeros((32, PAD), F32)
    sums[...] = jnp.zeros_like(sums)
    qb[1] = jnp.zeros((5, ROWS, CH), BF16)
    tb[0] = jnp.zeros((96, CH), BF16)
    gacc[...] = jnp.zeros_like(gacc)
    qd[...] = jnp.zeros_like(qd)
    vb[...] = jnp.zeros_like(vb)
    dsums[...] = jnp.zeros_like(dsums)
    bdacc[...] = jnp.zeros_like(bdacc)
    cpad[...] = jnp.zeros_like(cpad)

    @pl.when(s == 0)
    def _():
        htop[...] = jnp.zeros_like(htop)
        gn[0] = jnp.zeros((96, 128), F32)

    @pl.when(s == NQ - 1)
    def _():
        hbot[...] = jnp.zeros_like(hbot)
        gn[1] = jnp.zeros((96, 128), F32)

    @pl.when(k == 0)
    def _():
        cprev[...] = jnp.zeros_like(cprev)

    @pl.when(k == NC - 1)
    def _():
        jb[...] = jnp.zeros_like(jb)
        jmid[...] = jnp.zeros_like(jmid)
        jbot[...] = jnp.zeros_like(jbot)
        cnext[...] = jnp.zeros_like(cnext)

    for j in range(NC - 1):
        @pl.when(j >= k)
        def _():
            ew[j] = jnp.zeros((8, 128), F32)

    far = jnp.where(far_next, jnp.int32(1), jnp.int32(0)) + jnp.where(far_prev, jnp.int32(1), jnp.int32(0))
    pl.semaphore_wait(barrier, 4 + far + on_chain(1))
    hello_quad(rounds.at[0])

    def f_copy(c):
        at = pl.multiple_of(c * CX, CX)
        return remote(
            sec.at[0, pl.ds(0, UP), pl.ds(at, CX)], fb.at[:, pl.ds(at, CX)],
            s_f, r_f.at[c], jnp.minimum(k + 1, NC - 1), s,
        )

    def j_copy(c):
        at = pl.multiple_of(c * CX, CX)
        return remote(
            sec.at[0, pl.ds(UP, LOW), pl.ds(at, CX)], jb.at[:, pl.ds(at, CX)],
            s_j, r_j.at[c], jnp.maximum(k - 1, 0), s,
        )

    @pl.loop(0, NX)
    def _(c):
        @pl.when(has_next)
        def _():
            f_copy(c).start()

        @pl.when(has_prev)
        def _():
            j_copy(c).start()

    up_top = remote(etop, hbot, s_h.at[0], r_h.at[0], k, jnp.maximum(s - 1, 0))
    down_bot = remote(ebot, htop, s_h.at[1], r_h.at[1], k, jnp.minimum(s + 1, NQ - 1))
    mid_prev = remote(emid, jmid, s_h.at[2], r_h.at[2], jnp.maximum(k - 1, 0), s)
    bot_prev = remote(hbot, jbot, s_h.at[3], r_h.at[3], jnp.maximum(k - 1, 0), s)

    for i in range(3):
        in_copy(i).wait()
    etop[...] = ib[0:16, :].astype(F32)[0:1]
    ebot[...] = ib[ROWS - 16 : ROWS, :].astype(F32)[15:16]
    emid[...] = ib[UP - 16 : UP, :].astype(F32)[15:16]

    @pl.when(s > 0)
    def _():
        up_top.start()

    @pl.when(s < NQ - 1)
    def _():
        down_bot.start()

    @pl.when(has_prev)
    def _():
        mid_prev.start()

    for d in consts:
        d.wait()
    lane = lax.broadcasted_iota(jnp.int32, (8, 128), 1)

    v = cd[pl.ds(CH, CH), :].astype(F32)
    ln = lax.broadcasted_iota(jnp.int32, (CH, 128), 1)
    knot = jnp.where(ln < GRID, ln, ln - GRID)
    for h in range(2):
        a = v if h == 0 else pltpu.roll(v, 128 - 2 * h, 1)
        b = pltpu.roll(v, 127 - 2 * h, 1)
        wb[:, h * 128 : (h + 1) * 128] = v * jnp.where(ln < GRID, a, b)

    @pl.loop(0, NCH // 4)
    def _(c4):
      for c in [4 * c4 + u for u in range(4)]:
        at = pl.multiple_of(c * CH, CH)
        for h in range(2):
            partner = knot + jnp.where(ln < GRID, 2 * h, 2 * h + 1)
            near = (jnp.abs(2 * (knot - 4 * c) - 3) < 16) & (partner < GRID)
            t = pltpu.roll(wb[:, h * 128 : (h + 1) * 128], lax.rem(4 * c + 124, 128), 1)
            w1[pl.ds(at, CH), h * 128 : (h + 1) * 128] = jnp.where(near, t, 0.0).astype(BF16)

    variant = jnp.where(s == 0, 0, jnp.where(s == NQ - 1, 2, 1))
    RB = 32

    def spot(c):
        return pl.multiple_of(jnp.maximum(c, 0) * CH, CH)

    for i in range(3, 5):
        in_copy(i).wait()

    pl.semaphore_wait(rounds.at[0], 4)
    hello_quad(rounds.at[1])

    @pl.loop(0, NCH // 2)
    def _(p):
        for c in [2 * p, 2 * p + 1]:
            at = pl.multiple_of(c * CH, CH)
            u = jnp.dot(rt[variant, 32:64, :], ib[:, pl.ds(at, CH)], preferred_element_type=F32)
            ub[0:8, pl.ds(at + PAD, CH)] = u[0:8] + u[8:16]
            ub[8:16, pl.ds(at + PAD, CH)] = u[16:24] + u[24:32]
            s1 = jnp.zeros((8, CH), F32)
            s2 = jnp.zeros((8, CH), F32)
            for r in range(0, ROWS, RB):
                x = ib[r : r + RB, pl.ds(at, CH)].astype(F32)
                i32[8 + r : 8 + r + RB, pl.ds(at + PAD, CH)] = x
                for t in range(0, RB, 8):
                    xt = x[t : t + 8]
                    s1 = s1 + xt
                    s2 = s2 + xt * xt
            sums[0] = sums[0] + s1[:, :128] + s1[:, 128:]
            sums[1] = sums[1] + s2[:, :128] + s2[:, 128:]

    @pl.when(s < NQ - 1)
    def _():
        up_top.wait_recv()

    @pl.when(s > 0)
    def _():
        down_bot.wait_recv()

    @pl.when(has_prev)
    def _():
        bot_prev.start()

    i32[7:8, PAD : PAD + COLS] = htop[...]
    i32[8 + ROWS : 9 + ROWS, PAD : PAD + COLS] = hbot[...]

    pl.semaphore_wait(rounds.at[1], 4)
    hello_quad(rounds.at[2])

    def tally(i, d, x):
        a = jnp.zeros((8, CH), F32)
        b = jnp.zeros((8, CH), F32)
        for t in range(0, d.shape[0], 8):
            a = a + d[t : t + 8]
            b = b + d[t : t + 8] * x[t : t + 8]
        dsums[i] = dsums[i] + a[:, :128] + a[:, 128:]
        dsums[i + 1] = dsums[i + 1] + b[:, :128] + b[:, 128:]

    def pixels(at, slot, with_anchor):
        for r in range(0, ROWS, RB):
            mid = i32[8 + r : 8 + r + RB, pl.ds(at, CH + 2 * PAD)]
            x = mid[:, PAD : PAD + CH]
            right = pltpu.roll(mid, CH + 2 * PAD - 1, 1)[:, PAD : PAD + CH]
            left = pltpu.roll(mid, 1, 1)[:, PAD : PAD + CH]
            lx = right - left
            lxb[r : r + RB, pl.ds(at, CH)] = lx
            tall = i32[r : r + RB + 16, pl.ds(at + PAD, CH)]
            below = pltpu.roll(tall, RB + 15, 0)[8 : 8 + RB]
            above = pltpu.roll(tall, 1, 0)[8 : 8 + RB]
            ly = below - above
            lyb[r : r + RB, pl.ds(at, CH)] = ly
            qb[slot, 0, r : r + RB, :] = (lx * lx).astype(BF16)
            qb[slot, 3, r : r + RB, :] = (x * right).astype(BF16)
            qb[slot, 1, r : r + RB, :] = (lx * ly).astype(BF16)
            qb[slot, 2, r : r + RB, :] = (ly * ly).astype(BF16)
            qb[slot, 4, r : r + RB, :] = (x * below).astype(BF16)
            if with_anchor:
                src, rr = (fb, r) if r < UP else (ab, r - UP)
                d = src[rr : rr + RB, pl.ds(at, CH)].astype(F32) - x
                qd[slot, 0, r : r + RB, :] = (d * lx).astype(BF16)
                qd[slot, 1, r : r + RB, :] = (d * ly).astype(BF16)
                tally(0, d, x)

    def rows_out(at, slot, with_anchor):
        for i in range(3):
            tb[slot, 32 * i : 32 + 32 * i, :] = jnp.dot(
                rt[variant, 0:32, :], qb[slot, i], preferred_element_type=F32
            ).astype(BF16)
        z = jnp.dot(rt[variant, 32:48, :], qb[slot, 3], preferred_element_type=F32)
        ub[16:24, pl.ds(at + PAD, CH)] = z[0:8] + z[8:16]
        q = jnp.dot(rt[variant, 64:80, :], qb[slot, 4], preferred_element_type=F32)
        ub[24:32, pl.ds(at + PAD, CH)] = q[0:8] + q[8:16]
        if with_anchor:
            for i in range(2):
                v = jnp.dot(rt[variant, 32:48, :], qd[slot, i], preferred_element_type=F32)
                v = v[0:8] + v[8:16]
                hi = v.astype(BF16).astype(F32)
                vb[slot, 16 * i : 16 * i + 16, :] = jnp.concatenate([hi, v - hi], axis=0).astype(BF16)

    def columns_out(at, slot, with_anchor):
        gacc[...] = gacc[...] + jnp.dot(tb[slot], w1[pl.ds(at, CH), :], preferred_element_type=F32)
        if with_anchor:
            b = jnp.dot(vb[slot, 0:32, :], cd[pl.ds(at, CH), :], preferred_element_type=F32)
            bdacc[0:8] = bdacc[0:8] + b[0:8] + b[8:16]
            bdacc[16:24] = bdacc[16:24] + b[16:24] + b[24:32]

    def own_pass(with_anchor):
        @pl.loop(0, NCH // 2)
        def _(p):
            @pl.when(p == 5)
            def _():
                pl.semaphore_wait(rounds.at[2], 4)
                hello_chain(rounds.at[3], 1)

            for u in range(2):
                c = 2 * p + u
                columns_out(spot(c - 2), u, with_anchor)
                pixels(spot(c), u, with_anchor)
                rows_out(spot(c - 1), 1 - u, with_anchor)

        columns_out(spot(NCH - 2), 0, with_anchor)
        rows_out(spot(NCH - 1), 1, with_anchor)
        columns_out(spot(NCH - 1), 1, with_anchor)

    @pl.when(k > 0)
    def _():
        own_pass(False)

    @pl.when(k == 0)
    def _():
        for d in anc_copies:
            d.wait()
        own_pass(True)

    first = lane < GRID

    def swap(v):
        return pltpu.roll(v, GRID, 1)

    quarter = lax.broadcasted_iota(jnp.int32, (8, 128), 0)

    def pack(a, b):
        return jnp.where(quarter < 4, pltpu.roll(a, 6, 0), pltpu.roll(b, 2, 0))

    order = [(di, h) for di in range(2) for h in range(1)]
    order = order + [(di, h) for di in range(4) for h in range(2) if (di, h) not in order]
    slots = []
    for di, h in order:
        part = lambda q: 0.25 * gacc[32 * q + 8 * di : 32 * q + 8 * di + 8, 128 * h : 128 * h + 128]
        xx, xy, yy = part(0), part(1), part(2)
        slots.append(jnp.where(first, xx, swap(yy)))
        slots.append(jnp.where(first, swap(xx), yy))
        slots.append(xy)
    for i in range(12):
        a, b = slots[2 * i], slots[2 * i + 1]
        gs[8 * i : 8 * i + 8, :] = pack(a, b)
        gp[8 * i : 8 * i + 8, :] = pack(pltpu.roll(a, 4, 0), pltpu.roll(b, 4, 0))

    to_next = remote(gp, gn.at[0], s_n.at[0], r_n.at[0], k, jnp.minimum(s + 1, NQ - 1))
    to_prev = remote(gp, gn.at[1], s_n.at[1], r_n.at[1], k, jnp.maximum(s - 1, 0))

    @pl.when(s < NQ - 1)
    def _():
        to_next.start()

    @pl.when(s > 0)
    def _():
        to_prev.start()

    @pl.loop(0, NCH // 4)
    def _(c4):
      for c in [4 * c4 + u for u in range(4)]:
        at = pl.multiple_of(c * CH, CH)
        wide = ub[:, pl.ds(at, CH + 2 * PAD)]
        right = pltpu.roll(wide, CH + 2 * PAD - 1, 1)[:, PAD : PAD + CH]
        left = pltpu.roll(wide, 1, 1)[:, PAD : PAD + CH]
        x = wide[:, PAD : PAD + CH]
        v = jnp.concatenate(
            [0.5 * (right[0:8] - left[0:8]), x[8:16], 0.5 * (x[16:24] - left[16:24]), x[24:32]], axis=0
        )
        hi = v.astype(BF16)
        lhs[0:32, pl.ds(at, CH)] = hi
        lhs[32:64, pl.ds(at, CH)] = (v - hi.astype(F32)).astype(BF16)

    bb = jnp.dot(lhs[...], cd[...], preferred_element_type=F32)
    bb = bb[0:32] + bb[32:64]
    bms[0:8, :] = jnp.where(first, bb[16:24], bb[24:32])
    bms[8:16, :] = jnp.where(first, bb[0:8], bb[8:16])

    def fold(a, b):
        ra = jnp.sum(a, axis=0, keepdims=True)
        rb = jnp.sum(b, axis=0, keepdims=True)
        return jnp.where(quarter == 0, ra, jnp.where(quarter == 1, rb, 0.0))

    bms[16:24, :] = fold(sums[0], sums[1])
    bm[s] = bms[...]

    def bm_copy(to, slot):
        return remote(bms, bm.at[slot], s_bm, r_bm, k, to)

    @pl.loop(1, NQ)
    def _(d):
        bm_copy(lax.rem(s + d, NQ), s).start()

    def gf_copy(to, slot):
        return remote(gfs, gf.at[slot], s_g.at[0], r_g.at[0], k, to)

    def gb_copy(to, slot):
        return remote(gbs, gb.at[slot], s_g.at[1], r_g.at[1], k, to)

    def gb2_copy(to, slot):
        return remote(gb2s, gb2.at[slot], s_g.at[2], r_g.at[2], k, to)

    def spread_gram():
        @pl.when(s > 0)
        def _():
            to_next.wait_recv()

        @pl.when(s < NQ - 1)
        def _():
            to_prev.wait_recv()

        lower_rows = (quarter == 0) | (quarter == 1) | (quarter == 4) | (quarter == 5)
        for i in range(12):
            b8 = slice(8 * i, 8 * i + 8)
            gt[b8, :] = gs[b8, :] + jnp.where(lower_rows, gn[0, b8, :], gn[1, b8, :])
        gfs[...] = gt[0:24, :]
        gbs[...] = gt[24:72, :].astype(BF16)
        gb2s[...] = jnp.concatenate([gt[72:96, :], jnp.zeros((8, 128), F32)], axis=0).astype(BF16)
        gb2[s] = gb2s[...]
        gf[s] = gfs[...]
        gb[s] = gbs[...]

        for to in others():
            gf_copy(to, s).start()

    @pl.when(has_next)
    def _():
        mid_prev.wait_recv()
        bot_prev.wait_recv()

    j32[7:8, PAD : PAD + COLS] = jmid[...]
    j32[8 + LOW : 9 + LOW, PAD : PAD + COLS] = jbot[...]

    def tuck(ref, at, a, b):
        ref[at : at + 1, :] = jnp.sum(a, axis=0, keepdims=True)
        ref[at + 1 : at + 2, :] = jnp.sum(b, axis=0, keepdims=True)

    def ba_copy(to, slot):
        return remote(baa, bdh.at[slot], s_ba, r_bh, k, to)

    def cross_rows(slot):
        v = jnp.concatenate(
            [jnp.dot(sp[...], qd[slot, i], preferred_element_type=F32) for i in range(2)], axis=0
        )
        v = jnp.concatenate(
            [v[0:8] + v[8:16], v[16:24] + v[24:32], v[32:40] + v[40:48], v[48:56] + v[56:64]], axis=0
        )
        hi = v.astype(BF16)
        vb[slot, 0:32, :] = hi
        vb[slot, 32:64, :] = (v - hi.astype(F32)).astype(BF16)

    def cross_columns(at, slot):
        b = jnp.dot(vb[slot], cd[pl.ds(at, CH), :], preferred_element_type=F32)
        bdacc[...] = bdacc[...] + b[0:32] + b[32:64]

    def both(at, slot, upper):
        for r in range(0, UP if upper else 0, RB):
            x = i32[8 + r : 8 + r + RB, pl.ds(at + PAD, CH)]
            d = fb[r : r + RB, pl.ds(at, CH)].astype(F32) - x
            qd[slot, 0, r : r + RB, :] = (d * lxb[r : r + RB, pl.ds(at, CH)]).astype(BF16)
            qd[slot, 1, r : r + RB, :] = (d * lyb[r : r + RB, pl.ds(at, CH)]).astype(BF16)
            tally(0, d, x)
        for r in range(0, LOW, RB):
            rr = UP + r
            mid = j32[8 + r : 8 + r + RB, pl.ds(at, CH + 2 * PAD)]
            x = mid[:, PAD : PAD + CH]
            right = pltpu.roll(mid, CH + 2 * PAD - 1, 1)[:, PAD : PAD + CH]
            left = pltpu.roll(mid, 1, 1)[:, PAD : PAD + CH]
            tall = j32[r : r + RB + 16, pl.ds(at + PAD, CH)]
            below = pltpu.roll(tall, RB + 15, 0)[8 : 8 + RB]
            above = pltpu.roll(tall, 1, 0)[8 : 8 + RB]
            d = i32[8 + rr : 8 + rr + RB, pl.ds(at + PAD, CH)] - x
            qd[slot, 0, rr : rr + RB, :] = (d * (right - left)).astype(BF16)
            qd[slot, 1, rr : rr + RB, :] = (d * (below - above)).astype(BF16)
            tally(2, d, x)

    def cross(upper):
        @pl.loop(0, NCH // 2)
        def _(p):
            @pl.when(p == HOOK)
            def _():
                spread_gram()

            arrive(p + 1)
            for u in range(2):
                c = 2 * p + u
                cross_columns(spot(c - 2), u)
                both(spot(c), u, upper)
                cross_rows(1 - u)

        cross_columns(spot(NCH - 2), 0)
        cross_rows(1)
        cross_columns(spot(NCH - 1), 1)

    @pl.when(k == 0)
    def _():
        baa[0:8, :] = 0.5 * jnp.where(first, bdacc[0:8], bdacc[16:24])
        bdacc[...] = jnp.zeros_like(bdacc)
        qd[...] = jnp.zeros_like(qd)
        vb[...] = jnp.zeros_like(vb)

        @pl.loop(1, NQ)
        def _(d):
            ba_copy(lax.rem(s + d, NQ), s).start()

        bdh[s] = baa[...]

    def arrive(piece):
        @pl.when(has_prev & (piece < NX))
        def _():
            f_copy(piece).wait_recv()

        @pl.when(has_next & (piece < NX))
        def _():
            j_copy(piece).wait_recv()

        at = pl.multiple_of(jnp.minimum(piece, NX - 1) * CX, CX)
        j32[8 : 8 + LOW, pl.ds(at + PAD, CX)] = jb[:, pl.ds(at, CX)].astype(F32)

    arrive(jnp.int32(0))

    @pl.when(k > 0)
    def _():
        cross(True)

    @pl.when(k == 0)
    def _():
        cross(False)

    bds[0:8, :] = 0.5 * jnp.where(first, bdacc[0:8], bdacc[16:24])
    bhs[0:8, :] = 0.5 * jnp.where(first, bdacc[8:16], bdacc[24:32])
    tuck(bds, 6, dsums[0], dsums[1])
    tuck(bhs, 0, dsums[2], dsums[3])

    def bo_copy(to, slot):
        return remote(bds, bdo.at[slot], s_bo, r_bo, k, to)

    def bh_copy(to, slot):
        return remote(bhs, bdh.at[slot], s_bh, r_bh, jnp.minimum(k + 1, NC - 1), to)

    pl.semaphore_wait(rounds.at[3], on_chain(1))
    hello_chain(rounds.at[4], 2)

    for to in others():
        @pl.when(has_next)
        def _():
            bh_copy(to, s).start()

        bo_copy(to, s).start()

    @pl.when(has_next)
    def _():
        bh_copy(s, s).start()

    bdo[s] = bds[...]

    for to in others():
        gb_copy(to, s).start()
        gb2_copy(to, s).start()


    def all_of(ref, n, ss, rs):
        return remote(ref.at[pl.ds(0, n)], ref.at[pl.ds(0, n)], ss, rs, k, lax.rem(s + 1, NQ))

    all_of(bm, NQ - 1, s_bm, r_bm).wait_recv()

    row = lax.broadcasted_iota(jnp.int32, (GRID, 128), 0)

    def merge(parts):
        even = jnp.concatenate(parts[0::2], axis=0)
        odd = jnp.concatenate(parts[1::2], axis=0)
        even = jnp.where(row < GRID - 2, pltpu.roll(even, GRID - 2, 0), 0.0)
        odd = jnp.where(row >= 2, pltpu.roll(odd, 2, 0), 0.0)
        return even + odd

    b_i = merge([bm[p, 0:8, :] for p in range(NQ)])
    b_1 = merge([bm[p, 8:16, :] for p in range(NQ)])

    def total(v):
        return jnp.sum(v, axis=(0, 1), keepdims=True)

    tot = bm[0, 16:24, :]
    for p in range(1, NQ):
        tot = tot + bm[p, 16:24, :]
    sum_i = total(tot[0:1])
    sum_ii = total(tot[1:2])

    all_of(bdo, NQ - 1, s_bo, r_bo).wait_recv()

    @pl.when(has_prev)
    def _():
        all_of(bdh, NQ, s_bh, r_bh).wait_recv()

    @pl.when(k == 0)
    def _():
        all_of(bdh, NQ - 1, s_ba, r_bh).wait_recv()

    parts = []
    tot_d = None
    tot_di = None
    for p in range(NQ):
        up, dn = bdo[p], bdh[p]
        parts.append(jnp.where(quarter < 6, up, 0.0) + jnp.where((quarter >= 2) | (k == 0), dn, 0.0))
        a = up[6:7] + jnp.where(k == 0, 0.0, dn[0:1])
        b = up[7:8] + jnp.where(k == 0, 0.0, dn[1:2])
        tot_d = a if p == 0 else tot_d + a
        tot_di = b if p == 0 else tot_di + b
    b_f = b_i + merge(parts)
    sum_f = sum_i + total(tot_d)
    sum_fi = sum_ii + total(tot_di)
    mean_f = sum_f * (1.0 / PIXELS)

    def apply_gram(c):
        cl = [c] + [pltpu.roll(c, 128 - d, 1) for d in range(1, 4)]
        cs = swap(c)
        csl = [cs] + [pltpu.roll(cs, 128 - d, 1) for d in range(1, 4)]
        out = None
        lacc = [None] * 4

        def add(a, b):
            return b if a is None else a + b

        for di in range(4):
            racc = None
            for dj in range(4):
                a = ga[4 * di + dj]
                x = gx[4 * di + dj]
                up = (lambda v: v) if di == 0 else (lambda v: pltpu.roll(v, GRID - di, 0))
                out = add(out, a * up(cl[dj]) + x * up(csl[dj]))
                if dj:
                    lacc[dj] = add(lacc[dj], a * up(c) + x * up(cs))
                if di:
                    racc = add(racc, a * cl[dj] + x * csl[dj])
                if di and dj:
                    racc = racc + pltpu.roll(a * c + x * cs, dj, 1)
            if di:
                out = out + pltpu.roll(racc, di, 0)
        for dj in range(1, 4):
            out = out + pltpu.roll(lacc[dj], dj, 1)
        return out

    def direction(c):
        if c is None:
            mean_w = sum_i * (1.0 / PIXELS)
            sq = sum_ii
            cross = sum_fi
            b_w = b_i
        else:
            h = apply_gram(c)
            mean_w = (sum_i + total(c * b_1)) * (1.0 / PIXELS)
            sq = sum_ii + total(c * (2.0 * b_i + h))
            cross = sum_fi + total(c * b_f)
            b_w = b_i + h
        var = sq - PIXELS * mean_w * mean_w
        cov = cross - PIXELS * mean_f * mean_w
        den = jnp.sqrt(var + EPS)
        ratio = cov / den / (var + EPS)
        grad = PIXELS * ((b_f - mean_f * b_1) / den - ratio * (b_w - mean_w * b_1))
        mag = total(grad * grad) * (1.0 / (GRID * 2 * GRID))
        return grad / jnp.sqrt(mag + EPS)

    rate = 1.0 / ITERATIONS

    def cp_copy(i):
        return remote(csend.at[i], cprev.at[i], s_cp.at[i], r_cp.at[i], jnp.minimum(k + 1, NC - 1), s)

    def cn_copy(i):
        return remote(csend.at[i], cnext.at[i], s_cn.at[i], r_cn.at[i], jnp.maximum(k - 1, 0), s)

    def exchange(i, c):
        csend[i] = c

        @pl.when(has_next)
        def _():
            cp_copy(i).start()

        @pl.when(has_prev)
        def _():
            cn_copy(i).start()

    def receive(i):
        @pl.when(has_prev)
        def _():
            cp_copy(i).wait_recv()

        @pl.when(has_next)
        def _():
            cn_copy(i).wait_recv()

    c = rate * direction(None)
    exchange(0, c)

    pl.semaphore_wait(rounds.at[4], on_chain(2))
    hello_chain(rounds.at[5], 4)

    all_of(gf, NQ - 1, s_g.at[0], r_g.at[0]).wait_recv()
    all_of(gb, NQ - 1, s_g.at[1], r_g.at[1]).wait_recv()
    all_of(gb2, NQ - 1, s_g.at[2], r_g.at[2]).wait_recv()
    for m in range(8):
        ab_f = [gf[2 * m + j] for j in range(2)]
        ab_b = [
            jnp.concatenate([gb[2 * m + j].astype(F32), gb2[2 * m + j].astype(F32)], axis=0) for j in range(2)
        ]
        for i in range(12):
            src = ab_f if i < 3 else ab_b
            o = 8 * i if i < 3 else 8 * (i - 3)
            a, b = src[0][o : o + 8], src[1][o : o + 8]
            pair = (
                jnp.where(quarter < 4, a, pltpu.roll(b, 4, 0)),
                jnp.where(quarter < 4, pltpu.roll(a, 4, 0), b),
            )
            for j in range(2):
                (di, h), which = order[(2 * i + j) // 3], (2 * i + j) % 3
                v = pair[j]
                if di and m == 7:
                    v = jnp.where(quarter < 8 - di, v, 0.0)
                m8 = slice(8 * m, 8 * m + 8)
                if which < 2:
                    ga[4 * di + 2 * h + which, m8, :] = v
                else:
                    o2 = swap(v)
                    gx[4 * di + 2 * h, m8, :] = jnp.where(first, v, o2)
                    gx[4 * di + 2 * h + 1, m8, :] = jnp.where(first, o2, v)

    for i in range(1, ITERATIONS - 1):
        step = c + rate * direction(c)
        receive(i - 1)
        c = step + SMOOTHING * (cprev[i - 1] - 2.0 * c + cnext[i - 1])
        exchange(i, c)
    step = c + rate * direction(c)

    base = pl.multiple_of(lax.div(4 * s + 6, 8) * 8, 8)
    even = lax.rem(s, 2) == 0

    def window(v):
        cpad[8 : 8 + GRID] = v
        w = cpad[pl.ds(base, 16), :]
        return jnp.where(even, w[6:14], w[2:10])

    cw = window(c)
    mine = window(step) - jnp.where(k == 0, SMOOTHING, 0.0) * cw
    ew_s[...] = mine

    pl.semaphore_wait(rounds.at[5], on_chain(4))

    def ew_copy(to, slot):
        return remote(ew_s, ew.at[slot], s_ew.at[to], r_ew.at[slot], to, s)

    for kk in range(NC - 1, 0, -1):
        @pl.when(kk > k)
        def _():
            ew_copy(kk, k).start()

    receive(ITERATIONS - 2)
    nxt = window(cnext[ITERATIONS - 2])
    own = mine + SMOOTHING * (nxt - cw)

    for kk in range(NC - 1):
        @pl.when(kk < k)
        def _():
            ew_copy(kk, kk).wait_recv()

    t = ew[0]
    for kk in range(1, NC - 1):
        t = t + ew[kk]
    t = t + own
    tw_s[...] = t

    def tw_copy(to, slot):
        return remote(tw_s, tw.at[slot], s_tw, r_tw, k, to)

    for to in others():
        tw_copy(to, s).start()

    tw[s] = t

    hi = t.astype(BF16)
    rest = t - hi.astype(F32)
    mid = rest.astype(BF16)
    low = (rest - mid.astype(F32)).astype(BF16)
    stack = jnp.concatenate(
        [v.astype(F32) for v in (hi, mid, low, hi, mid, hi)] + [jnp.zeros((80, 128), F32)], axis=0
    ).astype(BF16)
    mixed = jnp.dot(mx[...], stack, preferred_element_type=F32).astype(BF16).astype(F32) * 0.5
    big_first = lax.broadcasted_iota(jnp.int32, (ROWS, 128), 1) < GRID
    mixed_x = jnp.where(big_first, mixed, 0.0).astype(BF16)
    mixed_y = jnp.where(big_first, 0.0, mixed).astype(BF16)
    dims = (((1,), (1,)), ((), ()))

    @pl.loop(0, NCH // 8)
    def _(p):
        for u in range(8):
            at = pl.multiple_of((8 * p + u) * CH, CH)
            table = cd[pl.ds(at, CH), :]
            sx = lax.dot_general(mixed_x, table, dims, preferred_element_type=F32)
            sy = lax.dot_general(mixed_y, table, dims, preferred_element_type=F32)
            v = (
                i32[8 : 8 + ROWS, pl.ds(at + PAD, CH)]
                + sx * lxb[:, pl.ds(at, CH)]
                + sy * lyb[:, pl.ds(at, CH)]
            )
            reg[0, :, pl.ds(at, CH)] = v.astype(BF16)

    all_of(tw, NQ - 1, s_tw, r_tw).wait_recv()

    for m in range(8):
        acc[0, 8 * m : 8 * m + 8, :] = jnp.concatenate([tw[2 * m, 2:6, :], tw[2 * m + 1, 2:6, :]], axis=0)

    @pl.when(s > 0)
    def _():
        up_top.wait_send()

    @pl.when(s < NQ - 1)
    def _():
        down_bot.wait_send()

    @pl.when(has_prev)
    def _():
        mid_prev.wait_send()
        bot_prev.wait_send()


    @pl.when(has_next)
    def _():
        remote(sec.at[0, pl.ds(0, UP)], fb, s_f, r_f.at[0], jnp.minimum(k + 1, NC - 1), s).wait_send()

    @pl.when(has_prev)
    def _():
        remote(sec.at[0, pl.ds(UP, LOW)], jb, s_j, r_j.at[0], jnp.maximum(k - 1, 0), s).wait_send()

    @pl.when(s < NQ - 1)
    def _():
        to_next.wait_send()

    @pl.when(s > 0)
    def _():
        to_prev.wait_send()

    @pl.when(has_next)
    def _():
        all_of(bdh, NQ, s_bh, r_bh).wait_send()

    all_of(gf, NQ - 1, s_g.at[0], r_g.at[0]).wait_send()
    all_of(gb, NQ - 1, s_g.at[1], r_g.at[1]).wait_send()
    all_of(gb2, NQ - 1, s_g.at[2], r_g.at[2]).wait_send()
    all_of(bm, NQ - 1, s_bm, r_bm).wait_send()
    all_of(bdo, NQ - 1, s_bo, r_bo).wait_send()

    @pl.when(k == 0)
    def _():
        all_of(bdh, NQ - 1, s_ba, r_bh).wait_send()

    all_of(tw, NQ - 1, s_tw, r_tw).wait_send()

    for i in range(ITERATIONS - 1):
        @pl.when(has_next)
        def _():
            cp_copy(i).wait_send()

        @pl.when(has_prev)
        def _():
            cn_copy(i).wait_send()

    for kk in range(1, NC):
        @pl.when(kk > k)
        def _():
            ew_copy(kk, k).wait_send()


def solution(mesh):
    c, rows, split, mix = tables()

    def body(sections, anchor):
        v = pltpu.VMEM
        dma = pltpu.SemaphoreType.DMA
        row = v((1, COLS), F32)
        win = v((NQ, 8, 128), F32)
        scratch = [
            v((ROWS, COLS), BF16), v((UP, COLS), BF16), v((LOW, COLS), BF16), v((LOW, COLS), BF16),
            v((ROWS + 16, COLS + 2 * PAD), F32), v((LOW + 16, COLS + 2 * PAD), F32),
            v((ROWS, COLS), F32), v((ROWS, COLS), F32),
            v((COLS, 128), BF16), v((COLS, 256), BF16),
            v((3, 80, ROWS), BF16), v((32, ROWS), BF16), v((ROWS, 128), BF16),
            v((CH, 256), F32), v((2, 5, ROWS, CH), BF16), v((2, 96, CH), BF16), v((96, CH), F32),
            v((2, 2, ROWS, CH), BF16), v((2, 64, CH), BF16),
            v((32, COLS + 2 * PAD), F32), v((64, COLS), BF16), v((32, 128), F32),
            v((2, 8, 128), F32), v((4, 8, 128), F32),
            row, row, row, row, row, row, row,
            v((96, 128), F32), v((2, 96, 128), F32), v((96, 128), F32), v((96, 128), F32),
            v((24, 128), F32), v((48, 128), BF16), v((32, 128), BF16),
            v((NQ, 24, 128), F32), v((NQ, 48, 128), BF16), v((NQ, 32, 128), BF16),
            v((16, GRID, 128), F32), v((16, GRID, 128), F32),
            v((24, 128), F32), v((NQ, 24, 128), F32), v((8, 128), F32), v((8, 128), F32), v((8, 128), F32), win, win,
            v((GRID + 16, 128), F32), v((3, GRID, 128), F32), v((3, GRID, 128), F32), v((3, GRID, 128), F32),
            v((8, 128), F32), v((NC - 1, 8, 128), F32), v((8, 128), F32), v((NQ, 8, 128), F32),
            dma((5,)), dma((4,)), dma((2,)), pltpu.SemaphoreType.REGULAR((6,)),
            dma, dma((NX,)), dma, dma((NX,)), dma((4,)), dma((4,)), dma((2,)), dma((2,)),
            dma((3,)), dma((3,)), dma, dma, dma, dma, dma, dma, dma,
            dma((3,)), dma((3,)), dma((3,)), dma((3,)), dma((NC,)), dma((NC,)), dma, dma,
        ]
        anywhere = pl.BlockSpec(memory_space=pl.ANY)
        inside = pl.BlockSpec(memory_space=pltpu.VMEM)
        return pl.pallas_call(
            kernel,
            out_shape=(
                pltpu.VMEM((1, ROWS, COLS), BF16),
                pltpu.VMEM((1, GRID, 2 * GRID), F32),
            ),
            in_specs=[anywhere] * 6,
            out_specs=(inside, inside),
            scratch_shapes=scratch,
            compiler_params=pltpu.CompilerParams(
                collective_id=0, has_side_effects=True, vmem_limit_bytes=64_900_000
            ),
        )(
            sections, anchor,
            jnp.asarray(c, BF16), jnp.asarray(rows, BF16), jnp.asarray(split, BF16), jnp.asarray(mix, BF16),
        )

    return jax.shard_map(
        body, mesh=mesh,
        in_specs=(P("chain", "quad", None), P("quad", None)),
        out_specs=(P("chain", "quad", None), P("chain", None, None)),
        check_vma=False,
    )
```
